256 devices in a mesh: span: 64 (over y, z, core), depth: 4 (over x).
Axes of the slice: x: 4, y: 4, z: 8, core: 2. Of those that a mesh axis runs over, the one named last changes fastest.
Arguments:
- part_slab: int32 [4, 524288, 1], P('depth', 'span'), may hold values from 0 to 63; in each aligned block of 8192 rows (0 to 8191, 8192 to 16383, ..., all dimensions but the last counted through in order) at most 256 rows name the same one
- part_cell: int32 [4, 524288], P('depth', 'span'), may hold values from 0 to 65535
- part_volume: float32 [4, 524288], P('depth', 'span'), may hold values from 0.05 to 0.6
- part_drag: float32 [3, 4, 524288], P(None, 'depth', 'span'), may hold values from -6 to 6
- part_count: int32 [4, 64], P('depth', 'span'), may hold values from 7168 to 8192
- prior_solid: float32 [8, 1024, 2048], P(None, 'span', 'depth'), may hold values from 0 to 0.6
- prior_drag: float32 [3, 8, 1024, 2048], P(None, None, 'span', 'depth'), may hold values from -4 to 4
Outputs:
- fields: float32 [4, 8, 1024, 2048], P(None, None, 'span', 'depth')
- feedback: float32 [4, 4, 524288], P(None, 'depth', 'span')
The draws below stay inside these ranges and needn't reach their ends.
Inputs may be any that keep to these rules, and one draw needn't show every extreme that they name: `part_slab`: among the 8192 particle slots of one owner device, live or not, no slab is named more than 256 times; in every draw some device names a slab exactly 256 times.
All inputs are finite; a program needn't handle non-finite values.
Results may differ from the reference program's by a relative error of at most 0.0003.
Values sent between devices are 32-bit elements; how exact they have to be, the bound alone decides.
No kernel may reach another device: no remote copies, remote signals or barrier semaphores. Data moves between devices by JAX's collectives and lax.ppermute only.
A program may use at most 128 MiB of HBM per device.

```python
import math
import jax
import jax.numpy as jnp
import numpy as np

CX = 16
CY = 512
LAYERS = 8
SWEEPS = 6
PART_DEV = 8192
CAP = 256
NX = 1024
NY = 2048
SPAN_PARTS = 524288
N_SPAN = 64
N_DEPTH = 4


def with_ends(entries, own_key, low, top_value):
    spot = [jax.random.randint(jax.random.fold_in(own_key, axis), (), 0, length) for axis, length in enumerate(entries.shape)]
    longest = entries.shape.index(max(entries.shape))
    next_to = spot[:longest] + [(spot[longest] + 1) % entries.shape[longest]] + spot[longest + 1:]
    return entries.at[tuple(spot)].set(low).at[tuple(next_to)].set(top_value)


def levels(stream_key, extent, split, least, high):
    factor_of, own = 1.0, jax.random.fold_in(stream_key, 6)
    for axis_at, shards_of in split:
        draws = jnp.exp(jax.random.uniform(jax.random.fold_in(own, axis_at), (shards_of,), jnp.float32, least / len(split), high / len(split)))
        factor_of = factor_of * jnp.repeat(draws, extent[axis_at] // shards_of).reshape([-1 if axis == axis_at else 1 for axis in range(len(extent))])
    return factor_of


def deal_out(key, own, number, rows, number_of, top, most, skew):
    ranking = jax.random.permutation(key, number_of)
    crowded, usual = portions_of(number_of, rows * top, most, skew, True), portions_of(number_of, rows * top, most, skew, False)
    places = jnp.arange(number_of)

    def named(lengths, rotation):
        used = int((lengths > 0).sum())
        fixed = max(1, used // 4)
        passed = fixed + (places - fixed + rotation * (used - fixed)) % max(1, number_of - fixed)
        return jnp.zeros((number_of,), jnp.int32).at[ranking[jnp.where(places < fixed, places, passed)]].set(jnp.asarray(lengths, jnp.int32))

    lengths = jnp.where(number % 4 == 0, named(crowded, number // 4), named(usual, number - number // 4 - 1))
    mixed = jax.random.permutation(jax.random.fold_in(own, 3), number_of)
    giver, receiver = mixed[0:number_of // 2 * 2:2], mixed[1:number_of // 2 * 2:2]
    room = jnp.minimum(lengths[giver] - 1, most - lengths[receiver]) // 2
    room = jnp.where((giver == ranking[0]) | (receiver == ranking[0]) | (lengths[receiver] == 0), 0, jnp.maximum(room, 0))
    passed = jax.random.randint(jax.random.fold_in(own, 4), (number_of // 2,), 0, 1 << 20) % (room + 1)
    lengths = lengths.at[giver].add(-passed).at[receiver].add(passed)
    labels = jnp.searchsorted(jnp.cumsum(lengths), jnp.arange(rows * top), side="right").astype(jnp.int32)
    table = labels.reshape(top, rows).T
    table = table[jax.random.permutation(jax.random.fold_in(own, 1), rows)]
    rotation = jax.random.randint(jax.random.fold_in(own, 2), (rows, 1), 0, top)
    return jnp.take_along_axis(table, (jnp.arange(top)[None, :] + rotation) % top, axis=1)


def portions_of(number_of, total, most, lean, full):
    portions = [(1 << 20) // math.isqrt(grade ** lean) + 1 for grade in range(1, number_of + 1)]
    largest = most if full else min(most, max(-(-total // number_of), total * portions[0] // sum(portions)))
    least = 1 if total - largest >= number_of - 1 else 0
    holding, rest = [largest] + [least] * (number_of - 1), total - largest - least * (number_of - 1)
    while rest > 0:
        free = [i for i in range(1, number_of) if holding[i] < largest] or [i for i in range(1, number_of) if holding[i] < most]
        mass, remaining = sum([portions[i] for i in free]), rest
        for i in free:
            more = min(most - holding[i], max(1, remaining * portions[i] // mass), rest)
            holding[i] = holding[i] + more
            rest = rest - more
    return np.array(holding)


def normal_values(stream_key, dims, scale, bound, pieces=(), held_as=jnp.bfloat16):
    values = jax.random.normal(stream_key, dims, jnp.float32) * scale
    if len(pieces) > 0:
        values = levels(stream_key, dims, pieces, -0.22, 0.18) * values
    return jnp.clip(values, min=-bound, max=bound).astype(held_as)


def setup_inputs(seed: int = 0) -> dict:
    key_of = jax.random.split(jax.random.key(seed), 8)
    part_slab_keys = jax.random.split(jax.random.fold_in(key_of[0], 1), N_DEPTH * SPAN_PARTS // PART_DEV)
    part_slab_turns = jax.random.permutation(jax.random.fold_in(key_of[0], 3), N_DEPTH * SPAN_PARTS // PART_DEV)
    part_slab = jax.vmap(lambda own, number: deal_out(jax.random.fold_in(key_of[0], 2), own, number, PART_DEV, N_SPAN, 1, CAP, 2))(part_slab_keys, part_slab_turns).reshape((N_DEPTH, SPAN_PARTS, 1))
    part_cell = with_ends(jax.random.randint(key_of[1], (N_DEPTH, SPAN_PARTS), 0, LAYERS * CX * CY), jax.random.fold_in(key_of[1], 1), 0, (LAYERS * CX * CY) - 1).astype(jnp.int32)
    part_volume = jnp.clip(jnp.exp(math.log(0.6) - 2.4849067 * jax.random.uniform(key_of[2], (N_DEPTH, SPAN_PARTS), jnp.float32) ** levels(key_of[2], (N_DEPTH, SPAN_PARTS), ((0, 4), (1, 64)), -0.2, 0.2)), 0.05, 0.6)
    part_drag = normal_values(key_of[3], (3, N_DEPTH, SPAN_PARTS), 1.0, 6.0, ((1, 4), (2, 64)), jnp.float32)
    part_count = with_ends(jax.random.randint(key_of[4], (N_DEPTH, N_SPAN), PART_DEV * 7 // 8, PART_DEV + 1), jax.random.fold_in(key_of[4], 1), PART_DEV * 7 // 8, PART_DEV).astype(jnp.int32)
    prior_solid = jnp.clip(0.6 * jax.random.uniform(key_of[5], (LAYERS, NX, NY), jnp.float32) ** levels(key_of[5], (LAYERS, NX, NY), ((1, 64), (2, 4)), -0.2, 0.2), 0.0, 0.6)
    prior_drag = normal_values(key_of[6], (3, LAYERS, NX, NY), 0.5, 4.0, ((2, 64), (3, 4)), jnp.float32)
    return dict(part_slab=part_slab, part_cell=part_cell, part_volume=part_volume, part_drag=part_drag, part_count=part_count, prior_solid=prior_solid, prior_drag=prior_drag)


NU_WEIGHT = 1.0
PHI_LIMIT = 0.6


def relax_once(source, padded):
    beside = padded[:, :, 2:, 1:-1] + padded[:, :, :-2, 1:-1]
    beside = beside + padded[:, :, 1:-1, 2:] + padded[:, :, 1:-1, :-2]
    return (source + NU_WEIGHT * beside) / (1.0 + 4.0 * NU_WEIGHT)


def reference(part_slab, part_cell, part_volume, part_drag, part_count, prior_solid, prior_drag):
    depth_count = part_cell.shape[0]
    span_rows = part_cell.shape[1]
    grid_x = CX * N_SPAN
    grid_y = CY * N_DEPTH
    slab_index = part_slab[:, :, 0]
    column = jnp.arange(span_rows, dtype=jnp.int32)
    owner_index = column // PART_DEV
    within = column % PART_DEV
    counts = part_count[:, owner_index]
    live_weight = (within[None, :] < counts).astype(jnp.float32)
    layer_index = part_cell // (CX * CY)
    local_x = (part_cell // CY) % CX
    local_y = part_cell % CY
    depth_row = jnp.arange(depth_count, dtype=jnp.int32)[:, None]
    flat_index = layer_index * (grid_x * grid_y) + (slab_index * CX + local_x) * grid_y + depth_row * CY + local_y
    flat_index = flat_index.astype(jnp.int32).reshape(-1)
    payload = jnp.concatenate([part_volume[None], part_drag], axis=0) * live_weight[None]
    deposit = jax.ops.segment_sum(payload.reshape(4, -1).T, flat_index, num_segments=LAYERS * grid_x * grid_y)
    deposit = deposit.T.reshape(4, LAYERS, grid_x, grid_y)
    target = jnp.concatenate([jnp.minimum(deposit[:1], PHI_LIMIT), deposit[1:]], axis=0)
    smooth = jnp.concatenate([prior_solid[None], prior_drag], axis=0)
    for sweep_index in range(SWEEPS):
        padded = jnp.pad(smooth, ((0, 0), (0, 0), (1, 1), (1, 1)))
        smooth = relax_once(target, padded)
    void_fraction = 1.0 - smooth[0]
    fields = jnp.concatenate([void_fraction[None], -smooth[1:] / void_fraction[None]], axis=0)
    feedback = fields.reshape(4, -1)[:, flat_index].reshape(4, depth_count, span_rows) * live_weight[None]
    return (fields, feedback)
```

```python
import jax
import jax.numpy as jnp
from jax import lax
from jax.experimental import pallas as pl
from jax.experimental.pallas import tpu as pltpu
from jax.sharding import PartitionSpec as P

F32, BF16, I32 = jnp.float32, jnp.bfloat16, jnp.int32
OWNERS = 64
CAP = 256
LAYERS, CX, CY = 8, 16, 512
PARTS = 8192
HI, LO = 256, 256
ROWS = 2 * 5
BACK_ROWS = 8
SWEEPS = 6
PRIOR_RIM, TARGET_RIM = SWEEPS, SWEEPS - 1
PHI_LIMIT = 0.6


def halves(value):
    high = value.astype(BF16)
    return high, (value - high.astype(F32)).astype(BF16)


def spread(row, size):
    n = row.shape[1]
    packed = jnp.broadcast_to(row, (16, n)).astype(BF16)
    return jnp.broadcast_to(packed[None], (size // 16, 16, n)).reshape(size, n)


def index_rows(size, n):
    return lax.broadcasted_iota(I32, (size, n), 0).astype(F32).astype(BF16)


def row_is(row, size):
    return index_rows(size, row.shape[1]) == spread(row, size)


def one_hot(row, size):
    return jnp.where(row_is(row, size), jnp.ones((), BF16), jnp.zeros((), BF16))


def dot_nt(left, right):
    return lax.dot_general(left, right, (((1,), (1,)), ((), ())), preferred_element_type=F32)


def dot_nn(left, right):
    return lax.dot_general(left, right, (((1,), (0,)), ((), ())), preferred_element_type=F32)


PACK_BLOCK = 1024
SUB = 256


def pack_kernel(count_ref, slab_ref, cell_ref, volume_ref, drag_ref, out_ref, position_ref, acc):
    count = count_ref[0, 0]
    acc[...] = jnp.zeros_like(acc)
    before_mask = lax.broadcasted_iota(I32, (SUB, SUB + 128), 0)
    after_mask = lax.broadcasted_iota(I32, (SUB, SUB + 128), 1)
    upper = jnp.where((before_mask < after_mask) | (after_mask >= SUB), 1.0, 0.0).astype(BF16)

    def step(block, offset):
        hots, lefts = [], []
        for sub in range(PACK_BLOCK // SUB):
            start = pl.multiple_of(block * PACK_BLOCK + sub * SUB, SUB)
            spot = pl.ds(start, SUB)
            lane = lax.broadcasted_iota(I32, (1, SUB), 1) + start
            slab = jnp.where(lane < count, slab_ref[0:1, spot], OWNERS).astype(F32)
            member = row_is(slab, OWNERS)
            member_one = jnp.where(member, jnp.ones((), BF16), jnp.zeros((), BF16))
            ranks = dot_nn(member_one, upper)
            place = ranks[:, :SUB] + jnp.concatenate([offset, offset], axis=1)
            position = jnp.sum(place * member_one.astype(F32), axis=0, keepdims=True)
            offset = offset + ranks[:, SUB:]
            position_ref[0:1, spot] = position
            hots.append(one_hot(position, CAP))
            cell = cell_ref[0:1, spot]
            cell_high = lax.shift_right_logical(cell, 8)
            rows = [cell_high.astype(F32), (cell - cell_high * 256).astype(F32)]
            for value in [volume_ref[0:1, spot]] + [drag_ref[k, 0:1, spot] for k in range(3)]:
                high = value.astype(BF16).astype(F32)
                rows += [high, value - high]
            zero = jnp.zeros((), BF16)
            lefts.append(
                jnp.concatenate([jnp.where(member, spread(row, OWNERS), zero) for row in rows], axis=0)
            )
        acc[...] += dot_nt(jnp.concatenate(lefts, axis=1), jnp.concatenate(hots, axis=1))
        return offset

    lax.fori_loop(0, PARTS // PACK_BLOCK, step, jnp.zeros((OWNERS, 128), F32))
    for comp in range(5):
        high = acc[2 * comp * OWNERS : (2 * comp + 1) * OWNERS, :]
        low = acc[(2 * comp + 1) * OWNERS : (2 * comp + 2) * OWNERS, :]
        whole = high * 256.0 + low if comp == 0 else high + low
        for half in range(2):
            out_ref[pl.ds(2 * comp + half, OWNERS, stride=ROWS), :] = whole[:, half * 128 : (half + 1) * 128]


def pack(count, slab, cell, volume, drag):
    vmem = pl.BlockSpec(memory_space=pltpu.VMEM)
    return pl.pallas_call(
        pack_kernel,
        out_shape=(
            jax.ShapeDtypeStruct((OWNERS * ROWS, 128), F32),
            jax.ShapeDtypeStruct((1, PARTS), F32),
        ),
        in_specs=[pl.BlockSpec(memory_space=pltpu.SMEM), vmem, vmem, vmem, vmem],
        out_specs=(vmem, vmem),
        scratch_shapes=[pltpu.VMEM((10 * OWNERS, CAP), F32)],
        name="pack",
    )(count, slab, cell, volume, drag)


SOURCES_AT_ONCE = 4


def cell_split(cell):
    cell = cell.astype(I32)
    layer_x = lax.shift_right_logical(cell, 9)
    layer = lax.shift_right_logical(cell, 13)
    x = layer_x - layer * 16
    y_half = lax.shift_right_logical(cell, 8) - layer_x * 2
    high = (y_half * 16 + x) * 8 + layer
    low = cell - lax.shift_right_logical(cell, 8) * 256
    return high.astype(F32), low.astype(F32)


def source_row(ref, source, comp):
    base = source * ROWS + 2 * comp
    return jnp.concatenate([ref[pl.ds(base, 1), :], ref[pl.ds(base + 1, 1), :]], axis=1)


def deposit_kernel(recv_ref, out_ref, first_ref, last_ref):
    out_ref[...] = jnp.zeros_like(out_ref)
    zero = jnp.zeros((), BF16)

    def step(block, carry):
        lows, members, values = [], [], []
        for sub in range(SOURCES_AT_ONCE):
            source = block * SOURCES_AT_ONCE + sub
            high, low = cell_split(source_row(recv_ref, source, 0))
            lows.append(one_hot(low, LO))
            members.append(row_is(high, HI))
            parts = []
            for comp in range(4):
                value = source_row(recv_ref, source, comp + 1)
                top = value.astype(BF16).astype(F32)
                parts.append((top, value - top))
            values.append(parts)
        right = jnp.concatenate(lows, axis=1)
        right2 = jnp.concatenate([right, right], axis=1)
        for comp in range(4):
            left = [
                jnp.where(members[sub], spread(values[sub][comp][part], HI), zero)
                for part in range(2)
                for sub in range(SOURCES_AT_ONCE)
            ]
            out_ref[comp] += dot_nt(jnp.concatenate(left, axis=1), right2)
        return carry

    lax.fori_loop(0, OWNERS // SOURCES_AT_ONCE, step, 0)
    out_ref[0] = jnp.minimum(out_ref[0], PHI_LIMIT)
    for comp in range(4):
        for step_x in range(TARGET_RIM):
            spot = pl.ds((comp * TARGET_RIM + step_x) * LAYERS, LAYERS)
            for half in range(2):
                lanes = pl.ds(half * LO, LO)
                first_ref[spot, lanes] = out_ref[comp, pl.ds((half * CX + step_x) * LAYERS, LAYERS), :]
                x = CX - TARGET_RIM + step_x
                last_ref[spot, lanes] = out_ref[comp, pl.ds((half * CX + x) * LAYERS, LAYERS), :]


def deposit(received):
    vmem = pl.BlockSpec(memory_space=pltpu.VMEM)
    edge = jax.ShapeDtypeStruct((4 * TARGET_RIM * LAYERS, CY), F32)
    return pl.pallas_call(
        deposit_kernel,
        out_shape=(jax.ShapeDtypeStruct((4, HI, LO), F32), edge, edge),
        in_specs=[vmem],
        out_specs=(vmem, vmem, vmem),
        name="deposit",
    )(received)


GATHER_SOURCES = 2


def gather_kernel(table_ref, recv_ref, out_ref, tops, bottoms):
    for comp in range(4):
        tops[comp], bottoms[comp] = halves(table_ref[comp])

    def step(block, carry):
        highs, lows = [], []
        for sub in range(GATHER_SOURCES):
            high, low = cell_split(source_row(recv_ref, block * GATHER_SOURCES + sub, 0))
            highs.append(high)
            lows.append(one_hot(low, LO))
        low_hot = jnp.concatenate(lows, axis=1)
        high_row = jnp.concatenate(highs, axis=1)
        n = high_row.shape[1]
        member = lax.broadcasted_iota(I32, (HI, n), 0).astype(F32) == high_row
        rows = []
        for comp in range(4):
            value = dot_nn(tops[comp], low_hot) + dot_nn(bottoms[comp], low_hot)
            rows.append(jnp.sum(jnp.where(member, value, 0.0), axis=0, keepdims=True))
        for sub in range(GATHER_SOURCES):
            pieces = [
                row[:, sub * CAP + half * 128 : sub * CAP + (half + 1) * 128] for row in rows for half in range(2)
            ]
            start = pl.multiple_of((block * GATHER_SOURCES + sub) * BACK_ROWS, BACK_ROWS)
            out_ref[pl.ds(start, BACK_ROWS), :] = jnp.concatenate(pieces, axis=0)
        return carry

    lax.fori_loop(0, OWNERS // GATHER_SOURCES, step, 0)


def gather(table, received):
    vmem = pl.BlockSpec(memory_space=pltpu.VMEM)
    return pl.pallas_call(
        gather_kernel,
        out_shape=jax.ShapeDtypeStruct((OWNERS * BACK_ROWS, 128), F32),
        in_specs=[vmem, vmem],
        out_specs=vmem,
        scratch_shapes=[pltpu.VMEM((4, HI, LO), BF16)] * 2,
        name="gather",
    )(table, received)


PICK_BLOCK = 1024


def pick_kernel(count_ref, slab_ref, position_ref, back_ref, out_ref, tops, bottoms):
    count = count_ref[0, 0]
    for comp in range(4):
        tile = jnp.concatenate(
            [back_ref[pl.ds(2 * comp + half, OWNERS, stride=BACK_ROWS), :] for half in range(2)], axis=1
        )
        high, low = halves(tile)
        tops[comp * OWNERS : (comp + 1) * OWNERS, :] = high
        bottoms[comp * OWNERS : (comp + 1) * OWNERS, :] = low

    def step(block, carry):
        start = pl.multiple_of(block * PICK_BLOCK, PICK_BLOCK)
        spot = pl.ds(start, PICK_BLOCK)
        lane = lax.broadcasted_iota(I32, (1, PICK_BLOCK), 1) + start
        slab = jnp.where(lane < count, slab_ref[0:1, spot], OWNERS)
        position_hot = one_hot(position_ref[0:1, spot], CAP)
        value = dot_nn(tops[...], position_hot) + dot_nn(bottoms[...], position_hot)
        member = lax.broadcasted_iota(I32, (OWNERS, PICK_BLOCK), 0) == slab
        for comp in range(4):
            piece = value[comp * OWNERS : (comp + 1) * OWNERS, :]
            out_ref[comp, 0:1, spot] = jnp.sum(jnp.where(member, piece, 0.0), axis=0, keepdims=True)
        return carry

    lax.fori_loop(0, PARTS // PICK_BLOCK, step, 0)


def pick(count, slab, position, back):
    vmem = pl.BlockSpec(memory_space=pltpu.VMEM)
    return pl.pallas_call(
        pick_kernel,
        out_shape=jax.ShapeDtypeStruct((4, 1, PARTS), F32),
        in_specs=[pl.BlockSpec(memory_space=pltpu.SMEM), vmem, vmem, vmem],
        out_specs=vmem,
        scratch_shapes=[pltpu.VMEM((4 * OWNERS, CAP), BF16)] * 2,
        name="pick",
    )(count, slab, position, back)


def prior_kernel(solid_ref, drag_ref, rows_ref, first_ref, last_ref):
    for comp in range(4):
        for x in range(CX):
            row = solid_ref[:, x, :] if comp == 0 else drag_ref[comp - 1, :, x, :]
            rows_ref[pl.ds((comp * CX + x) * LAYERS, LAYERS), :] = row
            if x < PRIOR_RIM:
                first_ref[pl.ds((comp * PRIOR_RIM + x) * LAYERS, LAYERS), :] = row
            if x >= CX - PRIOR_RIM:
                spot = (comp * PRIOR_RIM + x - CX + PRIOR_RIM) * LAYERS
                last_ref[pl.ds(spot, LAYERS), :] = row


def prior(solid, drag):
    vmem = pl.BlockSpec(memory_space=pltpu.VMEM)
    edge = jax.ShapeDtypeStruct((4 * PRIOR_RIM * LAYERS, CY), F32)
    return pl.pallas_call(
        prior_kernel,
        out_shape=(jax.ShapeDtypeStruct((4 * CX * LAYERS, CY), F32), edge, edge),
        in_specs=[vmem, vmem],
        out_specs=(vmem, vmem, vmem),
        name="prior",
    )(solid, drag)


def row_list():
    rows = []
    for comp in range(4):
        rows += [(comp, False, x) for x in range(-PRIOR_RIM, CX + PRIOR_RIM)]
        rows += [(comp, True, x) for x in range(-TARGET_RIM, CX + TARGET_RIM)]
    return rows


SIDE_ROWS = -(-len(row_list()) // 16)


def row_piece(refs, row, start, size):
    target, target_above, target_below, prior_rows, prior_above, prior_below = refs
    comp, is_target, x = row
    above, below, rim = (target_above, target_below, TARGET_RIM) if is_target else (prior_above, prior_below, PRIOR_RIM)
    lanes = pl.ds(start, size)
    if x < 0:
        return above[pl.ds((comp * rim + x + rim) * LAYERS, LAYERS), lanes]
    if x >= CX:
        return below[pl.ds((comp * rim + x - CX) * LAYERS, LAYERS), lanes]
    if is_target:
        half = start // LO
        return target[comp, pl.ds((half * CX + x) * LAYERS, LAYERS), pl.ds(start - half * LO, size)]
    return prior_rows[pl.ds((comp * CX + x) * LAYERS, LAYERS), lanes]


def sides_kernel(*refs):
    ins, (left_ref, right_ref) = refs[:6], refs[6:]
    lane = lax.broadcasted_iota(I32, (LAYERS, 128), 1)
    rows = row_list()
    for group in range(SIDE_ROWS):
        left = jnp.zeros((LAYERS, 128), F32)
        right = jnp.zeros((LAYERS, 128), F32)
        for place, row in enumerate(rows[16 * group : 16 * group + 16]):
            here = (lane >= 8 * place) & (lane < 8 * place + 8)
            first = row_piece(ins, row, 0, 128)
            last = row_piece(ins, row, CY - 128, 128)
            left = jnp.where(here, pltpu.roll(first, 8 * place, 1) if place else first, left)
            shift = (8 * place + 8) % 128
            right = jnp.where(here, pltpu.roll(last, shift, 1) if shift else last, right)
        spot = pl.ds(group * LAYERS, LAYERS)
        left_ref[spot, :] = left
        right_ref[spot, :] = right


def sides(*arrays):
    vmem = pl.BlockSpec(memory_space=pltpu.VMEM)
    side = jax.ShapeDtypeStruct((SIDE_ROWS * LAYERS, 128), F32)
    return pl.pallas_call(
        sides_kernel,
        out_shape=(side, side),
        in_specs=[vmem] * 6,
        out_specs=(vmem, vmem),
        name="sides",
    )(*arrays)


WIDE = CY + 128


def relax_kernel(inside_ref, *refs):
    ins, (before_ref, after_ref), (fields_ref, table_ref), (state, source) = refs[:6], refs[6:8], refs[8:10], refs[10:]
    lane = lax.broadcasted_iota(I32, (LAYERS, 128), 1)
    for number, row in enumerate(row_list()):
        comp, is_target, x = row
        group, place = number // 16, number % 16
        spot = pl.ds(group * LAYERS, LAYERS)
        after = after_ref[spot, :]
        before = before_ref[spot, :]
        after = pltpu.roll(after, 128 - 8 * place, 1) if place else after
        shift = (120 - 8 * place) % 128
        before = pltpu.roll(before, shift, 1) if shift else before
        rim = jnp.where(lane < 8, after, jnp.where(lane >= 120, before, 0.0))
        into, at = (source, x + TARGET_RIM) if is_target else (state, x + PRIOR_RIM)
        for half in range(2):
            into[comp, at, :, pl.ds(half * LO, LO)] = row_piece(ins, row, half * LO, LO)
        into[comp, at, :, pl.ds(CY, 128)] = rim

    wide_lane = lax.broadcasted_iota(I32, (LAYERS, WIDE), 1)
    outside = ((wide_lane >= CY + 64) & (inside_ref[2] == 0)) | (
        (wide_lane >= CY) & (wide_lane < CY + 64) & (inside_ref[3] == 0)
    )
    factor = jnp.where(outside, 0.0, 0.2)
    above_factor = jnp.where(inside_ref[0] == 0, 0.0, factor)
    below_factor = jnp.where(inside_ref[1] == 0, 0.0, factor)

    def comp_step(comp, carry):
        for sweep in range(SWEEPS):
            rim = PRIOR_RIM - 1 - sweep
            above = state[comp, PRIOR_RIM - rim - 1]
            here = state[comp, PRIOR_RIM - rim]
            for x in range(-rim, CX + rim):
                below = state[comp, x + 1 + PRIOR_RIM]
                beside = above + below + pltpu.roll(here, 1, 1) + pltpu.roll(here, WIDE - 1, 1)
                scale = above_factor if x < 0 else below_factor if x >= CX else factor
                state[comp, x + PRIOR_RIM] = (source[comp, x + TARGET_RIM] + beside) * scale
                above, here = here, below
        return carry

    lax.fori_loop(0, 4, comp_step, 0)
    for x in range(CX):
        void = 1.0 - state[0, x + PRIOR_RIM, :, 0:CY]
        for comp in range(4):
            value = void if comp == 0 else -state[comp, x + PRIOR_RIM, :, 0:CY] / void
            fields_ref[comp, :, x, :] = value
            for half in range(2):
                table_ref[comp, pl.ds((half * CX + x) * LAYERS, LAYERS), :] = value[:, half * LO : (half + 1) * LO]


def relax(inside, *arrays):
    vmem = pl.BlockSpec(memory_space=pltpu.VMEM)
    return pl.pallas_call(
        relax_kernel,
        out_shape=(
            jax.ShapeDtypeStruct((4, LAYERS, CX, CY), F32),
            jax.ShapeDtypeStruct((4, HI, LO), F32),
        ),
        in_specs=[pl.BlockSpec(memory_space=pltpu.SMEM)] + [vmem] * 8,
        out_specs=(vmem, vmem),
        scratch_shapes=[
            pltpu.VMEM((4, CX + 2 * PRIOR_RIM, LAYERS, WIDE), F32),
            pltpu.VMEM((4, CX + 2 * TARGET_RIM, LAYERS, WIDE), F32),
        ],
        name="relax",
    )(inside, *arrays)


def shifted(array, axis, step):
    count = lax.axis_size(axis)
    pairs = [(i, i + step) for i in range(count) if 0 <= i + step < count]
    return lax.ppermute(array, axis, pairs)


def on_device(part_slab, part_cell, part_volume, part_drag, part_count, prior_solid, prior_drag):
    slab = part_slab.reshape(1, PARTS)
    prior_rows, prior_first, prior_last = prior(prior_solid, prior_drag)
    prior_above = shifted(prior_last, "span", 1)
    prior_below = shifted(prior_first, "span", -1)
    sent, position = pack(part_count, slab, part_cell, part_volume, part_drag)
    received = lax.all_to_all(sent.reshape(OWNERS, 5, 2, 128), "span", 0, 0, tiled=True)
    received = received.reshape(OWNERS * ROWS, 128)
    target, target_first, target_last = deposit(received)
    target_above = shifted(target_last, "span", 1)
    target_below = shifted(target_first, "span", -1)
    arrays = (target, target_above, target_below, prior_rows, prior_above, prior_below)
    side_first, side_last = sides(*arrays)
    before = shifted(side_last, "depth", 1)
    after = shifted(side_first, "depth", -1)
    row, col = lax.axis_index("span"), lax.axis_index("depth")
    inside = jnp.stack(
        [row > 0, row < lax.axis_size("span") - 1, col > 0, col < lax.axis_size("depth") - 1]
    ).astype(I32)
    fields, table = relax(inside, *arrays, before, after)
    returned = gather(table, received)
    back = lax.all_to_all(returned.reshape(OWNERS, BACK_ROWS, 128), "span", 0, 0, tiled=True)
    feedback = pick(part_count, slab, position, back.reshape(OWNERS * BACK_ROWS, 128))
    return fields, feedback


def solution(mesh):
    in_specs = (
        P("depth", "span", None),
        P("depth", "span"),
        P("depth", "span"),
        P(None, "depth", "span"),
        P("depth", "span"),
        P(None, "span", "depth"),
        P(None, None, "span", "depth"),
    )
    out_specs = (P(None, None, "span", "depth"), P(None, "depth", "span"))
    return jax.shard_map(on_device, mesh=mesh, in_specs=in_specs, out_specs=out_specs, check_vma=False)
```

```python
import jax
import jax.numpy as jnp
from jax import lax
from jax.experimental import pallas as pl
from jax.experimental.pallas import tpu as pltpu
from jax.sharding import PartitionSpec as P

F32, BF16, I32 = jnp.float32, jnp.bfloat16, jnp.int32
OWNERS = 64
CAP = 256
LAYERS, CX, CY = 8, 16, 512
PARTS = 8192
HI, LO = 256, 256
ROWS = 2 * 5
BACK_ROWS = 8
SWEEPS = 6
RIM = SWEEPS
SIDE_ROWS = 4 * CX // 16 * LAYERS
PHI_LIMIT = 0.6


def halves(value):
    high = value.astype(BF16)
    return high, (value - high.astype(F32)).astype(BF16)


def spread(row, size):
    n = row.shape[1]
    packed = jnp.broadcast_to(row, (16, n)).astype(BF16)
    return jnp.broadcast_to(packed[None], (size // 16, 16, n)).reshape(size, n)


def index_rows(size, n):
    return lax.broadcasted_iota(I32, (size, n), 0).astype(F32).astype(BF16)


def row_is(row, size):
    return index_rows(size, row.shape[1]) == spread(row, size)


def one_hot(row, size):
    return jnp.where(row_is(row, size), jnp.ones((), BF16), jnp.zeros((), BF16))


def dot_nt(left, right):
    return lax.dot_general(left, right, (((1,), (1,)), ((), ())), preferred_element_type=F32)


def dot_nn(left, right):
    return lax.dot_general(left, right, (((1,), (0,)), ((), ())), preferred_element_type=F32)


def fold_sides(pieces, left_ref, right_ref):
    lane = lax.broadcasted_iota(I32, (LAYERS, 128), 1)
    for group in range(4 * CX // 16):
        left = jnp.zeros((LAYERS, 128), F32)
        right = jnp.zeros((LAYERS, 128), F32)
        for place in range(16):
            first, last = pieces(group * 16 + place)
            here = (lane >= 8 * place) & (lane < 8 * place + 8)
            left = jnp.where(here, pltpu.roll(first, 8 * place, 1) if place else first, left)
            shift = (8 * place + 8) % 128
            right = jnp.where(here, pltpu.roll(last, shift, 1) if shift else last, right)
        left_ref[group * LAYERS : (group + 1) * LAYERS, :] = left
        right_ref[group * LAYERS : (group + 1) * LAYERS, :] = right


def unfold_side(row, before_ref, after_ref):
    lane = lax.broadcasted_iota(I32, (LAYERS, 128), 1)
    group, place = row // 16, row % 16
    after = after_ref[group * LAYERS : (group + 1) * LAYERS, :]
    before = before_ref[group * LAYERS : (group + 1) * LAYERS, :]
    after = pltpu.roll(after, 128 - 8 * place, 1) if place else after
    shift = (120 - 8 * place) % 128
    before = pltpu.roll(before, shift, 1) if shift else before
    return jnp.where(lane < 8, after, jnp.where(lane >= 120, before, 0.0))


PACK_BLOCK = 1024
SUB = 256


def pack_kernel(count_ref, slab_ref, cell_ref, volume_ref, drag_ref, out_ref, position_ref, acc):
    count = count_ref[0, 0]
    acc[...] = jnp.zeros_like(acc)
    before_mask = lax.broadcasted_iota(I32, (SUB, SUB + 128), 0)
    after_mask = lax.broadcasted_iota(I32, (SUB, SUB + 128), 1)
    upper = jnp.where((before_mask < after_mask) | (after_mask >= SUB), 1.0, 0.0).astype(BF16)

    def step(block, offset):
        hots, lefts = [], []
        for sub in range(PACK_BLOCK // SUB):
            start = pl.multiple_of(block * PACK_BLOCK + sub * SUB, SUB)
            spot = pl.ds(start, SUB)
            lane = lax.broadcasted_iota(I32, (1, SUB), 1) + start
            slab = jnp.where(lane < count, slab_ref[0:1, spot], OWNERS).astype(F32)
            member = row_is(slab, OWNERS)
            member_one = jnp.where(member, jnp.ones((), BF16), jnp.zeros((), BF16))
            ranks = dot_nn(member_one, upper)
            place = ranks[:, :SUB] + jnp.concatenate([offset, offset], axis=1)
            position = jnp.sum(place * member_one.astype(F32), axis=0, keepdims=True)
            offset = offset + ranks[:, SUB:]
            position_ref[0:1, spot] = position
            hots.append(one_hot(position, CAP))
            cell = cell_ref[0:1, spot]
            cell_high = lax.shift_right_logical(cell, 8)
            rows = [cell_high.astype(F32), (cell - cell_high * 256).astype(F32)]
            for value in [volume_ref[0:1, spot]] + [drag_ref[k, 0:1, spot] for k in range(3)]:
                high = value.astype(BF16).astype(F32)
                rows += [high, value - high]
            zero = jnp.zeros((), BF16)
            lefts.append(
                jnp.concatenate([jnp.where(member, spread(row, OWNERS), zero) for row in rows], axis=0)
            )
        acc[...] += dot_nt(jnp.concatenate(lefts, axis=1), jnp.concatenate(hots, axis=1))
        return offset

    lax.fori_loop(0, PARTS // PACK_BLOCK, step, jnp.zeros((OWNERS, 128), F32))
    for comp in range(5):
        high = acc[2 * comp * OWNERS : (2 * comp + 1) * OWNERS, :]
        low = acc[(2 * comp + 1) * OWNERS : (2 * comp + 2) * OWNERS, :]
        whole = high * 256.0 + low if comp == 0 else high + low
        for half in range(2):
            out_ref[pl.ds(2 * comp + half, OWNERS, stride=ROWS), :] = whole[:, half * 128 : (half + 1) * 128]


def pack(count, slab, cell, volume, drag):
    vmem = pl.BlockSpec(memory_space=pltpu.VMEM)
    return pl.pallas_call(
        pack_kernel,
        out_shape=(
            jax.ShapeDtypeStruct((OWNERS * ROWS, 128), F32),
            jax.ShapeDtypeStruct((1, PARTS), F32),
        ),
        in_specs=[pl.BlockSpec(memory_space=pltpu.SMEM), vmem, vmem, vmem, vmem],
        out_specs=(vmem, vmem),
        scratch_shapes=[pltpu.VMEM((10 * OWNERS, CAP), F32)],
        name="pack",
    )(count, slab, cell, volume, drag)


SOURCES_AT_ONCE = 4


def cell_split(cell):
    cell = cell.astype(I32)
    layer_x = lax.shift_right_logical(cell, 9)
    layer = lax.shift_right_logical(cell, 13)
    x = layer_x - layer * 16
    y_half = lax.shift_right_logical(cell, 8) - layer_x * 2
    high = (y_half * 16 + x) * 8 + layer
    low = cell - lax.shift_right_logical(cell, 8) * 256
    return high.astype(F32), low.astype(F32)


def source_row(ref, source, comp):
    base = source * ROWS + 2 * comp
    return jnp.concatenate([ref[pl.ds(base, 1), :], ref[pl.ds(base + 1, 1), :]], axis=1)


def deposit_kernel(recv_ref, out_ref, first_ref, last_ref):
    out_ref[...] = jnp.zeros_like(out_ref)
    zero = jnp.zeros((), BF16)

    def step(block, carry):
        lows, members, values = [], [], []
        for sub in range(SOURCES_AT_ONCE):
            source = block * SOURCES_AT_ONCE + sub
            high, low = cell_split(source_row(recv_ref, source, 0))
            lows.append(one_hot(low, LO))
            members.append(row_is(high, HI))
            parts = []
            for comp in range(4):
                value = source_row(recv_ref, source, comp + 1)
                top = value.astype(BF16).astype(F32)
                parts.append((top, value - top))
            values.append(parts)
        right = jnp.concatenate(lows, axis=1)
        right2 = jnp.concatenate([right, right], axis=1)
        for comp in range(4):
            left = [
                jnp.where(members[sub], spread(values[sub][comp][part], HI), zero)
                for part in range(2)
                for sub in range(SOURCES_AT_ONCE)
            ]
            out_ref[comp] += dot_nt(jnp.concatenate(left, axis=1), right2)
        return carry

    lax.fori_loop(0, OWNERS // SOURCES_AT_ONCE, step, 0)
    out_ref[0] = jnp.minimum(out_ref[0], PHI_LIMIT)

    def pieces(row):
        comp, x = row // CX, row % CX
        first = out_ref[comp, x * LAYERS : (x + 1) * LAYERS, 0:128]
        last = out_ref[comp, (CX + x) * LAYERS : (CX + x + 1) * LAYERS, LO - 128 : LO]
        return first, last

    fold_sides(pieces, first_ref, last_ref)


def deposit(received):
    vmem = pl.BlockSpec(memory_space=pltpu.VMEM)
    side = jax.ShapeDtypeStruct((SIDE_ROWS, 128), F32)
    return pl.pallas_call(
        deposit_kernel,
        out_shape=(jax.ShapeDtypeStruct((4, HI, LO), F32), side, side),
        in_specs=[vmem],
        out_specs=(vmem, vmem, vmem),
        name="deposit",
    )(received)


GATHER_SOURCES = 2


def gather_kernel(own_ref, above_ref, below_ref, recv_ref, fields_ref, out_ref, tops, bottoms):
    def smooth(comp, x):
        row = own_ref[pl.ds((comp * CX + x) * LAYERS, LAYERS), :]
        if x < RIM:
            row = row + above_ref[pl.ds((comp * RIM + x) * LAYERS, LAYERS), :]
        if x >= CX - RIM:
            row = row + below_ref[pl.ds((comp * RIM + x - CX + RIM) * LAYERS, LAYERS), :]
        return row

    for pair in range(0, CX, 2):
        void = [1.0 - smooth(0, x) for x in (pair, pair + 1)]
        for comp in range(4):
            rows = void if comp == 0 else [-smooth(comp, x) / v for x, v in zip((pair, pair + 1), void)]
            for x, row in zip((pair, pair + 1), rows):
                fields_ref[comp, :, x, :] = row
            high, low = halves(jnp.concatenate(rows, axis=0))
            for half in range(2):
                spot = pl.ds((half * CX + pair) * LAYERS, 2 * LAYERS)
                tops[comp, spot, :] = high[:, half * LO : (half + 1) * LO]
                bottoms[comp, spot, :] = low[:, half * LO : (half + 1) * LO]

    def step(block, carry):
        highs, lows = [], []
        for sub in range(GATHER_SOURCES):
            high, low = cell_split(source_row(recv_ref, block * GATHER_SOURCES + sub, 0))
            highs.append(high)
            lows.append(one_hot(low, LO))
        low_hot = jnp.concatenate(lows, axis=1)
        high_row = jnp.concatenate(highs, axis=1)
        n = high_row.shape[1]
        member = lax.broadcasted_iota(I32, (HI, n), 0).astype(F32) == high_row
        rows = []
        for comp in range(4):
            value = dot_nn(tops[comp], low_hot) + dot_nn(bottoms[comp], low_hot)
            rows.append(jnp.sum(jnp.where(member, value, 0.0), axis=0, keepdims=True))
        for sub in range(GATHER_SOURCES):
            pieces = [
                row[:, sub * CAP + half * 128 : sub * CAP + (half + 1) * 128] for row in rows for half in range(2)
            ]
            start = pl.multiple_of((block * GATHER_SOURCES + sub) * BACK_ROWS, BACK_ROWS)
            out_ref[pl.ds(start, BACK_ROWS), :] = jnp.concatenate(pieces, axis=0)
        return carry

    lax.fori_loop(0, OWNERS // GATHER_SOURCES, step, 0)


def gather(own, above, below, received):
    vmem = pl.BlockSpec(memory_space=pltpu.VMEM)
    return pl.pallas_call(
        gather_kernel,
        out_shape=(
            jax.ShapeDtypeStruct((4, LAYERS, CX, CY), F32),
            jax.ShapeDtypeStruct((OWNERS * BACK_ROWS, 128), F32),
        ),
        in_specs=[vmem] * 4,
        out_specs=(vmem, vmem),
        scratch_shapes=[pltpu.VMEM((4, HI, LO), BF16)] * 2,
        name="gather",
    )(own, above, below, received)


PICK_BLOCK = 1024


def pick_kernel(count_ref, slab_ref, position_ref, back_ref, out_ref, tops, bottoms):
    count = count_ref[0, 0]
    for comp in range(4):
        tile = jnp.concatenate(
            [back_ref[pl.ds(2 * comp + half, OWNERS, stride=BACK_ROWS), :] for half in range(2)], axis=1
        )
        high, low = halves(tile)
        tops[comp * OWNERS : (comp + 1) * OWNERS, :] = high
        bottoms[comp * OWNERS : (comp + 1) * OWNERS, :] = low

    def step(block, carry):
        start = pl.multiple_of(block * PICK_BLOCK, PICK_BLOCK)
        spot = pl.ds(start, PICK_BLOCK)
        lane = lax.broadcasted_iota(I32, (1, PICK_BLOCK), 1) + start
        slab = jnp.where(lane < count, slab_ref[0:1, spot], OWNERS)
        position_hot = one_hot(position_ref[0:1, spot], CAP)
        value = dot_nn(tops[...], position_hot) + dot_nn(bottoms[...], position_hot)
        member = lax.broadcasted_iota(I32, (OWNERS, PICK_BLOCK), 0) == slab
        for comp in range(4):
            piece = value[comp * OWNERS : (comp + 1) * OWNERS, :]
            out_ref[comp, 0:1, spot] = jnp.sum(jnp.where(member, piece, 0.0), axis=0, keepdims=True)
        return carry

    lax.fori_loop(0, PARTS // PICK_BLOCK, step, 0)


def pick(count, slab, position, back):
    vmem = pl.BlockSpec(memory_space=pltpu.VMEM)
    return pl.pallas_call(
        pick_kernel,
        out_shape=jax.ShapeDtypeStruct((4, 1, PARTS), F32),
        in_specs=[pl.BlockSpec(memory_space=pltpu.SMEM), vmem, vmem, vmem],
        out_specs=vmem,
        scratch_shapes=[pltpu.VMEM((4 * OWNERS, CAP), BF16)] * 2,
        name="pick",
    )(count, slab, position, back)


def prior_row(solid_ref, drag_ref, row):
    comp, x = row // CX, row % CX
    return solid_ref[:, x, :] if comp == 0 else drag_ref[comp - 1, :, x, :]


def prior_kernel(solid_left, drag_left, solid_right, drag_right, first_ref, last_ref):
    def pieces(row):
        return prior_row(solid_left, drag_left, row), prior_row(solid_right, drag_right, row)

    fold_sides(pieces, first_ref, last_ref)


def prior_sides(solid, drag):
    vmem = pl.BlockSpec(memory_space=pltpu.VMEM)
    side = jax.ShapeDtypeStruct((SIDE_ROWS, 128), F32)
    edges = []
    for block in (0, CY // 128 - 1):
        edges.append(pl.BlockSpec((LAYERS, CX, 128), lambda i, block=block: (0, 0, block)))
        edges.append(pl.BlockSpec((3, LAYERS, CX, 128), lambda i, block=block: (0, 0, 0, block)))
    return pl.pallas_call(
        prior_kernel,
        grid=(1,),
        out_shape=(side, side),
        in_specs=edges,
        out_specs=(pl.BlockSpec((SIDE_ROWS, 128), lambda i: (0, 0)),) * 2,
        name="prior_sides",
    )(solid, drag, solid, drag)


WIDE = CY + 128


def relax_kernel(
    inside_ref, target_ref, solid_ref, drag_ref, before, after, prior_before, prior_after,
    own_ref, up_ref, down_ref, state, source,
):
    blank = jnp.zeros((LAYERS, WIDE), F32)
    for comp in range(4):
        for x in range(RIM):
            state[comp, x] = blank
            state[comp, RIM + CX + x] = blank
        for x in range(CX):
            row = comp * CX + x
            for half in range(2):
                spot = pl.ds((half * CX + x) * LAYERS, LAYERS)
                source[comp, x, :, half * LO : (half + 1) * LO] = target_ref[comp, spot, :]
            source[comp, x, :, CY:WIDE] = unfold_side(row, before, after)
            state[comp, RIM + x, :, 0:CY] = prior_row(solid_ref, drag_ref, row)
            state[comp, RIM + x, :, CY:WIDE] = unfold_side(row, prior_before, prior_after)

    lane = lax.broadcasted_iota(I32, (LAYERS, WIDE), 1)
    outside = ((lane >= CY + 64) & (inside_ref[2] == 0)) | (
        (lane >= CY) & (lane < CY + 64) & (inside_ref[3] == 0)
    )
    factor = jnp.where(outside, 0.0, 0.2)
    above_factor = jnp.where(inside_ref[0] == 0, 0.0, factor)
    below_factor = jnp.where(inside_ref[1] == 0, 0.0, factor)

    def comp_step(comp, carry):
        for sweep in range(SWEEPS):
            rim = sweep + 1
            above, here = blank, blank
            for x in range(-rim, CX + rim):
                below = state[comp, x + 1 + RIM] if x + 1 < CX + sweep else blank
                total = above + below
                if -sweep <= x < CX + sweep:
                    total = total + pltpu.roll(here, 1, 1) + pltpu.roll(here, WIDE - 1, 1)
                if 0 <= x < CX:
                    total = total + source[comp, x]
                scale = above_factor if x < 0 else below_factor if x >= CX else factor
                state[comp, x + RIM] = total * scale
                above, here = here, below
        return carry

    lax.fori_loop(0, 4, comp_step, 0)
    for comp in range(4):
        for x in range(CX):
            own_ref[pl.ds((comp * CX + x) * LAYERS, LAYERS), :] = state[comp, RIM + x, :, 0:CY]
        for x in range(RIM):
            spot = pl.ds((comp * RIM + x) * LAYERS, LAYERS)
            up_ref[spot, :] = state[comp, x, :, 0:CY]
            down_ref[spot, :] = state[comp, RIM + CX + x, :, 0:CY]


def relax(inside, *arrays):
    vmem = pl.BlockSpec(memory_space=pltpu.VMEM)
    rim = jax.ShapeDtypeStruct((4 * RIM * LAYERS, CY), F32)
    return pl.pallas_call(
        relax_kernel,
        out_shape=(jax.ShapeDtypeStruct((4 * CX * LAYERS, CY), F32), rim, rim),
        in_specs=[pl.BlockSpec(memory_space=pltpu.SMEM)] + [vmem] * 7,
        out_specs=(vmem, vmem, vmem),
        scratch_shapes=[
            pltpu.VMEM((4, CX + 2 * RIM, LAYERS, WIDE), F32),
            pltpu.VMEM((4, CX, LAYERS, WIDE), F32),
        ],
        name="relax",
    )(inside, *arrays)


def shifted(array, axis, step):
    count = lax.axis_size(axis)
    pairs = [(i, i + step) for i in range(count) if 0 <= i + step < count]
    return lax.ppermute(array, axis, pairs)


def on_device(part_slab, part_cell, part_volume, part_drag, part_count, prior_solid, prior_drag):
    slab = part_slab.reshape(1, PARTS)
    row, col = lax.axis_index("span"), lax.axis_index("depth")
    inside = jnp.stack(
        [row > 0, row < lax.axis_size("span") - 1, col > 0, col < lax.axis_size("depth") - 1]
    ).astype(I32)
    sent, position = pack(part_count, slab, part_cell, part_volume, part_drag)
    received = lax.all_to_all(sent.reshape(OWNERS, 5, 2, 128), "span", 0, 0, tiled=True)
    received = received.reshape(OWNERS * ROWS, 128)
    prior_first, prior_last = prior_sides(prior_solid, prior_drag)
    prior_before = shifted(prior_last, "depth", 1)
    prior_after = shifted(prior_first, "depth", -1)
    target, first, last = deposit(received)
    before = shifted(last, "depth", 1)
    after = shifted(first, "depth", -1)
    own, up, down = relax(
        inside, target, prior_solid, prior_drag, before, after, prior_before, prior_after
    )
    from_above = shifted(down, "span", 1)
    from_below = shifted(up, "span", -1)
    fields, returned = gather(own, from_above, from_below, received)
    back = lax.all_to_all(returned.reshape(OWNERS, BACK_ROWS, 128), "span", 0, 0, tiled=True)
    feedback = pick(part_count, slab, position, back.reshape(OWNERS * BACK_ROWS, 128))
    return fields, feedback


def solution(mesh):
    in_specs = (
        P("depth", "span", None),
        P("depth", "span"),
        P("depth", "span"),
        P(None, "depth", "span"),
        P("depth", "span"),
        P(None, "span", "depth"),
        P(None, None, "span", "depth"),
    )
    out_specs = (P(None, None, "span", "depth"), P(None, "depth", "span"))
    return jax.shard_map(on_device, mesh=mesh, in_specs=in_specs, out_specs=out_specs, check_vma=False)
```

```python
import jax
import jax.numpy as jnp
from jax import lax
from jax.experimental import pallas as pl
from jax.experimental.pallas import tpu as pltpu
from jax.sharding import PartitionSpec as P

F32, BF16, I32 = jnp.float32, jnp.bfloat16, jnp.int32
MIB = 1 << 20
OWNERS = 64
CAP = 256
LAYERS, CX, CY = 8, 16, 512
PARTS = 8192
HI, LO = 256, 256
ROWS = 2 * 5
BACK_ROWS = 8
SWEEPS = 6
RIM = SWEEPS
SIDE_ROWS = 2 * 4 * CX // 16 * LAYERS
PHI_LIMIT = 0.6


def halves(value):
    high = value.astype(BF16)
    return high, (value - high.astype(F32)).astype(BF16)


def spread(row, size):
    n = row.shape[1]
    packed = jnp.broadcast_to(row, (16, n)).astype(BF16)
    return jnp.broadcast_to(packed[None], (size // 16, 16, n)).reshape(size, n)


def index_rows(size, n):
    return lax.broadcasted_iota(I32, (size, n), 0).astype(F32).astype(BF16)


def row_is(row, size):
    return index_rows(size, row.shape[1]) == spread(row, size)


def one_hot(row, size):
    return jnp.where(row_is(row, size), jnp.ones((), BF16), jnp.zeros((), BF16))


def dot_nt(left, right):
    return lax.dot_general(left, right, (((1,), (1,)), ((), ())), preferred_element_type=F32)


def dot_nn(left, right):
    return lax.dot_general(left, right, (((1,), (0,)), ((), ())), preferred_element_type=F32)


def at_edge(axis):
    place = lax.axis_index(axis)
    return place == 0, place == lax.axis_size(axis) - 1


def fold_sides(pieces, left_ref, right_ref):
    lane = lax.broadcasted_iota(I32, (LAYERS, 128), 1)
    for group in range(SIDE_ROWS // LAYERS):
        left = jnp.zeros((LAYERS, 128), F32)
        right = jnp.zeros((LAYERS, 128), F32)
        for place in range(16):
            first, last = pieces(group * 16 + place)
            here = (lane >= 8 * place) & (lane < 8 * place + 8)
            left = jnp.where(here, pltpu.roll(first, 8 * place, 1) if place else first, left)
            shift = (8 * place + 8) % 128
            right = jnp.where(here, pltpu.roll(last, shift, 1) if shift else last, right)
        left_ref[group * LAYERS : (group + 1) * LAYERS, :] = left
        right_ref[group * LAYERS : (group + 1) * LAYERS, :] = right


def unfold_side(row, before_ref, after_ref, is_before, is_after):
    group, place = row // 16, row % 16
    after = after_ref[group * LAYERS : (group + 1) * LAYERS, :]
    before = before_ref[group * LAYERS : (group + 1) * LAYERS, :]
    after = pltpu.roll(after, 128 - 8 * place, 1) if place else after
    shift = (120 - 8 * place) % 128
    before = pltpu.roll(before, shift, 1) if shift else before
    return jnp.where(is_after, after, jnp.where(is_before, before, 0.0))


def prior_row(solid_ref, drag_ref, row, lanes):
    comp, x = row // CX, row % CX
    return solid_ref[:, x, lanes] if comp == 0 else drag_ref[comp - 1, :, x, lanes]


PACK_BLOCK = 1024
SUB = 256


def pack_kernel(count_ref, slab_ref, cell_ref, volume_ref, drag_ref, out_ref, position_ref, acc):
    count = count_ref[0, 0]
    acc[...] = jnp.zeros_like(acc)
    before_mask = lax.broadcasted_iota(I32, (SUB, SUB + 128), 0)
    after_mask = lax.broadcasted_iota(I32, (SUB, SUB + 128), 1)
    upper = jnp.where((before_mask < after_mask) | (after_mask >= SUB), 1.0, 0.0).astype(BF16)

    def step(block, offset):
        hots, lefts = [], []
        for sub in range(PACK_BLOCK // SUB):
            start = pl.multiple_of(block * PACK_BLOCK + sub * SUB, SUB)
            spot = pl.ds(start, SUB)
            lane = lax.broadcasted_iota(I32, (1, SUB), 1) + start
            slab = jnp.where(lane < count, slab_ref[0:1, spot], OWNERS).astype(F32)
            member = row_is(slab, OWNERS)
            member_one = jnp.where(member, jnp.ones((), BF16), jnp.zeros((), BF16))
            ranks = dot_nn(member_one, upper)
            place = ranks[:, :SUB] + jnp.concatenate([offset, offset], axis=1)
            position = jnp.sum(place * member_one.astype(F32), axis=0, keepdims=True)
            offset = offset + ranks[:, SUB:]
            position_ref[0:1, spot] = position
            hots.append(one_hot(position, CAP))
            cell = cell_ref[0:1, spot]
            cell_high = lax.shift_right_logical(cell, 8)
            rows = [cell_high.astype(F32), (cell - cell_high * 256).astype(F32)]
            for value in [volume_ref[0:1, spot]] + [drag_ref[k, 0:1, spot] for k in range(3)]:
                high = value.astype(BF16).astype(F32)
                rows += [high, value - high]
            zero = jnp.zeros((), BF16)
            lefts.append(
                jnp.concatenate([jnp.where(member, spread(row, OWNERS), zero) for row in rows], axis=0)
            )
        acc[...] += dot_nt(jnp.concatenate(lefts, axis=1), jnp.concatenate(hots, axis=1))
        return offset

    lax.fori_loop(0, PARTS // PACK_BLOCK, step, jnp.zeros((OWNERS, 128), F32))
    for comp in range(5):
        high = acc[2 * comp * OWNERS : (2 * comp + 1) * OWNERS, :]
        low = acc[(2 * comp + 1) * OWNERS : (2 * comp + 2) * OWNERS, :]
        whole = high * 256.0 + low if comp == 0 else high + low
        for half in range(2):
            out_ref[pl.ds(2 * comp + half, OWNERS, stride=ROWS), :] = whole[:, half * 128 : (half + 1) * 128]


def pack(count, slab, cell, volume, drag):
    vmem = pl.BlockSpec(memory_space=pltpu.VMEM)
    return pl.pallas_call(
        pack_kernel,
        out_shape=(
            jax.ShapeDtypeStruct((OWNERS * ROWS, 128), F32),
            jax.ShapeDtypeStruct((1, PARTS), F32),
        ),
        in_specs=[pl.BlockSpec(memory_space=pltpu.SMEM), vmem, vmem, vmem, vmem],
        out_specs=(vmem, vmem),
        scratch_shapes=[pltpu.VMEM((10 * OWNERS, CAP), F32)],
        name="pack",
        compiler_params=pltpu.CompilerParams(vmem_limit_bytes=8 * MIB),
    )(count, slab, cell, volume, drag)


SOURCES_AT_ONCE = 4


def cell_split(cell):
    cell = cell.astype(I32)
    layer_x = lax.shift_right_logical(cell, 9)
    layer = lax.shift_right_logical(cell, 13)
    x = layer_x - layer * 16
    y_half = lax.shift_right_logical(cell, 8) - layer_x * 2
    high = (y_half * 16 + x) * 8 + layer
    low = cell - lax.shift_right_logical(cell, 8) * 256
    return high.astype(F32), low.astype(F32)


def source_row(ref, source, comp):
    base = source * ROWS + 2 * comp
    return jnp.concatenate([ref[pl.ds(base, 1), :], ref[pl.ds(base + 1, 1), :]], axis=1)


def deposit_kernel(recv_ref, solid_ref, drag_ref, out_ref, first_ref, last_ref):
    out_ref[...] = jnp.zeros_like(out_ref)
    zero = jnp.zeros((), BF16)

    def step(block, carry):
        lows, members, values = [], [], []
        for sub in range(SOURCES_AT_ONCE):
            source = block * SOURCES_AT_ONCE + sub
            high, low = cell_split(source_row(recv_ref, source, 0))
            lows.append(one_hot(low, LO))
            members.append(row_is(high, HI))
            parts = []
            for comp in range(4):
                value = source_row(recv_ref, source, comp + 1)
                top = value.astype(BF16).astype(F32)
                parts.append((top, value - top))
            values.append(parts)
        right = jnp.concatenate(lows, axis=1)
        right2 = jnp.concatenate([right, right], axis=1)
        for comp in range(4):
            left = [
                jnp.where(members[sub], spread(values[sub][comp][part], HI), zero)
                for part in range(2)
                for sub in range(SOURCES_AT_ONCE)
            ]
            out_ref[comp] += dot_nt(jnp.concatenate(left, axis=1), right2)
        return carry

    lax.fori_loop(0, OWNERS // SOURCES_AT_ONCE, step, 0)
    out_ref[0] = jnp.minimum(out_ref[0], PHI_LIMIT)

    def pieces(row):
        if row >= 4 * CX:
            row -= 4 * CX
            return tuple(prior_row(solid_ref, drag_ref, row, pl.ds(at, 128)) for at in (0, CY - 128))
        comp, x = row // CX, row % CX
        first = out_ref[comp, x * LAYERS : (x + 1) * LAYERS, 0:128]
        last = out_ref[comp, (CX + x) * LAYERS : (CX + x + 1) * LAYERS, LO - 128 : LO]
        return first, last

    fold_sides(pieces, first_ref, last_ref)


def deposit(received, solid, drag):
    vmem = pl.BlockSpec(memory_space=pltpu.VMEM)
    side = jax.ShapeDtypeStruct((SIDE_ROWS, 128), F32)
    return pl.pallas_call(
        deposit_kernel,
        out_shape=(jax.ShapeDtypeStruct((4, HI, LO), F32), side, side),
        in_specs=[vmem] * 3,
        out_specs=(vmem, vmem, vmem),
        name="deposit",
        compiler_params=pltpu.CompilerParams(vmem_limit_bytes=12 * MIB),
    )(received, solid, drag)


GATHER_SOURCES = 2


def gather_kernel(own_ref, above_ref, below_ref, recv_ref, fields_ref, out_ref, tops, bottoms):
    top, bottom = at_edge("span")

    def smooth(comp, x):
        row = own_ref[pl.ds((comp * CX + x) * LAYERS, LAYERS), :]
        if x < RIM:
            row = row + jnp.where(top, 0.0, above_ref[pl.ds((comp * RIM + x) * LAYERS, LAYERS), :])
        if x >= CX - RIM:
            row = row + jnp.where(bottom, 0.0, below_ref[pl.ds((comp * RIM + x - CX + RIM) * LAYERS, LAYERS), :])
        return row

    for pair in range(0, CX, 2):
        void = [1.0 - smooth(0, x) for x in (pair, pair + 1)]
        for comp in range(4):
            rows = void if comp == 0 else [-smooth(comp, x) / v for x, v in zip((pair, pair + 1), void)]
            for x, row in zip((pair, pair + 1), rows):
                fields_ref[comp, :, x, :] = row
            high, low = halves(jnp.concatenate(rows, axis=0))
            for half in range(2):
                spot = pl.ds((half * CX + pair) * LAYERS, 2 * LAYERS)
                tops[comp, spot, :] = high[:, half * LO : (half + 1) * LO]
                bottoms[comp, spot, :] = low[:, half * LO : (half + 1) * LO]

    def step(block, carry):
        highs, lows = [], []
        for sub in range(GATHER_SOURCES):
            high, low = cell_split(source_row(recv_ref, block * GATHER_SOURCES + sub, 0))
            highs.append(high)
            lows.append(one_hot(low, LO))
        low_hot = jnp.concatenate(lows, axis=1)
        high_row = jnp.concatenate(highs, axis=1)
        n = high_row.shape[1]
        member = lax.broadcasted_iota(I32, (HI, n), 0).astype(F32) == high_row
        rows = []
        for comp in range(4):
            value = dot_nn(tops[comp], low_hot) + dot_nn(bottoms[comp], low_hot)
            rows.append(jnp.sum(jnp.where(member, value, 0.0), axis=0, keepdims=True))
        for sub in range(GATHER_SOURCES):
            pieces = [
                row[:, sub * CAP + half * 128 : sub * CAP + (half + 1) * 128] for row in rows for half in range(2)
            ]
            start = pl.multiple_of((block * GATHER_SOURCES + sub) * BACK_ROWS, BACK_ROWS)
            out_ref[pl.ds(start, BACK_ROWS), :] = jnp.concatenate(pieces, axis=0)
        return carry

    lax.fori_loop(0, OWNERS // GATHER_SOURCES, step, 0)


def gather(own, above, below, received):
    vmem = pl.BlockSpec(memory_space=pltpu.VMEM)
    return pl.pallas_call(
        gather_kernel,
        out_shape=(
            jax.ShapeDtypeStruct((4, LAYERS, CX, CY), F32),
            jax.ShapeDtypeStruct((OWNERS * BACK_ROWS, 128), F32),
        ),
        in_specs=[vmem] * 4,
        out_specs=(vmem, vmem),
        scratch_shapes=[pltpu.VMEM((4, HI, LO), BF16)] * 2,
        name="gather",
        compiler_params=pltpu.CompilerParams(vmem_limit_bytes=16 * MIB),
    )(own, above, below, received)


PICK_BLOCK = 1024


def pick_kernel(count_ref, slab_ref, position_ref, back_ref, out_ref, tops, bottoms):
    count = count_ref[0, 0]
    for comp in range(4):
        tile = jnp.concatenate(
            [back_ref[pl.ds(2 * comp + half, OWNERS, stride=BACK_ROWS), :] for half in range(2)], axis=1
        )
        high, low = halves(tile)
        tops[comp * OWNERS : (comp + 1) * OWNERS, :] = high
        bottoms[comp * OWNERS : (comp + 1) * OWNERS, :] = low

    def step(block, carry):
        start = pl.multiple_of(block * PICK_BLOCK, PICK_BLOCK)
        spot = pl.ds(start, PICK_BLOCK)
        lane = lax.broadcasted_iota(I32, (1, PICK_BLOCK), 1) + start
        slab = jnp.where(lane < count, slab_ref[0:1, spot], OWNERS)
        position_hot = one_hot(position_ref[0:1, spot], CAP)
        value = dot_nn(tops[...], position_hot) + dot_nn(bottoms[...], position_hot)
        member = lax.broadcasted_iota(I32, (OWNERS, PICK_BLOCK), 0) == slab
        for comp in range(4):
            piece = value[comp * OWNERS : (comp + 1) * OWNERS, :]
            out_ref[comp, 0:1, spot] = jnp.sum(jnp.where(member, piece, 0.0), axis=0, keepdims=True)
        return carry

    lax.fori_loop(0, PARTS // PICK_BLOCK, step, 0)


def pick(count, slab, position, back):
    vmem = pl.BlockSpec(memory_space=pltpu.VMEM)
    return pl.pallas_call(
        pick_kernel,
        out_shape=jax.ShapeDtypeStruct((4, 1, PARTS), F32),
        in_specs=[pl.BlockSpec(memory_space=pltpu.SMEM), vmem, vmem, vmem],
        out_specs=vmem,
        scratch_shapes=[pltpu.VMEM((4 * OWNERS, CAP), BF16)] * 2,
        name="pick",
        compiler_params=pltpu.CompilerParams(vmem_limit_bytes=8 * MIB),
    )(count, slab, position, back)


WIDE = CY + 128


def relax_kernel(
    target_ref, solid_ref, drag_ref, before, after, own_ref, up_ref, down_ref, state, source
):
    top, bottom = at_edge("span")
    first, last = at_edge("depth")
    near = lax.broadcasted_iota(I32, (LAYERS, 128), 1)
    is_before = (near >= 120) & jnp.logical_not(first)
    is_after = (near < 8) & jnp.logical_not(last)
    blank = jnp.zeros((LAYERS, WIDE), F32)
    for comp in range(4):
        for x in range(RIM):
            state[comp, x] = blank
            state[comp, RIM + CX + x] = blank
        for x in range(CX):
            row = comp * CX + x
            for half in range(2):
                spot = pl.ds((half * CX + x) * LAYERS, LAYERS)
                source[comp, x, :, half * LO : (half + 1) * LO] = target_ref[comp, spot, :]
            source[comp, x, :, CY:WIDE] = unfold_side(row, before, after, is_before, is_after)
            state[comp, RIM + x, :, 0:CY] = prior_row(solid_ref, drag_ref, row, slice(None))
            state[comp, RIM + x, :, CY:WIDE] = unfold_side(4 * CX + row, before, after, is_before, is_after)

    lane = lax.broadcasted_iota(I32, (LAYERS, WIDE), 1)
    outside = ((lane >= CY + 64) & first) | ((lane >= CY) & (lane < CY + 64) & last)
    factor = jnp.where(outside, 0.0, 0.2)
    above_factor = jnp.where(top, 0.0, factor)
    below_factor = jnp.where(bottom, 0.0, factor)

    def comp_step(comp, carry):
        for sweep in range(SWEEPS):
            rim = sweep + 1
            above, here = blank, blank
            for x in range(-rim, CX + rim):
                below = state[comp, x + 1 + RIM] if x + 1 < CX + sweep else blank
                total = above + below
                if -sweep <= x < CX + sweep:
                    total = total + pltpu.roll(here, 1, 1) + pltpu.roll(here, WIDE - 1, 1)
                if 0 <= x < CX:
                    total = total + source[comp, x]
                scale = above_factor if x < 0 else below_factor if x >= CX else factor
                state[comp, x + RIM] = total * scale
                above, here = here, below
        return carry

    lax.fori_loop(0, 4, comp_step, 0)
    for comp in range(4):
        for x in range(CX):
            own_ref[pl.ds((comp * CX + x) * LAYERS, LAYERS), :] = state[comp, RIM + x, :, 0:CY]
        for x in range(RIM):
            spot = pl.ds((comp * RIM + x) * LAYERS, LAYERS)
            up_ref[spot, :] = state[comp, x, :, 0:CY]
            down_ref[spot, :] = state[comp, RIM + CX + x, :, 0:CY]


def relax(*arrays):
    vmem = pl.BlockSpec(memory_space=pltpu.VMEM)
    rim = jax.ShapeDtypeStruct((4 * RIM * LAYERS, CY), F32)
    return pl.pallas_call(
        relax_kernel,
        out_shape=(jax.ShapeDtypeStruct((4 * CX * LAYERS, CY), F32), rim, rim),
        in_specs=[vmem] * 5,
        out_specs=(vmem, vmem, vmem),
        scratch_shapes=[
            pltpu.VMEM((4, CX + 2 * RIM, LAYERS, WIDE), F32),
            pltpu.VMEM((4, CX, LAYERS, WIDE), F32),
        ],
        name="relax",
        compiler_params=pltpu.CompilerParams(vmem_limit_bytes=16 * MIB),
    )(*arrays)


def shifted(array, axis, step):
    count = lax.axis_size(axis)
    return lax.ppermute(array, axis, [(i, (i + step) % count) for i in range(count)])


def on_device(part_slab, part_cell, part_volume, part_drag, part_count, prior_solid, prior_drag):
    slab = part_slab.reshape(1, PARTS)
    sent, position = pack(part_count, slab, part_cell, part_volume, part_drag)
    received = lax.all_to_all(sent.reshape(OWNERS, 5, 2, 128), "span", 0, 0, tiled=True)
    received = received.reshape(OWNERS * ROWS, 128)
    target, first, last = deposit(received, prior_solid, prior_drag)
    before = shifted(last, "depth", 1)
    after = shifted(first, "depth", -1)
    own, up, down = relax(target, prior_solid, prior_drag, before, after)
    from_above = shifted(down, "span", 1)
    from_below = shifted(up, "span", -1)
    fields, returned = gather(own, from_above, from_below, received)
    back = lax.all_to_all(returned.reshape(OWNERS, BACK_ROWS, 128), "span", 0, 0, tiled=True)
    feedback = pick(part_count, slab, position, back.reshape(OWNERS * BACK_ROWS, 128))
    return fields, feedback


def solution(mesh):
    in_specs = (
        P("depth", "span", None),
        P("depth", "span"),
        P("depth", "span"),
        P(None, "depth", "span"),
        P("depth", "span"),
        P(None, "span", "depth"),
        P(None, None, "span", "depth"),
    )
    out_specs = (P(None, None, "span", "depth"), P(None, "depth", "span"))
    return jax.shard_map(on_device, mesh=mesh, in_specs=in_specs, out_specs=out_specs, check_vma=False)
```

```python
import jax
import jax.numpy as jnp
from jax import lax
from jax.experimental import pallas as pl
from jax.experimental.pallas import tpu as pltpu
from jax.sharding import PartitionSpec as P

F32, BF16, I32 = jnp.float32, jnp.bfloat16, jnp.int32
MIB = 1 << 20
OWNERS = 64
CAP = 256
LAYERS, CX, CY = 8, 16, 512
PARTS = 8192
HI, LO = 256, 256
ROWS = 2 * 5
BACK_ROWS = 8
SWEEPS = 6
RIM = SWEEPS
SIDE_ROWS = 2 * 4 * CX // 16 * LAYERS
PHI_LIMIT = 0.6


def halves(value):
    high = value.astype(BF16)
    return high, (value - high.astype(F32)).astype(BF16)


def spread(row, size):
    n = row.shape[1]
    packed = jnp.broadcast_to(row, (16, n)).astype(BF16)
    return jnp.broadcast_to(packed[None], (size // 16, 16, n)).reshape(size, n)


def index_rows(size, n):
    return lax.broadcasted_iota(I32, (size, n), 0).astype(F32).astype(BF16)


def row_is(row, size):
    return index_rows(size, row.shape[1]) == spread(row, size)


def one_hot(row, size):
    return jnp.where(row_is(row, size), jnp.ones((), BF16), jnp.zeros((), BF16))


def dot_nt(left, right):
    return lax.dot_general(left, right, (((1,), (1,)), ((), ())), preferred_element_type=F32)


def dot_nn(left, right):
    return lax.dot_general(left, right, (((1,), (0,)), ((), ())), preferred_element_type=F32)


def at_edge(axis):
    place = lax.axis_index(axis)
    return place == 0, place == lax.axis_size(axis) - 1


def fold_sides(pieces, left_ref, right_ref):
    lane = lax.broadcasted_iota(I32, (LAYERS, 128), 1)
    for group in range(SIDE_ROWS // LAYERS):
        left = jnp.zeros((LAYERS, 128), F32)
        right = jnp.zeros((LAYERS, 128), F32)
        for place in range(16):
            first, last = pieces(group * 16 + place)
            here = (lane >= 8 * place) & (lane < 8 * place + 8)
            left = jnp.where(here, pltpu.roll(first, 8 * place, 1) if place else first, left)
            shift = (8 * place + 8) % 128
            right = jnp.where(here, pltpu.roll(last, shift, 1) if shift else last, right)
        left_ref[group * LAYERS : (group + 1) * LAYERS, :] = left
        right_ref[group * LAYERS : (group + 1) * LAYERS, :] = right


def unfold_side(row, before_ref, after_ref, is_before, is_after):
    group, place = row // 16, row % 16
    after = after_ref[group * LAYERS : (group + 1) * LAYERS, :]
    before = before_ref[group * LAYERS : (group + 1) * LAYERS, :]
    after = pltpu.roll(after, 128 - 8 * place, 1) if place else after
    shift = (120 - 8 * place) % 128
    before = pltpu.roll(before, shift, 1) if shift else before
    return jnp.where(is_after, after, jnp.where(is_before, before, 0.0))


def prior_row(solid_ref, drag_ref, row, lanes):
    comp, x = row // CX, row % CX
    return solid_ref[:, x, lanes] if comp == 0 else drag_ref[comp - 1, :, x, lanes]


PACK_BLOCK = 1024
SUB = 256
CLASSES = 4


def pack_kernel(
    count_ref, slab_any, cell_any, volume_any, drag_any, out_ref, position_ref,
    slab_ref, cell_ref, volume_ref, drag_ref, acc, sems,
):
    sources, targets = (slab_any, cell_any, volume_any, drag_any), (slab_ref, cell_ref, volume_ref, drag_ref)
    copies = [pltpu.make_async_copy(f, t, sems.at[i]) for i, (f, t) in enumerate(zip(sources, targets))]
    for copy in copies:
        copy.start()
    count = count_ref[0, 0]
    acc[...] = jnp.zeros_like(acc)
    earlier = lax.broadcasted_iota(I32, (SUB, SUB), 0)
    later = lax.broadcasted_iota(I32, (SUB, SUB), 1)
    upper = jnp.where(earlier <= later, 1.0, 0.0).astype(BF16)
    for copy in copies:
        copy.wait()

    def live_slab(start, size):
        lane = lax.broadcasted_iota(I32, (1, size), 1) + start
        return jnp.where(lane < count, slab_ref[0:1, pl.ds(start, size)], CLASSES * OWNERS)

    def classes(start, size):
        return lax.shift_right_logical(cell_ref[0:1, pl.ds(start, size)], 14)

    def count_step(block, counts):
        start = pl.multiple_of(block * PACK_BLOCK, PACK_BLOCK)
        member = one_hot(live_slab(start, PACK_BLOCK).astype(F32), OWNERS)
        kind = one_hot(classes(start, PACK_BLOCK).astype(F32), 128)
        return counts + dot_nt(member, kind)

    counts = lax.fori_loop(0, PARTS // PACK_BLOCK, count_step, jnp.zeros((OWNERS, 128), F32))
    numbers = [jnp.broadcast_to(counts[:, kind : kind + 1], (OWNERS, 128)) for kind in range(CLASSES)]
    starts, end = [], jnp.zeros((OWNERS, 128), F32)
    for kind in range(CLASSES):
        rest = sum(numbers[kind:])
        starts.append(jnp.maximum(end, jnp.minimum(float(kind * CAP // CLASSES), CAP - rest)))
        end = starts[-1] + numbers[kind]

    def step(block, offset):
        hots, lefts = [], []
        for sub in range(PACK_BLOCK // SUB):
            start = pl.multiple_of(block * PACK_BLOCK + sub * SUB, SUB)
            spot = pl.ds(start, SUB)
            slab = live_slab(start, SUB)
            member = row_is(slab.astype(F32), OWNERS)
            sorted_one = one_hot((slab + classes(start, SUB) * OWNERS).astype(F32), CLASSES * OWNERS)
            ranks = dot_nn(sorted_one, upper)
            place = ranks + jnp.concatenate([offset, offset], axis=1)
            position = jnp.sum(place * sorted_one.astype(F32), axis=0, keepdims=True) - 1.0
            offset = offset + jnp.broadcast_to(ranks[:, SUB - 1 : SUB], offset.shape)
            position_ref[0:1, spot] = position
            hots.append(one_hot(position, CAP))
            cell = cell_ref[0:1, spot]
            cell_high = lax.shift_right_logical(cell, 8)
            rows = [cell_high.astype(F32), (cell - cell_high * 256).astype(F32)]
            for value in [volume_ref[0:1, spot]] + [drag_ref[k, 0:1, spot] for k in range(3)]:
                high = value.astype(BF16).astype(F32)
                rows += [high, value - high]
            zero = jnp.zeros((), BF16)
            lefts.append(
                jnp.concatenate([jnp.where(member, spread(row, OWNERS), zero) for row in rows], axis=0)
            )
        acc[...] += dot_nt(jnp.concatenate(lefts, axis=1), jnp.concatenate(hots, axis=1))
        return offset

    lax.fori_loop(0, PARTS // PACK_BLOCK, step, jnp.concatenate(starts, axis=0))
    for comp in range(5):
        high = acc[2 * comp * OWNERS : (2 * comp + 1) * OWNERS, :]
        low = acc[(2 * comp + 1) * OWNERS : (2 * comp + 2) * OWNERS, :]
        whole = high * 256.0 + low if comp == 0 else high + low
        for half in range(2):
            out_ref[pl.ds(2 * comp + half, OWNERS, stride=ROWS), :] = whole[:, half * 128 : (half + 1) * 128]


def pack(count, slab, cell, volume, drag):
    vmem = pl.BlockSpec(memory_space=pltpu.VMEM)
    hbm = pl.BlockSpec(memory_space=pltpu.HBM)
    return pl.pallas_call(
        pack_kernel,
        out_shape=(
            jax.ShapeDtypeStruct((OWNERS * ROWS, 128), F32),
            jax.ShapeDtypeStruct((1, PARTS), F32),
        ),
        in_specs=[pl.BlockSpec(memory_space=pltpu.SMEM), hbm, hbm, hbm, hbm],
        out_specs=(vmem, vmem),
        scratch_shapes=[
            pltpu.VMEM((1, PARTS), I32),
            pltpu.VMEM((1, PARTS), I32),
            pltpu.VMEM((1, PARTS), F32),
            pltpu.VMEM((3, 1, PARTS), F32),
            pltpu.VMEM((10 * OWNERS, CAP), F32),
            pltpu.SemaphoreType.DMA((4,)),
        ],
        compiler_params=pltpu.CompilerParams(vmem_limit_bytes=8 * MIB),
        name="pack",
    )(count, slab, cell, volume, drag)


CHUNKS, CHUNK = 16, 1024
CLASS_HIGH = 64
TABLE_ROWS = 4 * HI


def target_row(comp, side, block):
    return (comp * 2 + side) * HI + block * LAYERS


def swap_halves(first, second):
    lane = lax.broadcasted_iota(I32, (8, 128), 1)
    return (
        jnp.where(lane < 64, first, pltpu.roll(second, 64, 1)),
        jnp.where(lane < 64, pltpu.roll(first, 64, 1), second),
    )


def fill_low_hot(low_hot, low_ref, chunk):
    for r in range(8):
        low_hot[:, r * 128 : (r + 1) * 128] = one_hot(low_ref[chunk, r : r + 1, :], LO)


def deposit_kernel(
    recv_ref, solid_any, drag_any,
    out_ref, first_ref, last_ref, prior_ref, high_ref, low_ref, bounds_ref,
    solid_ref, drag_ref, values, acc, low_hot, left, spreads, sems,
):
    copies = [
        pltpu.make_async_copy(solid_any, solid_ref, sems.at[0]),
        pltpu.make_async_copy(drag_any, drag_ref, sems.at[1]),
    ]
    for copy in copies:
        copy.start()
    acc[...] = jnp.zeros_like(acc)
    zero = jnp.zeros((), BF16)

    def chunked(comp):
        tile = jnp.concatenate([recv_ref[pl.ds(2 * comp + half, OWNERS, stride=ROWS), :] for half in range(2)], axis=0)
        slots = jnp.transpose(tile)
        pairs = [swap_halves(slots[16 * m : 16 * m + 8], slots[16 * m + 8 : 16 * m + 16]) for m in range(8)]
        return [pair[0] for pair in pairs] + [pair[1] for pair in pairs]

    volumes = chunked(1)
    for chunk, cell in enumerate(chunked(0)):
        cell = cell.astype(I32)
        layer = lax.shift_right_logical(cell, 13)
        layer_x = lax.shift_right_logical(cell, 9)
        layer_xy = lax.shift_right_logical(cell, 8)
        high = layer * 32 + (layer_xy - layer_x * 2) * 16 + layer_x - layer * 16
        high_ref[chunk] = high.astype(F32)
        low_ref[chunk] = (cell - layer_xy * 256).astype(F32)
        values[0, chunk] = volumes[chunk]
        live = volumes[chunk] > 0.0
        kind = lax.shift_right_logical(layer, 1).astype(F32)
        bounds_ref[chunk, 0] = jnp.min(jnp.where(live, kind, float(CLASSES))).astype(I32)
        bounds_ref[chunk, 1] = jnp.max(jnp.where(live, kind, -1.0)).astype(I32) + 1
    for comp in range(1, 4):
        for chunk, value in enumerate(chunked(comp + 1)):
            values[comp, chunk] = value

    def step(chunk, carry):
        fill_low_hot(low_hot, low_ref, chunk)
        for comp in range(4):
            value = values[comp, chunk]
            top = value.astype(BF16).astype(F32)
            for part, piece in enumerate((top, value - top)):
                for r in range(8):
                    row = jnp.broadcast_to(piece[r : r + 1], (16, 128)).astype(BF16)
                    spreads[comp, :, part * CHUNK + r * 128 : part * CHUNK + (r + 1) * 128] = row

        def class_step(kind, carry):
            key = high_ref[chunk] - (kind * CLASS_HIGH).astype(F32)
            for r in range(8):
                member = row_is(key[r : r + 1], CLASS_HIGH)
                for comp in range(4):
                    for part in range(2):
                        lanes = slice(part * CHUNK + r * 128, part * CHUNK + (r + 1) * 128)
                        value = spreads[comp, :, lanes]
                        value = jnp.broadcast_to(value[None], (CLASS_HIGH // 16, 16, 128)).reshape(CLASS_HIGH, 128)
                        picked = jnp.where(member, value, zero)
                        for layer in range(2):
                            left[pl.ds(layer * 128 + comp * 32, 32), lanes] = picked[layer * 32 : layer * 32 + 32]
            spot = pl.ds(pl.multiple_of(kind * 256, 256), 256)
            acc[spot, :] += dot_nt(left[:, 0:CHUNK], low_hot[...]) + dot_nt(left[:, CHUNK : 2 * CHUNK], low_hot[...])
            return carry

        lax.fori_loop(bounds_ref[chunk, 0], bounds_ref[chunk, 1], class_step, 0)
        return carry

    lax.fori_loop(0, CHUNKS, step, 0)
    for copy in copies:
        copy.wait()
    for comp in range(4):
        for layer in range(LAYERS):
            rows = acc[pl.ds(layer * 128 + comp * 32, 32), :]
            if comp == 0:
                rows = jnp.minimum(rows, PHI_LIMIT)
            for side in range(2):
                spot = pl.ds(target_row(comp, side, 0) + layer, 32, stride=LAYERS)
                out_ref[spot, :] = rows[:, side * 128 : (side + 1) * 128]
        for x in range(CX):
            row = comp * CX + x
            prior_ref[row * LAYERS : (row + 1) * LAYERS, :] = prior_row(solid_ref, drag_ref, row, slice(None))

    def pieces(row):
        if row >= 4 * CX:
            row -= 4 * CX
            spot = slice(row * LAYERS, (row + 1) * LAYERS)
            return prior_ref[spot, 0:128], prior_ref[spot, CY - 128 : CY]
        comp, x = row // CX, row % CX
        at = target_row(comp, 0, x), target_row(comp, 1, CX + x)
        return out_ref[at[0] : at[0] + LAYERS, :], out_ref[at[1] : at[1] + LAYERS, :]

    fold_sides(pieces, first_ref, last_ref)


def deposit(received, solid, drag):
    vmem = pl.BlockSpec(memory_space=pltpu.VMEM)
    hbm = pl.BlockSpec(memory_space=pltpu.HBM)
    side = jax.ShapeDtypeStruct((SIDE_ROWS, 128), F32)
    index = jax.ShapeDtypeStruct((CHUNKS, 8, 128), F32)
    return pl.pallas_call(
        deposit_kernel,
        out_shape=(
            jax.ShapeDtypeStruct((4 * 2 * HI, 128), F32),
            side,
            side,
            jax.ShapeDtypeStruct((4 * CX * LAYERS, CY), F32),
            index,
            index,
            jax.ShapeDtypeStruct((CHUNKS, 2), I32),
        ),
        in_specs=[vmem, hbm, hbm],
        out_specs=(vmem,) * 6 + (pl.BlockSpec(memory_space=pltpu.SMEM),),
        scratch_shapes=[
            pltpu.VMEM((LAYERS, CX, CY), F32),
            pltpu.VMEM((3, LAYERS, CX, CY), F32),
            pltpu.VMEM((4, CHUNKS, 8, 128), F32),
            pltpu.VMEM((TABLE_ROWS, LO), F32),
            pltpu.VMEM((LO, CHUNK), BF16),
            pltpu.VMEM((256, 2 * CHUNK), BF16),
            pltpu.VMEM((4, 16, 2 * CHUNK), BF16),
            pltpu.SemaphoreType.DMA((2,)),
        ],
        compiler_params=pltpu.CompilerParams(vmem_limit_bytes=16 * MIB),
        name="deposit",
    )(received, solid, drag)


def gather_kernel(
    bounds_ref, own_ref, above_ref, below_ref, high_ref, low_ref, fields_any, out_ref,
    fields, table, tops, bottoms, low_hot, found, sem,
):
    top, bottom = at_edge("span")

    def smooth(comp, x):
        row = own_ref[pl.ds((comp * CX + x) * LAYERS, LAYERS), :]
        if x < RIM:
            row = row + jnp.where(top, 0.0, above_ref[pl.ds((comp * RIM + x) * LAYERS, LAYERS), :])
        if x >= CX - RIM:
            row = row + jnp.where(bottom, 0.0, below_ref[pl.ds((comp * RIM + x - CX + RIM) * LAYERS, LAYERS), :])
        return row

    for x in range(CX):
        void = 1.0 - smooth(0, x)
        for comp in range(4):
            row = void if comp == 0 else -smooth(comp, x) / void
            fields[comp, :, x, :] = row
            for half in range(2):
                for side in range(2):
                    spot = pl.ds(side * TABLE_ROWS + comp * 32 + half * CX + x, LAYERS, stride=128)
                    table[spot, :] = row[:, half * LO + side * 128 : half * LO + side * 128 + 128]
    copy = pltpu.make_async_copy(fields, fields_any, sem)
    copy.start()
    for block in range(CLASSES):
        spot = slice(block * 256, block * 256 + 256)
        for side in range(2):
            lanes = slice(side * 128, side * 128 + 128)
            at = side * TABLE_ROWS + block * 256
            tops[spot, lanes], bottoms[spot, lanes] = halves(table[at : at + 256, :])
    ids = lax.broadcasted_iota(I32, (CLASS_HIGH, 128), 0).astype(F32)

    def step(chunk, carry):
        fill_low_hot(low_hot, low_ref, chunk)

        def class_step(kind, sums):
            key = high_ref[chunk] - (kind * CLASS_HIGH).astype(F32)
            spot = pl.ds(pl.multiple_of(kind * 256, 256), 256)
            value = dot_nn(tops[spot, :], low_hot[...]) + dot_nn(bottoms[spot, :], low_hot[...])
            pieces = [[] for comp in range(4)]
            for r in range(8):
                member = ids == key[r : r + 1]
                for comp in range(4):
                    rows = [
                        jnp.where(
                            member[layer * 32 : layer * 32 + 32],
                            value[layer * 128 + comp * 32 : layer * 128 + comp * 32 + 32, r * 128 : (r + 1) * 128],
                            0.0,
                        )
                        for layer in range(2)
                    ]
                    pieces[comp].append(jnp.sum(rows[0] + rows[1], axis=0, keepdims=True))
            return tuple(total + jnp.concatenate(piece, axis=0) for total, piece in zip(sums, pieces))

        start = (jnp.zeros((8, 128), F32),) * 4
        sums = lax.fori_loop(bounds_ref[chunk, 0], bounds_ref[chunk, 1], class_step, start)
        for comp in range(4):
            found[comp, chunk] = sums[comp]
        return carry

    lax.fori_loop(0, CHUNKS, step, 0)
    for comp in range(4):
        slots = []
        for m in range(8):
            slots += swap_halves(found[comp, m], found[comp, m + 8])
        tile = jnp.transpose(jnp.concatenate(slots, axis=0))
        for half in range(2):
            out_ref[pl.ds(2 * comp + half, OWNERS, stride=BACK_ROWS), :] = tile[half * OWNERS : (half + 1) * OWNERS]
    copy.wait()


def gather(bounds, *arrays):
    vmem = pl.BlockSpec(memory_space=pltpu.VMEM)
    return pl.pallas_call(
        gather_kernel,
        out_shape=(
            jax.ShapeDtypeStruct((4, LAYERS, CX, CY), F32),
            jax.ShapeDtypeStruct((OWNERS * BACK_ROWS, 128), F32),
        ),
        in_specs=[pl.BlockSpec(memory_space=pltpu.SMEM)] + [vmem] * 5,
        out_specs=(pl.BlockSpec(memory_space=pltpu.HBM), vmem),
        scratch_shapes=[
            pltpu.VMEM((4, LAYERS, CX, CY), F32),
            pltpu.VMEM((2 * TABLE_ROWS, 128), F32),
            pltpu.VMEM((TABLE_ROWS, LO), BF16),
            pltpu.VMEM((TABLE_ROWS, LO), BF16),
            pltpu.VMEM((LO, CHUNK), BF16),
            pltpu.VMEM((4, CHUNKS, 8, 128), F32),
            pltpu.SemaphoreType.DMA,
        ],
        compiler_params=pltpu.CompilerParams(vmem_limit_bytes=16 * MIB),
        name="gather",
    )(bounds, *arrays)


PICK_BLOCK = 1024


def pick_kernel(count_ref, slab_ref, position_ref, back_ref, out_ref, tops, bottoms):
    count = count_ref[0, 0]
    for comp in range(4):
        tile = jnp.concatenate(
            [back_ref[pl.ds(2 * comp + half, OWNERS, stride=BACK_ROWS), :] for half in range(2)], axis=1
        )
        high, low = halves(tile)
        tops[comp * OWNERS : (comp + 1) * OWNERS, :] = high
        bottoms[comp * OWNERS : (comp + 1) * OWNERS, :] = low

    def step(block, carry):
        start = pl.multiple_of(block * PICK_BLOCK, PICK_BLOCK)
        spot = pl.ds(start, PICK_BLOCK)
        lane = lax.broadcasted_iota(I32, (1, PICK_BLOCK), 1) + start
        slab = jnp.where(lane < count, slab_ref[0:1, spot], OWNERS)
        position_hot = one_hot(position_ref[0:1, spot], CAP)
        value = dot_nn(tops[...], position_hot) + dot_nn(bottoms[...], position_hot)
        member = lax.broadcasted_iota(I32, (OWNERS, PICK_BLOCK), 0) == slab
        for comp in range(4):
            piece = value[comp * OWNERS : (comp + 1) * OWNERS, :]
            out_ref[comp, 0:1, spot] = jnp.sum(jnp.where(member, piece, 0.0), axis=0, keepdims=True)
        return carry

    lax.fori_loop(0, PARTS // PICK_BLOCK, step, 0)


def pick(count, slab, position, back):
    vmem = pl.BlockSpec(memory_space=pltpu.VMEM)
    return pl.pallas_call(
        pick_kernel,
        out_shape=jax.ShapeDtypeStruct((4, 1, PARTS), F32),
        in_specs=[pl.BlockSpec(memory_space=pltpu.SMEM), vmem, vmem, vmem],
        out_specs=vmem,
        scratch_shapes=[pltpu.VMEM((4 * OWNERS, CAP), BF16)] * 2,
        name="pick",
        compiler_params=pltpu.CompilerParams(vmem_limit_bytes=8 * MIB),
    )(count, slab, position, back)


WIDE = CY + 128


def relax_kernel(
    target_ref, prior_ref, before, after, own_ref, up_ref, down_ref, state, source
):
    top, bottom = at_edge("span")
    first, last = at_edge("depth")
    near = lax.broadcasted_iota(I32, (LAYERS, 128), 1)
    is_before = (near >= 120) & jnp.logical_not(first)
    is_after = (near < 8) & jnp.logical_not(last)
    blank = jnp.zeros((LAYERS, WIDE), F32)
    for comp in range(4):
        for x in range(RIM):
            state[comp, x] = blank
            state[comp, RIM + CX + x] = blank
        for x in range(CX):
            row = comp * CX + x
            for half in range(2):
                for side in range(2):
                    at, lanes = target_row(comp, side, half * CX + x), half * LO + side * 128
                    source[comp, x, :, lanes : lanes + 128] = target_ref[at : at + LAYERS, :]
            source[comp, x, :, CY:WIDE] = unfold_side(row, before, after, is_before, is_after)
            state[comp, RIM + x, :, 0:CY] = prior_ref[row * LAYERS : (row + 1) * LAYERS, :]
            state[comp, RIM + x, :, CY:WIDE] = unfold_side(4 * CX + row, before, after, is_before, is_after)

    lane = lax.broadcasted_iota(I32, (LAYERS, WIDE), 1)
    outside = ((lane >= CY + 64) & first) | ((lane >= CY) & (lane < CY + 64) & last)
    factor = jnp.where(outside, 0.0, 0.2)
    above_factor = jnp.where(top, 0.0, factor)
    below_factor = jnp.where(bottom, 0.0, factor)

    def comp_step(comp, carry):
        for sweep in range(SWEEPS):
            rim = sweep + 1
            above, here = blank, blank
            for x in range(-rim, CX + rim):
                below = state[comp, x + 1 + RIM] if x + 1 < CX + sweep else blank
                total = above + below
                if -sweep <= x < CX + sweep:
                    total = total + pltpu.roll(here, 1, 1) + pltpu.roll(here, WIDE - 1, 1)
                if 0 <= x < CX:
                    total = total + source[comp, x]
                scale = above_factor if x < 0 else below_factor if x >= CX else factor
                state[comp, x + RIM] = total * scale
                above, here = here, below
        return carry

    lax.fori_loop(0, 4, comp_step, 0)
    for comp in range(4):
        for x in range(CX):
            own_ref[pl.ds((comp * CX + x) * LAYERS, LAYERS), :] = state[comp, RIM + x, :, 0:CY]
        for x in range(RIM):
            spot = pl.ds((comp * RIM + x) * LAYERS, LAYERS)
            up_ref[spot, :] = state[comp, x, :, 0:CY]
            down_ref[spot, :] = state[comp, RIM + CX + x, :, 0:CY]


def relax(*arrays):
    vmem = pl.BlockSpec(memory_space=pltpu.VMEM)
    rim = jax.ShapeDtypeStruct((4 * RIM * LAYERS, CY), F32)
    return pl.pallas_call(
        relax_kernel,
        out_shape=(jax.ShapeDtypeStruct((4 * CX * LAYERS, CY), F32), rim, rim),
        in_specs=[vmem] * 4,
        out_specs=(vmem, vmem, vmem),
        scratch_shapes=[
            pltpu.VMEM((4, CX + 2 * RIM, LAYERS, WIDE), F32),
            pltpu.VMEM((4, CX, LAYERS, WIDE), F32),
        ],
        name="relax",
        compiler_params=pltpu.CompilerParams(vmem_limit_bytes=16 * MIB),
    )(*arrays)


def shifted(array, axis, step):
    count = lax.axis_size(axis)
    return lax.ppermute(array, axis, [(i, (i + step) % count) for i in range(count)])


def on_device(part_slab, part_cell, part_volume, part_drag, part_count, prior_solid, prior_drag):
    slab = part_slab.reshape(1, PARTS)
    sent, position = pack(part_count, slab, part_cell, part_volume, part_drag)
    received = lax.all_to_all(sent.reshape(OWNERS, 5, 2, 128), "span", 0, 0, tiled=True)
    received = received.reshape(OWNERS * ROWS, 128)
    target, first, last, prior, high, low, bounds = deposit(received, prior_solid, prior_drag)
    before = shifted(last, "depth", 1)
    after = shifted(first, "depth", -1)
    own, up, down = relax(target, prior, before, after)
    from_above = shifted(down, "span", 1)
    from_below = shifted(up, "span", -1)
    fields, returned = gather(bounds, own, from_above, from_below, high, low)
    back = lax.all_to_all(returned.reshape(OWNERS, BACK_ROWS, 128), "span", 0, 0, tiled=True)
    feedback = pick(part_count, slab, position, back.reshape(OWNERS * BACK_ROWS, 128))
    return fields, feedback


def solution(mesh):
    in_specs = (
        P("depth", "span", None),
        P("depth", "span"),
        P("depth", "span"),
        P(None, "depth", "span"),
        P("depth", "span"),
        P(None, "span", "depth"),
        P(None, None, "span", "depth"),
    )
    out_specs = (P(None, None, "span", "depth"), P(None, "depth", "span"))
    return jax.shard_map(on_device, mesh=mesh, in_specs=in_specs, out_specs=out_specs, check_vma=False)
```

```python
import functools

import jax
import jax.numpy as jnp
from jax import lax
from jax.experimental import pallas as pl
from jax.experimental.pallas import tpu as pltpu
from jax.sharding import PartitionSpec as P

F32, BF16, I32 = jnp.float32, jnp.bfloat16, jnp.int32
MIB = 1 << 20
OWNERS = 64
CAP = 256
LAYERS, CX, CY = 8, 16, 512
PARTS = 8192
HI, LO = 256, 256
ROWS = 2 * 5
BACK_ROWS = 8
SWEEPS = 6
RIM = SWEEPS
GROUPS, GROUP = 2, 2
SIDE_ROWS = 2 * 4 * CX // 16 * LAYERS
PHI_LIMIT = 0.6


def halves(value):
    high = value.astype(BF16)
    return high, (value - high.astype(F32)).astype(BF16)


def spread(row, size):
    n = row.shape[1]
    packed = jnp.broadcast_to(row, (16, n)).astype(BF16)
    return jnp.broadcast_to(packed[None], (size // 16, 16, n)).reshape(size, n)


def index_rows(size, n):
    return lax.broadcasted_iota(I32, (size, n), 0).astype(F32).astype(BF16)


def row_is(row, size):
    return index_rows(size, row.shape[1]) == spread(row, size)


def one_hot(row, size):
    return jnp.where(row_is(row, size), jnp.ones((), BF16), jnp.zeros((), BF16))


def dot_nt(left, right):
    return lax.dot_general(left, right, (((1,), (1,)), ((), ())), preferred_element_type=F32)


def dot_nn(left, right):
    return lax.dot_general(left, right, (((1,), (0,)), ((), ())), preferred_element_type=F32)


def at_edge(axis):
    place = lax.axis_index(axis)
    return place == 0, place == lax.axis_size(axis) - 1


def fold_sides(pieces, left_ref, right_ref):
    lane = lax.broadcasted_iota(I32, (LAYERS, 128), 1)
    for group in range(SIDE_ROWS // LAYERS):
        left = jnp.zeros((LAYERS, 128), F32)
        right = jnp.zeros((LAYERS, 128), F32)
        for place in range(16):
            first, last = pieces(group * 16 + place)
            here = (lane >= 8 * place) & (lane < 8 * place + 8)
            left = jnp.where(here, pltpu.roll(first, 8 * place, 1) if place else first, left)
            shift = (8 * place + 8) % 128
            right = jnp.where(here, pltpu.roll(last, shift, 1) if shift else last, right)
        left_ref[group * LAYERS : (group + 1) * LAYERS, :] = left
        right_ref[group * LAYERS : (group + 1) * LAYERS, :] = right


def unfold_side(row, before_ref, after_ref, is_before, is_after):
    group, place = row // 16, row % 16
    after = after_ref[group * LAYERS : (group + 1) * LAYERS, :]
    before = before_ref[group * LAYERS : (group + 1) * LAYERS, :]
    after = pltpu.roll(after, 128 - 8 * place, 1) if place else after
    shift = (120 - 8 * place) % 128
    before = pltpu.roll(before, shift, 1) if shift else before
    return jnp.where(is_after, after, jnp.where(is_before, before, 0.0))


def prior_row(solid_ref, drag_ref, row, lanes):
    comp, x = row // CX, row % CX
    return solid_ref[:, x, lanes] if comp == 0 else drag_ref[comp - 1, :, x, lanes]


PACK_BLOCK = 1024
SUB = 256
CLASSES = 4


def pack_kernel(
    count_ref, slab_any, cell_any, volume_any, drag_any, out_ref, position_ref,
    slab_ref, cell_ref, volume_ref, drag_ref, acc, sems,
):
    sources, targets = (slab_any, cell_any, volume_any, drag_any), (slab_ref, cell_ref, volume_ref, drag_ref)
    copies = [pltpu.make_async_copy(f, t, sems.at[i]) for i, (f, t) in enumerate(zip(sources, targets))]
    for copy in copies:
        copy.start()
    count = count_ref[0, 0]
    acc[...] = jnp.zeros_like(acc)
    earlier = lax.broadcasted_iota(I32, (SUB, SUB), 0)
    later = lax.broadcasted_iota(I32, (SUB, SUB), 1)
    upper = jnp.where(earlier <= later, 1.0, 0.0).astype(BF16)
    for copy in copies:
        copy.wait()

    def live_slab(start, size):
        lane = lax.broadcasted_iota(I32, (1, size), 1) + start
        return jnp.where(lane < count, slab_ref[0:1, pl.ds(start, size)], CLASSES * OWNERS)

    def classes(start, size):
        cell = cell_ref[0:1, pl.ds(start, size)]
        return (lax.shift_right_logical(cell, 8) & 1) * 2 + (lax.shift_right_logical(cell, 12) & 1)

    def count_step(block, counts):
        start = pl.multiple_of(block * PACK_BLOCK, PACK_BLOCK)
        member = one_hot(live_slab(start, PACK_BLOCK).astype(F32), OWNERS)
        kind = one_hot(classes(start, PACK_BLOCK).astype(F32), 128)
        return counts + dot_nt(member, kind)

    counts = lax.fori_loop(0, PARTS // PACK_BLOCK, count_step, jnp.zeros((OWNERS, 128), F32))
    numbers = [jnp.broadcast_to(counts[:, kind : kind + 1], (OWNERS, 128)) for kind in range(CLASSES)]
    starts, end = [], jnp.zeros((OWNERS, 128), F32)
    for kind in range(CLASSES):
        rest = sum(numbers[kind:])
        starts.append(jnp.maximum(end, jnp.minimum(float(kind * CAP // CLASSES), CAP - rest)))
        end = starts[-1] + numbers[kind]

    def step(block, offset):
        hots, lefts = [], []
        for sub in range(PACK_BLOCK // SUB):
            start = pl.multiple_of(block * PACK_BLOCK + sub * SUB, SUB)
            spot = pl.ds(start, SUB)
            slab = live_slab(start, SUB)
            member = row_is(slab.astype(F32), OWNERS)
            sorted_one = one_hot((slab + classes(start, SUB) * OWNERS).astype(F32), CLASSES * OWNERS)
            ranks = dot_nn(sorted_one, upper)
            place = ranks + jnp.concatenate([offset, offset], axis=1)
            position = jnp.sum(place * sorted_one.astype(F32), axis=0, keepdims=True) - 1.0
            offset = offset + jnp.broadcast_to(ranks[:, SUB - 1 : SUB], offset.shape)
            position_ref[0:1, spot] = position
            hots.append(one_hot(position, CAP))
            cell = cell_ref[0:1, spot]
            cell_high = lax.shift_right_logical(cell, 8)
            rows = [cell_high.astype(F32), (cell - cell_high * 256).astype(F32)]
            for value in [volume_ref[0:1, spot]] + [drag_ref[k, 0:1, spot] for k in range(3)]:
                high = value.astype(BF16).astype(F32)
                rows += [high, value - high]
            zero = jnp.zeros((), BF16)
            lefts.append(
                jnp.concatenate([jnp.where(member, spread(row, OWNERS), zero) for row in rows], axis=0)
            )
        acc[...] += dot_nt(jnp.concatenate(lefts, axis=1), jnp.concatenate(hots, axis=1))
        return offset

    lax.fori_loop(0, PARTS // PACK_BLOCK, step, jnp.concatenate(starts, axis=0))
    for comp in range(5):
        high = acc[2 * comp * OWNERS : (2 * comp + 1) * OWNERS, :]
        low = acc[(2 * comp + 1) * OWNERS : (2 * comp + 2) * OWNERS, :]
        whole = high * 256.0 + low if comp == 0 else high + low
        for half in range(2):
            out_ref[pl.ds(2 * comp + half, OWNERS, stride=ROWS), :] = whole[:, half * 128 : (half + 1) * 128]


def pack(count, slab, cell, volume, drag):
    vmem = pl.BlockSpec(memory_space=pltpu.VMEM)
    hbm = pl.BlockSpec(memory_space=pltpu.HBM)
    return pl.pallas_call(
        pack_kernel,
        out_shape=(
            jax.ShapeDtypeStruct((OWNERS * ROWS, 128), F32),
            jax.ShapeDtypeStruct((1, PARTS), F32),
        ),
        in_specs=[pl.BlockSpec(memory_space=pltpu.SMEM), hbm, hbm, hbm, hbm],
        out_specs=(vmem, vmem),
        scratch_shapes=[
            pltpu.VMEM((1, PARTS), I32),
            pltpu.VMEM((1, PARTS), I32),
            pltpu.VMEM((1, PARTS), F32),
            pltpu.VMEM((3, 1, PARTS), F32),
            pltpu.VMEM((10 * OWNERS, CAP), F32),
            pltpu.SemaphoreType.DMA((4,)),
        ],
        compiler_params=pltpu.CompilerParams(vmem_limit_bytes=8 * MIB),
        name="pack",
    )(count, slab, cell, volume, drag)


CHUNKS, CHUNK = 16, 1024
CLASS_HIGH = HI // CLASSES


def swap_halves(first, second):
    lane = lax.broadcasted_iota(I32, (8, 128), 1)
    return (
        jnp.where(lane < 64, first, pltpu.roll(second, 64, 1)),
        jnp.where(lane < 64, pltpu.roll(first, 64, 1), second),
    )


def low_hots(low_ref, chunk):
    return jnp.concatenate([one_hot(low_ref[chunk, r : r + 1, :], LO) for r in range(8)], axis=1)


def deposit_kernel(
    recv_ref, solid_any, drag_any,
    out_ref, first_ref, last_ref, prior_ref, high_ref, low_ref, bounds_ref,
    solid_ref, drag_ref, values, sems,
):
    copies = [
        pltpu.make_async_copy(solid_any, solid_ref, sems.at[0]),
        pltpu.make_async_copy(drag_any, drag_ref, sems.at[1]),
    ]
    for copy in copies:
        copy.start()
    out_ref[...] = jnp.zeros_like(out_ref)
    zero = jnp.zeros((), BF16)

    def chunked(comp):
        tile = jnp.concatenate([recv_ref[pl.ds(2 * comp + half, OWNERS, stride=ROWS), :] for half in range(2)], axis=0)
        slots = jnp.transpose(tile)
        pairs = [swap_halves(slots[16 * m : 16 * m + 8], slots[16 * m + 8 : 16 * m + 16]) for m in range(8)]
        return [pair[0] for pair in pairs] + [pair[1] for pair in pairs]

    volumes = chunked(1)
    for chunk, cell in enumerate(chunked(0)):
        cell = cell.astype(I32)
        layer = lax.shift_right_logical(cell, 13)
        high = ((lax.shift_right_logical(cell, 8) & 1) * 16 + (lax.shift_right_logical(cell, 9) & 15)) * 8 + layer
        high_ref[chunk] = high.astype(F32)
        low_ref[chunk] = (cell & 255).astype(F32)
        values[0, chunk] = volumes[chunk]
        live = volumes[chunk] > 0.0
        kind = lax.shift_right_logical(high, 6).astype(F32)
        bounds_ref[chunk, 0] = jnp.min(jnp.where(live, kind, float(CLASSES))).astype(I32)
        bounds_ref[chunk, 1] = jnp.max(jnp.where(live, kind, -1.0)).astype(I32) + 1
    for comp in range(1, 4):
        for chunk, value in enumerate(chunked(comp + 1)):
            values[comp, chunk] = value

    def step(chunk, carry):
        def class_step(kind, carry):
            key = high_ref[chunk] - (kind * CLASS_HIGH).astype(F32)
            members = [row_is(key[r : r + 1], CLASS_HIGH) for r in range(8)]
            lows = low_hots(low_ref, chunk)
            left = []
            for comp in range(4):
                value = values[comp, chunk]
                top = value.astype(BF16).astype(F32)
                left.append(
                    jnp.concatenate(
                        [
                            jnp.where(members[r], spread(piece[r : r + 1], CLASS_HIGH), zero)
                            for piece in (top, value - top)
                            for r in range(8)
                        ],
                        axis=1,
                    )
                )
            total = dot_nt(jnp.concatenate(left, axis=0), jnp.concatenate([lows, lows], axis=1))
            spot = pl.ds(pl.multiple_of(kind * CLASS_HIGH, CLASS_HIGH), CLASS_HIGH)
            for comp in range(4):
                out_ref[comp, spot, :] += total[comp * CLASS_HIGH : (comp + 1) * CLASS_HIGH, :]
            return carry

        return lax.fori_loop(bounds_ref[chunk, 0], bounds_ref[chunk, 1], class_step, carry)

    lax.fori_loop(0, CHUNKS, step, 0)
    out_ref[0] = jnp.minimum(out_ref[0], PHI_LIMIT)
    for copy in copies:
        copy.wait()
    for row in range(4 * CX):
        prior_ref[row * LAYERS : (row + 1) * LAYERS, :] = prior_row(solid_ref, drag_ref, row, slice(None))

    def pieces(row):
        if row >= 4 * CX:
            row -= 4 * CX
            spot = slice(row * LAYERS, (row + 1) * LAYERS)
            return prior_ref[spot, 0:128], prior_ref[spot, CY - 128 : CY]
        comp, x = row // CX, row % CX
        first = out_ref[comp, x * LAYERS : (x + 1) * LAYERS, 0:128]
        last = out_ref[comp, (CX + x) * LAYERS : (CX + x + 1) * LAYERS, LO - 128 : LO]
        return first, last

    fold_sides(pieces, first_ref, last_ref)


def deposit(received, solid, drag):
    vmem = pl.BlockSpec(memory_space=pltpu.VMEM)
    hbm = pl.BlockSpec(memory_space=pltpu.HBM)
    side = jax.ShapeDtypeStruct((SIDE_ROWS, 128), F32)
    index = jax.ShapeDtypeStruct((CHUNKS, 8, 128), F32)
    return pl.pallas_call(
        deposit_kernel,
        out_shape=(
            jax.ShapeDtypeStruct((4, HI, LO), F32),
            side,
            side,
            jax.ShapeDtypeStruct((4 * CX * LAYERS, CY), F32),
            index,
            index,
            jax.ShapeDtypeStruct((CHUNKS, 2), I32),
        ),
        in_specs=[vmem, hbm, hbm],
        out_specs=(vmem,) * 6 + (pl.BlockSpec(memory_space=pltpu.SMEM),),
        scratch_shapes=[
            pltpu.VMEM((LAYERS, CX, CY), F32),
            pltpu.VMEM((3, LAYERS, CX, CY), F32),
            pltpu.VMEM((4, CHUNKS, 8, 128), F32),
            pltpu.SemaphoreType.DMA((2,)),
        ],
        compiler_params=pltpu.CompilerParams(vmem_limit_bytes=16 * MIB),
        name="deposit",
    )(received, solid, drag)


def gather_kernel(bounds_ref, *refs):
    own_refs, above_refs, below_refs = refs[0:GROUPS], refs[GROUPS : 2 * GROUPS], refs[2 * GROUPS : 3 * GROUPS]
    high_ref, low_ref, fields_any, out_ref, fields, tops, bottoms, found, sem = refs[3 * GROUPS :]
    top, bottom = at_edge("span")

    def smooth(comp, x):
        group, comp = comp // GROUP, comp % GROUP
        row = own_refs[group][pl.ds((comp * CX + x) * LAYERS, LAYERS), :]
        if x < RIM:
            spot = pl.ds((comp * RIM + x) * LAYERS, LAYERS)
            row = row + jnp.where(top, 0.0, above_refs[group][spot, :])
        if x >= CX - RIM:
            spot = pl.ds((comp * RIM + x - CX + RIM) * LAYERS, LAYERS)
            row = row + jnp.where(bottom, 0.0, below_refs[group][spot, :])
        return row

    for pair in range(0, CX, 2):
        void = [1.0 - smooth(0, x) for x in (pair, pair + 1)]
        for comp in range(4):
            rows = void if comp == 0 else [-smooth(comp, x) / v for x, v in zip((pair, pair + 1), void)]
            for x, row in zip((pair, pair + 1), rows):
                fields[comp, :, x, :] = row
            high, low = halves(jnp.concatenate(rows, axis=0))
            for half in range(2):
                spot = pl.ds((half * CX + pair) * LAYERS, 2 * LAYERS)
                tops[comp, spot, :] = high[:, half * LO : (half + 1) * LO]
                bottoms[comp, spot, :] = low[:, half * LO : (half + 1) * LO]
    copy = pltpu.make_async_copy(fields, fields_any, sem)
    copy.start()
    ids = lax.broadcasted_iota(I32, (CLASS_HIGH, 128), 0).astype(F32)

    def step(chunk, carry):
        def class_step(kind, sums):
            key = high_ref[chunk] - (kind * CLASS_HIGH).astype(F32)
            lows = low_hots(low_ref, chunk)
            spot = pl.ds(pl.multiple_of(kind * CLASS_HIGH, CLASS_HIGH), CLASS_HIGH)
            members = [ids == key[r : r + 1] for r in range(8)]
            table = [jnp.concatenate([part[comp, spot, :] for comp in range(4)], axis=0) for part in (tops, bottoms)]
            value = dot_nn(table[0], lows) + dot_nn(table[1], lows)
            new = []
            for comp in range(4):
                rows = value[comp * CLASS_HIGH : (comp + 1) * CLASS_HIGH]
                pieces = [
                    jnp.sum(jnp.where(members[r], rows[:, r * 128 : (r + 1) * 128], 0.0), axis=0, keepdims=True)
                    for r in range(8)
                ]
                new.append(sums[comp] + jnp.concatenate(pieces, axis=0))
            return tuple(new)

        start = (jnp.zeros((8, 128), F32),) * 4
        sums = lax.fori_loop(bounds_ref[chunk, 0], bounds_ref[chunk, 1], class_step, start)
        for comp in range(4):
            found[comp, chunk] = sums[comp]
        return carry

    lax.fori_loop(0, CHUNKS, step, 0)
    for comp in range(4):
        slots = []
        for m in range(8):
            slots += swap_halves(found[comp, m], found[comp, m + 8])
        tile = jnp.transpose(jnp.concatenate(slots, axis=0))
        for half in range(2):
            out_ref[pl.ds(2 * comp + half, OWNERS, stride=BACK_ROWS), :] = tile[half * OWNERS : (half + 1) * OWNERS]
    copy.wait()


def gather(bounds, owns, aboves, belows, high, low):
    vmem = pl.BlockSpec(memory_space=pltpu.VMEM)
    return pl.pallas_call(
        gather_kernel,
        out_shape=(
            jax.ShapeDtypeStruct((4, LAYERS, CX, CY), F32),
            jax.ShapeDtypeStruct((OWNERS * BACK_ROWS, 128), F32),
        ),
        in_specs=[pl.BlockSpec(memory_space=pltpu.SMEM)] + [vmem] * (3 * GROUPS + 2),
        out_specs=(pl.BlockSpec(memory_space=pltpu.HBM), vmem),
        scratch_shapes=[
            pltpu.VMEM((4, LAYERS, CX, CY), F32),
            pltpu.VMEM((4, HI, LO), BF16),
            pltpu.VMEM((4, HI, LO), BF16),
            pltpu.VMEM((4, CHUNKS, 8, 128), F32),
            pltpu.SemaphoreType.DMA,
        ],
        compiler_params=pltpu.CompilerParams(vmem_limit_bytes=16 * MIB),
        name="gather",
    )(bounds, *owns, *aboves, *belows, high, low)


PICK_BLOCK = 1024


def pick_kernel(count_ref, slab_ref, position_ref, back_ref, out_ref, tops, bottoms):
    count = count_ref[0, 0]
    for comp in range(4):
        tile = jnp.concatenate(
            [back_ref[pl.ds(2 * comp + half, OWNERS, stride=BACK_ROWS), :] for half in range(2)], axis=1
        )
        high, low = halves(tile)
        tops[comp * OWNERS : (comp + 1) * OWNERS, :] = high
        bottoms[comp * OWNERS : (comp + 1) * OWNERS, :] = low

    def step(block, carry):
        start = pl.multiple_of(block * PICK_BLOCK, PICK_BLOCK)
        spot = pl.ds(start, PICK_BLOCK)
        lane = lax.broadcasted_iota(I32, (1, PICK_BLOCK), 1) + start
        slab = jnp.where(lane < count, slab_ref[0:1, spot], OWNERS)
        position_hot = one_hot(position_ref[0:1, spot], CAP)
        value = dot_nn(tops[...], position_hot) + dot_nn(bottoms[...], position_hot)
        member = lax.broadcasted_iota(I32, (OWNERS, PICK_BLOCK), 0) == slab
        for comp in range(4):
            piece = value[comp * OWNERS : (comp + 1) * OWNERS, :]
            out_ref[comp, 0:1, spot] = jnp.sum(jnp.where(member, piece, 0.0), axis=0, keepdims=True)
        return carry

    lax.fori_loop(0, PARTS // PICK_BLOCK, step, 0)


def pick(count, slab, position, back):
    vmem = pl.BlockSpec(memory_space=pltpu.VMEM)
    return pl.pallas_call(
        pick_kernel,
        out_shape=jax.ShapeDtypeStruct((4, 1, PARTS), F32),
        in_specs=[pl.BlockSpec(memory_space=pltpu.SMEM), vmem, vmem, vmem],
        out_specs=vmem,
        scratch_shapes=[pltpu.VMEM((4 * OWNERS, CAP), BF16)] * 2,
        name="pick",
        compiler_params=pltpu.CompilerParams(vmem_limit_bytes=8 * MIB),
    )(count, slab, position, back)


WIDE = CY + 128
RELAX_FLOPS = 40_000_000


def relax_kernel(
    base, target_ref, prior_ref, before, after, own_ref, up_ref, down_ref, state, source
):
    top, bottom = at_edge("span")
    first, last = at_edge("depth")
    near = lax.broadcasted_iota(I32, (LAYERS, 128), 1)
    is_before = (near >= 120) & jnp.logical_not(first)
    is_after = (near < 8) & jnp.logical_not(last)
    blank = jnp.zeros((LAYERS, WIDE), F32)
    for comp in range(GROUP):
        for x in range(RIM):
            state[comp, x] = blank
            state[comp, RIM + CX + x] = blank
        for x in range(CX):
            row = (base + comp) * CX + x
            for half in range(2):
                spot = pl.ds((half * CX + x) * LAYERS, LAYERS)
                source[comp, x, :, half * LO : (half + 1) * LO] = target_ref[base + comp, spot, :]
            source[comp, x, :, CY:WIDE] = unfold_side(row, before, after, is_before, is_after)
            state[comp, RIM + x, :, 0:CY] = prior_ref[row * LAYERS : (row + 1) * LAYERS, :]
            state[comp, RIM + x, :, CY:WIDE] = unfold_side(4 * CX + row, before, after, is_before, is_after)

    lane = lax.broadcasted_iota(I32, (LAYERS, WIDE), 1)
    outside = ((lane >= CY + 64) & first) | ((lane >= CY) & (lane < CY + 64) & last)
    factor = jnp.where(outside, 0.0, 0.2)
    above_factor = jnp.where(top, 0.0, factor)
    below_factor = jnp.where(bottom, 0.0, factor)

    def comp_step(comp, carry):
        for sweep in range(SWEEPS):
            rim = sweep + 1
            above, here = blank, blank
            for x in range(-rim, CX + rim):
                below = state[comp, x + 1 + RIM] if x + 1 < CX + sweep else blank
                total = above + below
                if -sweep <= x < CX + sweep:
                    total = total + pltpu.roll(here, 1, 1) + pltpu.roll(here, WIDE - 1, 1)
                if 0 <= x < CX:
                    total = total + source[comp, x]
                scale = above_factor if x < 0 else below_factor if x >= CX else factor
                state[comp, x + RIM] = total * scale
                above, here = here, below
        return carry

    lax.fori_loop(0, GROUP, comp_step, 0)
    for comp in range(GROUP):
        for x in range(CX):
            own_ref[pl.ds((comp * CX + x) * LAYERS, LAYERS), :] = state[comp, RIM + x, :, 0:CY]
        for x in range(RIM):
            spot = pl.ds((comp * RIM + x) * LAYERS, LAYERS)
            up_ref[spot, :] = state[comp, x, :, 0:CY]
            down_ref[spot, :] = state[comp, RIM + CX + x, :, 0:CY]


def relax(base, *arrays):
    vmem = pl.BlockSpec(memory_space=pltpu.VMEM)
    rim = jax.ShapeDtypeStruct((GROUP * RIM * LAYERS, CY), F32)
    return pl.pallas_call(
        functools.partial(relax_kernel, base),
        out_shape=(jax.ShapeDtypeStruct((GROUP * CX * LAYERS, CY), F32), rim, rim),
        in_specs=[vmem] * 4,
        out_specs=(vmem, vmem, vmem),
        scratch_shapes=[
            pltpu.VMEM((GROUP, CX + 2 * RIM, LAYERS, WIDE), F32),
            pltpu.VMEM((GROUP, CX, LAYERS, WIDE), F32),
        ],
        compiler_params=pltpu.CompilerParams(vmem_limit_bytes=12 * MIB),
        cost_estimate=pl.CostEstimate(flops=RELAX_FLOPS, bytes_accessed=4 * MIB, transcendentals=0),
        name=f"relax_{base}",
    )(*arrays)


def shifted(array, axis, step):
    count = lax.axis_size(axis)
    return lax.ppermute(array, axis, [(i, (i + step) % count) for i in range(count)])


def on_device(part_slab, part_cell, part_volume, part_drag, part_count, prior_solid, prior_drag):
    slab = part_slab.reshape(1, PARTS)
    in_hbm = [pltpu.with_memory_space_constraint(a, pltpu.HBM) for a in (slab, part_cell, part_volume, part_drag)]
    sent, position = pack(part_count, *in_hbm)
    received = lax.all_to_all(sent.reshape(OWNERS, 5, 2, 128), "span", 0, 0, tiled=True)
    received = received.reshape(OWNERS * ROWS, 128)
    target, first, last, prior, high, low, bounds = deposit(
        received, *[pltpu.with_memory_space_constraint(a, pltpu.HBM) for a in (prior_solid, prior_drag)]
    )
    before = shifted(last, "depth", 1)
    after = shifted(first, "depth", -1)
    owns, aboves, belows = [], [], []
    for group in range(GROUPS):
        own, up, down = relax(group * GROUP, target, prior, before, after)
        owns.append(own)
        aboves.append(shifted(down, "span", 1))
        belows.append(shifted(up, "span", -1))
    fields, returned = gather(bounds, owns, aboves, belows, high, low)
    back = lax.all_to_all(returned.reshape(OWNERS, BACK_ROWS, 128), "span", 0, 0, tiled=True)
    feedback = pick(part_count, slab, position, back.reshape(OWNERS * BACK_ROWS, 128))
    return fields, feedback


def solution(mesh):
    in_specs = (
        P("depth", "span", None),
        P("depth", "span"),
        P("depth", "span"),
        P(None, "depth", "span"),
        P("depth", "span"),
        P(None, "span", "depth"),
        P(None, None, "span", "depth"),
    )
    out_specs = (P(None, None, "span", "depth"), P(None, "depth", "span"))
    return jax.shard_map(on_device, mesh=mesh, in_specs=in_specs, out_specs=out_specs, check_vma=False)
```

```python
import functools

import jax
import jax.numpy as jnp
from jax import lax
from jax.experimental import pallas as pl
from jax.experimental.pallas import tpu as pltpu
from jax.sharding import PartitionSpec as P

F32, BF16, I32 = jnp.float32, jnp.bfloat16, jnp.int32
MIB = 1 << 20
OWNERS = 64
CAP = 256
LAYERS, CX, CY = 8, 16, 512
PARTS = 8192
HI, LO = 256, 256
ROWS = 2 * 5
BACK_ROWS = 8
SWEEPS = 6
RIM = SWEEPS
GROUPS, GROUP = 1, 4
SIDE_ROWS = 2 * 4 * CX // 16 * LAYERS
PHI_LIMIT = 0.6


def halves(value):
    high = value.astype(BF16)
    return high, (value - high.astype(F32)).astype(BF16)


def spread(row, size):
    n = row.shape[1]
    packed = jnp.broadcast_to(row, (16, n)).astype(BF16)
    return jnp.broadcast_to(packed[None], (size // 16, 16, n)).reshape(size, n)


def index_rows(size, n):
    return lax.broadcasted_iota(I32, (size, n), 0).astype(F32).astype(BF16)


def row_is(row, size):
    return index_rows(size, row.shape[1]) == spread(row, size)


def one_hot(row, size):
    return jnp.where(row_is(row, size), jnp.ones((), BF16), jnp.zeros((), BF16))


def dot_nt(left, right):
    return lax.dot_general(left, right, (((1,), (1,)), ((), ())), preferred_element_type=F32)


def dot_nn(left, right):
    return lax.dot_general(left, right, (((1,), (0,)), ((), ())), preferred_element_type=F32)


def at_edge(axis):
    place = lax.axis_index(axis)
    return place == 0, place == lax.axis_size(axis) - 1


def fold_sides(pieces, left_ref, right_ref):
    lane = lax.broadcasted_iota(I32, (LAYERS, 128), 1)
    for group in range(SIDE_ROWS // LAYERS):
        left = jnp.zeros((LAYERS, 128), F32)
        right = jnp.zeros((LAYERS, 128), F32)
        for place in range(16):
            first, last = pieces(group * 16 + place)
            here = (lane >= 8 * place) & (lane < 8 * place + 8)
            left = jnp.where(here, pltpu.roll(first, 8 * place, 1) if place else first, left)
            shift = (8 * place + 8) % 128
            right = jnp.where(here, pltpu.roll(last, shift, 1) if shift else last, right)
        left_ref[group * LAYERS : (group + 1) * LAYERS, :] = left
        right_ref[group * LAYERS : (group + 1) * LAYERS, :] = right


def unfold_side(row, before_ref, after_ref, is_before, is_after):
    group, place = row // 16, row % 16
    after = after_ref[group * LAYERS : (group + 1) * LAYERS, :]
    before = before_ref[group * LAYERS : (group + 1) * LAYERS, :]
    after = pltpu.roll(after, 128 - 8 * place, 1) if place else after
    shift = (120 - 8 * place) % 128
    before = pltpu.roll(before, shift, 1) if shift else before
    return jnp.where(is_after, after, jnp.where(is_before, before, 0.0))


def prior_row(solid_ref, drag_ref, row, lanes):
    comp, x = row // CX, row % CX
    return solid_ref[:, x, lanes] if comp == 0 else drag_ref[comp - 1, :, x, lanes]


PACK_BLOCK = 4096
SUB = 256
CLASSES = 4


def pack_kernel(
    count_ref, slab_any, cell_any, volume_any, drag_any, out_ref, position_ref,
    slab_ref, cell_ref, volume_ref, drag_ref, acc, sems,
):
    sources, targets = (slab_any, cell_any, volume_any, drag_any), (slab_ref, cell_ref, volume_ref, drag_ref)
    copies = [pltpu.make_async_copy(f, t, sems.at[i]) for i, (f, t) in enumerate(zip(sources, targets))]
    for copy in copies:
        copy.start()
    count = count_ref[0, 0]
    acc[...] = jnp.zeros_like(acc)
    earlier = lax.broadcasted_iota(I32, (SUB, SUB), 0)
    later = lax.broadcasted_iota(I32, (SUB, SUB), 1)
    upper = jnp.where(earlier <= later, 1.0, 0.0).astype(BF16)
    for copy in copies[:2]:
        copy.wait()

    def live_slab(start, size):
        lane = lax.broadcasted_iota(I32, (1, size), 1) + start
        return jnp.where(lane < count, slab_ref[0:1, pl.ds(start, size)], CLASSES * OWNERS)

    def classes(start, size):
        cell = cell_ref[0:1, pl.ds(start, size)]
        return (lax.shift_right_logical(cell, 8) & 1) * 2 + (lax.shift_right_logical(cell, 12) & 1)

    def count_step(block, counts):
        start = pl.multiple_of(block * PACK_BLOCK, PACK_BLOCK)
        member = one_hot(live_slab(start, PACK_BLOCK).astype(F32), OWNERS)
        kind = one_hot(classes(start, PACK_BLOCK).astype(F32), 128)
        return counts + dot_nt(member, kind)

    counts = lax.fori_loop(0, PARTS // PACK_BLOCK, count_step, jnp.zeros((OWNERS, 128), F32))
    numbers = [jnp.broadcast_to(counts[:, kind : kind + 1], (OWNERS, 128)) for kind in range(CLASSES)]
    for copy in copies[2:]:
        copy.wait()
    starts, end = [], jnp.zeros((OWNERS, 128), F32)
    for kind in range(CLASSES):
        rest = sum(numbers[kind:])
        starts.append(jnp.maximum(end, jnp.minimum(float(kind * CAP // CLASSES), CAP - rest)))
        end = starts[-1] + numbers[kind]

    def step(block, offset):
        hots, lefts = [], []
        for sub in range(PACK_BLOCK // SUB):
            start = pl.multiple_of(block * PACK_BLOCK + sub * SUB, SUB)
            spot = pl.ds(start, SUB)
            slab = live_slab(start, SUB)
            member = row_is(slab.astype(F32), OWNERS)
            sorted_one = one_hot((slab + classes(start, SUB) * OWNERS).astype(F32), CLASSES * OWNERS)
            ranks = dot_nn(sorted_one, upper)
            place = ranks + jnp.concatenate([offset, offset], axis=1)
            position = jnp.sum(place * sorted_one.astype(F32), axis=0, keepdims=True) - 1.0
            offset = offset + jnp.broadcast_to(ranks[:, SUB - 1 : SUB], offset.shape)
            position_ref[0:1, spot] = position
            hots.append(one_hot(position, CAP))
            cell = cell_ref[0:1, spot]
            cell_high = lax.shift_right_logical(cell, 8)
            rows = [cell_high.astype(F32), (cell - cell_high * 256).astype(F32)]
            for value in [volume_ref[0:1, spot]] + [drag_ref[k, 0:1, spot] for k in range(3)]:
                high = value.astype(BF16).astype(F32)
                rows += [high, value - high]
            zero = jnp.zeros((), BF16)
            lefts.append(
                jnp.concatenate([jnp.where(member, spread(row, OWNERS), zero) for row in rows], axis=0)
            )
        acc[...] += dot_nt(jnp.concatenate(lefts, axis=1), jnp.concatenate(hots, axis=1))
        return offset

    lax.fori_loop(0, PARTS // PACK_BLOCK, step, jnp.concatenate(starts, axis=0))
    for comp in range(5):
        high = acc[2 * comp * OWNERS : (2 * comp + 1) * OWNERS, :]
        low = acc[(2 * comp + 1) * OWNERS : (2 * comp + 2) * OWNERS, :]
        whole = high * 256.0 + low if comp == 0 else high + low
        for half in range(2):
            out_ref[pl.ds(2 * comp + half, OWNERS, stride=ROWS), :] = whole[:, half * 128 : (half + 1) * 128]


def pack(count, slab, cell, volume, drag):
    vmem = pl.BlockSpec(memory_space=pltpu.VMEM)
    hbm = pl.BlockSpec(memory_space=pltpu.HBM)
    return pl.pallas_call(
        pack_kernel,
        out_shape=(
            jax.ShapeDtypeStruct((OWNERS * ROWS, 128), F32),
            jax.ShapeDtypeStruct((1, PARTS), F32),
        ),
        in_specs=[pl.BlockSpec(memory_space=pltpu.SMEM), hbm, hbm, hbm, hbm],
        out_specs=(vmem, vmem),
        scratch_shapes=[
            pltpu.VMEM((1, PARTS), I32),
            pltpu.VMEM((1, PARTS), I32),
            pltpu.VMEM((1, PARTS), F32),
            pltpu.VMEM((3, 1, PARTS), F32),
            pltpu.VMEM((10 * OWNERS, CAP), F32),
            pltpu.SemaphoreType.DMA((4,)),
        ],
        compiler_params=pltpu.CompilerParams(vmem_limit_bytes=8 * MIB),
        name="pack",
    )(count, slab, cell, volume, drag)


CHUNKS, CHUNK = 16, 1024
CLASS_HIGH = HI // CLASSES
ABREAST = 4
ITEMS = CHUNKS * CLASSES + 8
NOWHERE = 1024


def swap_halves(first, second):
    lane = lax.broadcasted_iota(I32, (8, 128), 1)
    return (
        jnp.where(lane < 64, first, pltpu.roll(second, 64, 1)),
        jnp.where(lane < 64, pltpu.roll(first, 64, 1), second),
    )


def low_hots(low_ref, chunk):
    return jnp.concatenate([one_hot(low_ref[chunk, r : r + 1, :], LO) for r in range(8)], axis=1)


def deposit_kernel(
    recv_ref, solid_any, drag_any,
    out_ref, first_ref, last_ref, prior_ref, high_ref, low_ref, items_ref,
    solid_ref, drag_ref, values, bounds_ref, sems,
):
    copies = [
        pltpu.make_async_copy(solid_any, solid_ref, sems.at[0]),
        pltpu.make_async_copy(drag_any, drag_ref, sems.at[1]),
    ]
    for copy in copies:
        copy.start()
    out_ref[...] = jnp.zeros_like(out_ref)
    zero = jnp.zeros((), BF16)

    def chunked(comp):
        tile = jnp.concatenate([recv_ref[pl.ds(2 * comp + half, OWNERS, stride=ROWS), :] for half in range(2)], axis=0)
        slots = jnp.transpose(tile)
        pairs = [swap_halves(slots[16 * m : 16 * m + 8], slots[16 * m + 8 : 16 * m + 16]) for m in range(8)]
        return [pair[0] for pair in pairs] + [pair[1] for pair in pairs]

    volumes = chunked(1)
    for chunk, cell in enumerate(chunked(0)):
        cell = cell.astype(I32)
        layer = lax.shift_right_logical(cell, 13)
        high = ((lax.shift_right_logical(cell, 8) & 1) * 16 + (lax.shift_right_logical(cell, 9) & 15)) * 8 + layer
        high_ref[chunk] = high.astype(F32)
        low_ref[chunk] = (cell & 255).astype(F32)
        values[0, chunk] = volumes[chunk]
        live = volumes[chunk] > 0.0
        kind = lax.shift_right_logical(high, 6).astype(F32)
        bounds_ref[chunk, 0] = jnp.min(jnp.where(live, kind, float(CLASSES))).astype(I32)
        bounds_ref[chunk, 1] = jnp.max(jnp.where(live, kind, -1.0)).astype(I32) + 1
    for comp in range(1, 4):
        for chunk, value in enumerate(chunked(comp + 1)):
            values[comp, chunk] = value

    def list_chunk(chunk, count):
        def list_class(kind, count):
            items_ref[0, count] = chunk
            items_ref[1, count] = kind * CLASS_HIGH
            items_ref[2, count] = kind * CLASS_HIGH
            return count + 1

        return lax.fori_loop(bounds_ref[chunk, 0], bounds_ref[chunk, 1], list_class, count)

    count = lax.fori_loop(0, CHUNKS, list_chunk, 0)
    for spare in range(ABREAST):
        items_ref[0, count + spare] = 0
        items_ref[1, count + spare] = NOWHERE
        items_ref[2, count + spare] = 0
    steps = (count + ABREAST - 1) // ABREAST
    items_ref[0, ITEMS - 1] = steps

    def step(index, carry):
        totals = []
        for item in range(ABREAST):
            chunk = items_ref[0, index * ABREAST + item]
            key = high_ref[chunk] - items_ref[1, index * ABREAST + item].astype(F32)
            members = [row_is(key[r : r + 1], CLASS_HIGH) for r in range(8)]
            lows = low_hots(low_ref, chunk)
            left = []
            for comp in range(4):
                value = values[comp, chunk]
                top = value.astype(BF16).astype(F32)
                left.append(
                    jnp.concatenate(
                        [
                            jnp.where(members[r], spread(piece[r : r + 1], CLASS_HIGH), zero)
                            for piece in (top, value - top)
                            for r in range(8)
                        ],
                        axis=1,
                    )
                )
            totals.append(dot_nt(jnp.concatenate(left, axis=0), jnp.concatenate([lows, lows], axis=1)))
        for item in range(ABREAST):
            spot = pl.ds(pl.multiple_of(items_ref[2, index * ABREAST + item], CLASS_HIGH), CLASS_HIGH)
            for comp in range(4):
                out_ref[comp, spot, :] += totals[item][comp * CLASS_HIGH : (comp + 1) * CLASS_HIGH, :]
        return carry

    lax.fori_loop(0, steps, step, 0)
    out_ref[0] = jnp.minimum(out_ref[0], PHI_LIMIT)
    for copy in copies:
        copy.wait()
    for row in range(4 * CX):
        prior_ref[row * LAYERS : (row + 1) * LAYERS, :] = prior_row(solid_ref, drag_ref, row, slice(None))

    def pieces(row):
        if row >= 4 * CX:
            row -= 4 * CX
            spot = slice(row * LAYERS, (row + 1) * LAYERS)
            return prior_ref[spot, 0:128], prior_ref[spot, CY - 128 : CY]
        comp, x = row // CX, row % CX
        first = out_ref[comp, x * LAYERS : (x + 1) * LAYERS, 0:128]
        last = out_ref[comp, (CX + x) * LAYERS : (CX + x + 1) * LAYERS, LO - 128 : LO]
        return first, last

    fold_sides(pieces, first_ref, last_ref)


def deposit(received, solid, drag):
    vmem = pl.BlockSpec(memory_space=pltpu.VMEM)
    hbm = pl.BlockSpec(memory_space=pltpu.HBM)
    side = jax.ShapeDtypeStruct((SIDE_ROWS, 128), F32)
    index = jax.ShapeDtypeStruct((CHUNKS, 8, 128), F32)
    return pl.pallas_call(
        deposit_kernel,
        out_shape=(
            jax.ShapeDtypeStruct((4, HI, LO), F32),
            side,
            side,
            jax.ShapeDtypeStruct((4 * CX * LAYERS, CY), F32),
            index,
            index,
            jax.ShapeDtypeStruct((3, ITEMS), I32),
        ),
        in_specs=[vmem, hbm, hbm],
        out_specs=(vmem,) * 6 + (pl.BlockSpec(memory_space=pltpu.SMEM),),
        scratch_shapes=[
            pltpu.VMEM((LAYERS, CX, CY), F32),
            pltpu.VMEM((3, LAYERS, CX, CY), F32),
            pltpu.VMEM((4, CHUNKS, 8, 128), F32),
            pltpu.SMEM((CHUNKS, 2), I32),
            pltpu.SemaphoreType.DMA((2,)),
        ],
        compiler_params=pltpu.CompilerParams(vmem_limit_bytes=16 * MIB),
        name="deposit",
    )(received, solid, drag)


def gather_kernel(items_ref, *refs):
    own_refs, above_refs, below_refs = refs[0:GROUPS], refs[GROUPS : 2 * GROUPS], refs[2 * GROUPS : 3 * GROUPS]
    high_ref, low_ref, fields_any, out_ref, fields, tops, bottoms, found, sem = refs[3 * GROUPS :]
    top, bottom = at_edge("span")

    def smooth(comp, x):
        group, comp = comp // GROUP, comp % GROUP
        row = own_refs[group][pl.ds((comp * CX + x) * LAYERS, LAYERS), :]
        if x < RIM:
            spot = pl.ds((comp * RIM + x) * LAYERS, LAYERS)
            row = row + jnp.where(top, 0.0, above_refs[group][spot, :])
        if x >= CX - RIM:
            spot = pl.ds((comp * RIM + x - CX + RIM) * LAYERS, LAYERS)
            row = row + jnp.where(bottom, 0.0, below_refs[group][spot, :])
        return row

    for pair in range(0, CX, 2):
        void = [1.0 - smooth(0, x) for x in (pair, pair + 1)]
        for comp in range(4):
            rows = void if comp == 0 else [-smooth(comp, x) / v for x, v in zip((pair, pair + 1), void)]
            for x, row in zip((pair, pair + 1), rows):
                fields[comp, :, x, :] = row
            high, low = halves(jnp.concatenate(rows, axis=0))
            for half in range(2):
                spot = pl.ds((half * CX + pair) * LAYERS, 2 * LAYERS)
                tops[comp, spot, :] = high[:, half * LO : (half + 1) * LO]
                bottoms[comp, spot, :] = low[:, half * LO : (half + 1) * LO]
    copy = pltpu.make_async_copy(fields, fields_any, sem)
    copy.start()
    ids = lax.broadcasted_iota(I32, (CLASS_HIGH, 128), 0).astype(F32)

    found[...] = jnp.zeros_like(found)

    def step(index, carry):
        news = []
        for item in range(ABREAST):
            chunk = items_ref[0, index * ABREAST + item]
            key = high_ref[chunk] - items_ref[1, index * ABREAST + item].astype(F32)
            lows = low_hots(low_ref, chunk)
            spot = pl.ds(pl.multiple_of(items_ref[2, index * ABREAST + item], CLASS_HIGH), CLASS_HIGH)
            members = [ids == key[r : r + 1] for r in range(8)]
            table = [jnp.concatenate([part[comp, spot, :] for comp in range(4)], axis=0) for part in (tops, bottoms)]
            value = dot_nn(table[0], lows) + dot_nn(table[1], lows)
            new = []
            for comp in range(4):
                rows = value[comp * CLASS_HIGH : (comp + 1) * CLASS_HIGH]
                pieces = [
                    jnp.sum(jnp.where(members[r], rows[:, r * 128 : (r + 1) * 128], 0.0), axis=0, keepdims=True)
                    for r in range(8)
                ]
                new.append(jnp.concatenate(pieces, axis=0))
            news.append(new)
        for item in range(ABREAST):
            chunk = items_ref[0, index * ABREAST + item]
            for comp in range(4):
                found[comp, chunk] += news[item][comp]
        return carry

    lax.fori_loop(0, items_ref[0, ITEMS - 1], step, 0)
    for comp in range(4):
        slots = []
        for m in range(8):
            slots += swap_halves(found[comp, m], found[comp, m + 8])
        tile = jnp.transpose(jnp.concatenate(slots, axis=0))
        for half in range(2):
            out_ref[pl.ds(2 * comp + half, OWNERS, stride=BACK_ROWS), :] = tile[half * OWNERS : (half + 1) * OWNERS]
    copy.wait()


def gather(items, owns, aboves, belows, high, low):
    vmem = pl.BlockSpec(memory_space=pltpu.VMEM)
    return pl.pallas_call(
        gather_kernel,
        out_shape=(
            jax.ShapeDtypeStruct((4, LAYERS, CX, CY), F32),
            jax.ShapeDtypeStruct((OWNERS * BACK_ROWS, 128), F32),
        ),
        in_specs=[pl.BlockSpec(memory_space=pltpu.SMEM)] + [vmem] * (3 * GROUPS + 2),
        out_specs=(pl.BlockSpec(memory_space=pltpu.HBM), vmem),
        scratch_shapes=[
            pltpu.VMEM((4, LAYERS, CX, CY), F32),
            pltpu.VMEM((4, HI, LO), BF16),
            pltpu.VMEM((4, HI, LO), BF16),
            pltpu.VMEM((4, CHUNKS, 8, 128), F32),
            pltpu.SemaphoreType.DMA,
        ],
        compiler_params=pltpu.CompilerParams(vmem_limit_bytes=16 * MIB),
        name="gather",
    )(items, *owns, *aboves, *belows, high, low)


PICK_BLOCK = 4096


def pick_kernel(count_ref, slab_ref, position_ref, back_ref, out_ref, tops, bottoms):
    count = count_ref[0, 0]
    for comp in range(4):
        tile = jnp.concatenate(
            [back_ref[pl.ds(2 * comp + half, OWNERS, stride=BACK_ROWS), :] for half in range(2)], axis=1
        )
        high, low = halves(tile)
        tops[comp * OWNERS : (comp + 1) * OWNERS, :] = high
        bottoms[comp * OWNERS : (comp + 1) * OWNERS, :] = low

    def step(block, carry):
        start = pl.multiple_of(block * PICK_BLOCK, PICK_BLOCK)
        spot = pl.ds(start, PICK_BLOCK)
        lane = lax.broadcasted_iota(I32, (1, PICK_BLOCK), 1) + start
        slab = jnp.where(lane < count, slab_ref[0:1, spot], OWNERS)
        position_hot = one_hot(position_ref[0:1, spot], CAP)
        value = dot_nn(tops[...], position_hot) + dot_nn(bottoms[...], position_hot)
        member = lax.broadcasted_iota(I32, (OWNERS, PICK_BLOCK), 0) == slab
        for comp in range(4):
            piece = value[comp * OWNERS : (comp + 1) * OWNERS, :]
            out_ref[comp, 0:1, spot] = jnp.sum(jnp.where(member, piece, 0.0), axis=0, keepdims=True)
        return carry

    lax.fori_loop(0, PARTS // PICK_BLOCK, step, 0)


def pick(count, slab, position, back):
    vmem = pl.BlockSpec(memory_space=pltpu.VMEM)
    return pl.pallas_call(
        pick_kernel,
        out_shape=jax.ShapeDtypeStruct((4, 1, PARTS), F32),
        in_specs=[pl.BlockSpec(memory_space=pltpu.SMEM), vmem, vmem, vmem],
        out_specs=vmem,
        scratch_shapes=[pltpu.VMEM((4 * OWNERS, CAP), BF16)] * 2,
        name="pick",
        compiler_params=pltpu.CompilerParams(vmem_limit_bytes=8 * MIB),
    )(count, slab, position, back)


WIDE = CY + 128
RELAX_FLOPS = 40_000_000


def relax_kernel(
    base, target_ref, prior_ref, before, after, own_ref, up_ref, down_ref, state, source
):
    top, bottom = at_edge("span")
    first, last = at_edge("depth")
    near = lax.broadcasted_iota(I32, (LAYERS, 128), 1)
    is_before = (near >= 120) & jnp.logical_not(first)
    is_after = (near < 8) & jnp.logical_not(last)
    blank = jnp.zeros((LAYERS, WIDE), F32)
    for comp in range(GROUP):
        for x in range(RIM):
            state[comp, x] = blank
            state[comp, RIM + CX + x] = blank
        for x in range(CX):
            row = (base + comp) * CX + x
            for half in range(2):
                spot = pl.ds((half * CX + x) * LAYERS, LAYERS)
                source[comp, x, :, half * LO : (half + 1) * LO] = target_ref[base + comp, spot, :]
            source[comp, x, :, CY:WIDE] = unfold_side(row, before, after, is_before, is_after)
            state[comp, RIM + x, :, 0:CY] = prior_ref[row * LAYERS : (row + 1) * LAYERS, :]
            state[comp, RIM + x, :, CY:WIDE] = unfold_side(4 * CX + row, before, after, is_before, is_after)

    lane = lax.broadcasted_iota(I32, (LAYERS, WIDE), 1)
    outside = ((lane >= CY + 64) & first) | ((lane >= CY) & (lane < CY + 64) & last)
    factor = jnp.where(outside, 0.0, 0.2)
    above_factor = jnp.where(top, 0.0, factor)
    below_factor = jnp.where(bottom, 0.0, factor)

    def comp_step(comp, carry):
        for sweep in range(SWEEPS):
            rim = sweep + 1
            above, here = blank, blank
            for x in range(-rim, CX + rim):
                below = state[comp, x + 1 + RIM] if x + 1 < CX + sweep else blank
                total = above + below
                if -sweep <= x < CX + sweep:
                    total = total + pltpu.roll(here, 1, 1) + pltpu.roll(here, WIDE - 1, 1)
                if 0 <= x < CX:
                    total = total + source[comp, x]
                scale = above_factor if x < 0 else below_factor if x >= CX else factor
                state[comp, x + RIM] = total * scale
                above, here = here, below
        return carry

    lax.fori_loop(0, GROUP, comp_step, 0)
    for comp in range(GROUP):
        for x in range(CX):
            own_ref[pl.ds((comp * CX + x) * LAYERS, LAYERS), :] = state[comp, RIM + x, :, 0:CY]
        for x in range(RIM):
            spot = pl.ds((comp * RIM + x) * LAYERS, LAYERS)
            up_ref[spot, :] = state[comp, x, :, 0:CY]
            down_ref[spot, :] = state[comp, RIM + CX + x, :, 0:CY]


def relax(base, *arrays):
    vmem = pl.BlockSpec(memory_space=pltpu.VMEM)
    rim = jax.ShapeDtypeStruct((GROUP * RIM * LAYERS, CY), F32)
    return pl.pallas_call(
        functools.partial(relax_kernel, base),
        out_shape=(jax.ShapeDtypeStruct((GROUP * CX * LAYERS, CY), F32), rim, rim),
        in_specs=[vmem] * 4,
        out_specs=(vmem, vmem, vmem),
        scratch_shapes=[
            pltpu.VMEM((GROUP, CX + 2 * RIM, LAYERS, WIDE), F32),
            pltpu.VMEM((GROUP, CX, LAYERS, WIDE), F32),
        ],
        compiler_params=pltpu.CompilerParams(vmem_limit_bytes=12 * MIB),
        cost_estimate=pl.CostEstimate(flops=RELAX_FLOPS, bytes_accessed=4 * MIB, transcendentals=0),
        name=f"relax_{base}",
    )(*arrays)


def shifted(array, axis, step):
    count = lax.axis_size(axis)
    return lax.ppermute(array, axis, [(i, (i + step) % count) for i in range(count)])


def on_device(part_slab, part_cell, part_volume, part_drag, part_count, prior_solid, prior_drag):
    slab = part_slab.reshape(1, PARTS)
    in_hbm = [pltpu.with_memory_space_constraint(a, pltpu.HBM) for a in (slab, part_cell, part_volume, part_drag)]
    sent, position = pack(part_count, *in_hbm)
    received = lax.all_to_all(sent.reshape(OWNERS, 5, 2, 128), "span", 0, 0, tiled=True)
    received = received.reshape(OWNERS * ROWS, 128)
    target, first, last, prior, high, low, items = deposit(
        received, *[pltpu.with_memory_space_constraint(a, pltpu.HBM) for a in (prior_solid, prior_drag)]
    )
    before = shifted(last, "depth", 1)
    after = shifted(first, "depth", -1)
    owns, aboves, belows = [], [], []
    for group in range(GROUPS):
        own, up, down = relax(group * GROUP, target, prior, before, after)
        owns.append(own)
        aboves.append(shifted(down, "span", 1))
        belows.append(shifted(up, "span", -1))
    fields, returned = gather(items, owns, aboves, belows, high, low)
    back = lax.all_to_all(returned.reshape(OWNERS, BACK_ROWS, 128), "span", 0, 0, tiled=True)
    feedback = pick(part_count, slab, position, back.reshape(OWNERS * BACK_ROWS, 128))
    return fields, feedback


def solution(mesh):
    in_specs = (
        P("depth", "span", None),
        P("depth", "span"),
        P("depth", "span"),
        P(None, "depth", "span"),
        P("depth", "span"),
        P(None, "span", "depth"),
        P(None, None, "span", "depth"),
    )
    out_specs = (P(None, None, "span", "depth"), P(None, "depth", "span"))
    return jax.shard_map(on_device, mesh=mesh, in_specs=in_specs, out_specs=out_specs, check_vma=False)
```

```python
import functools

import jax
import jax.numpy as jnp
from jax import lax
from jax.experimental import pallas as pl
from jax.experimental.pallas import tpu as pltpu
from jax.sharding import PartitionSpec as P

F32, BF16, I32 = jnp.float32, jnp.bfloat16, jnp.int32
MIB = 1 << 20
OWNERS = 64
CAP = 256
LAYERS, CX, CY = 8, 16, 512
PARTS = 8192
HI, LO = 256, 256
ROWS = 2 * 5
BACK_ROWS = 8
SWEEPS = 6
RIM = SWEEPS
SIDE_ROWS = 2 * 4 * CX // 16 * LAYERS
PHI_LIMIT = 0.6


def halves(value):
    high = value.astype(BF16)
    return high, (value - high.astype(F32)).astype(BF16)


def spread(row, size):
    n = row.shape[1]
    packed = jnp.broadcast_to(row, (16, n)).astype(BF16)
    return jnp.broadcast_to(packed[None], (size // 16, 16, n)).reshape(size, n)


def index_rows(size, n):
    return lax.broadcasted_iota(I32, (size, n), 0).astype(F32).astype(BF16)


def row_is(row, size):
    return index_rows(size, row.shape[1]) == spread(row, size)


def one_hot(row, size):
    return jnp.where(row_is(row, size), jnp.ones((), BF16), jnp.zeros((), BF16))


def dot_nt(left, right):
    return lax.dot_general(left, right, (((1,), (1,)), ((), ())), preferred_element_type=F32)


def dot_nn(left, right):
    return lax.dot_general(left, right, (((1,), (0,)), ((), ())), preferred_element_type=F32)


def at_edge(axis):
    place = lax.axis_index(axis)
    return place == 0, place == lax.axis_size(axis) - 1


def fold_sides(pieces, left_ref, right_ref):
    lane = lax.broadcasted_iota(I32, (LAYERS, 128), 1)
    for group in range(SIDE_ROWS // LAYERS):
        left = jnp.zeros((LAYERS, 128), F32)
        right = jnp.zeros((LAYERS, 128), F32)
        for place in range(16):
            first, last = pieces(group * 16 + place)
            here = (lane >= 8 * place) & (lane < 8 * place + 8)
            left = jnp.where(here, pltpu.roll(first, 8 * place, 1) if place else first, left)
            shift = (8 * place + 8) % 128
            right = jnp.where(here, pltpu.roll(last, shift, 1) if shift else last, right)
        left_ref[group * LAYERS : (group + 1) * LAYERS, :] = left
        right_ref[group * LAYERS : (group + 1) * LAYERS, :] = right


def unfold_side(row, before_ref, after_ref, is_before, is_after):
    group, place = row // 16, row % 16
    after = after_ref[group * LAYERS : (group + 1) * LAYERS, :]
    before = before_ref[group * LAYERS : (group + 1) * LAYERS, :]
    after = pltpu.roll(after, 128 - 8 * place, 1) if place else after
    shift = (120 - 8 * place) % 128
    before = pltpu.roll(before, shift, 1) if shift else before
    return jnp.where(is_after, after, jnp.where(is_before, before, 0.0))


def prior_row(solid_ref, drag_ref, row, lanes):
    comp, x = row // CX, row % CX
    return solid_ref[:, x, lanes] if comp == 0 else drag_ref[comp - 1, :, x, lanes]


PACK_BLOCK = 4096
SUB = 256
CLASSES = 4


def pack_kernel(
    count_ref, slab_any, cell_any, volume_any, drag_any, out_ref, position_ref,
    slab_ref, cell_ref, volume_ref, drag_ref, acc, sems,
):
    sources, targets = (slab_any, cell_any, volume_any, drag_any), (slab_ref, cell_ref, volume_ref, drag_ref)
    copies = [pltpu.make_async_copy(f, t, sems.at[i]) for i, (f, t) in enumerate(zip(sources, targets))]
    for copy in copies:
        copy.start()
    count = count_ref[0, 0]
    acc[...] = jnp.zeros_like(acc)
    earlier = lax.broadcasted_iota(I32, (SUB, SUB), 0)
    later = lax.broadcasted_iota(I32, (SUB, SUB), 1)
    upper = jnp.where(earlier <= later, 1.0, 0.0).astype(BF16)
    for copy in copies[:2]:
        copy.wait()

    def live_slab(start, size):
        lane = lax.broadcasted_iota(I32, (1, size), 1) + start
        return jnp.where(lane < count, slab_ref[0:1, pl.ds(start, size)], CLASSES * OWNERS)

    def classes(start, size):
        cell = cell_ref[0:1, pl.ds(start, size)]
        return (lax.shift_right_logical(cell, 8) & 1) * 2 + (lax.shift_right_logical(cell, 12) & 1)

    def count_step(block, counts):
        start = pl.multiple_of(block * PACK_BLOCK, PACK_BLOCK)
        member = one_hot(live_slab(start, PACK_BLOCK).astype(F32), OWNERS)
        kind = one_hot(classes(start, PACK_BLOCK).astype(F32), 128)
        return counts + dot_nt(member, kind)

    counts = lax.fori_loop(0, PARTS // PACK_BLOCK, count_step, jnp.zeros((OWNERS, 128), F32))
    numbers = [jnp.broadcast_to(counts[:, kind : kind + 1], (OWNERS, 128)) for kind in range(CLASSES)]
    for copy in copies[2:]:
        copy.wait()
    starts, end = [], jnp.zeros((OWNERS, 128), F32)
    for kind in range(CLASSES):
        rest = sum(numbers[kind:])
        starts.append(jnp.maximum(end, jnp.minimum(float(kind * CAP // CLASSES), CAP - rest)))
        end = starts[-1] + numbers[kind]

    def step(block, offset):
        hots, lefts = [], []
        for sub in range(PACK_BLOCK // SUB):
            start = pl.multiple_of(block * PACK_BLOCK + sub * SUB, SUB)
            spot = pl.ds(start, SUB)
            slab = live_slab(start, SUB)
            member = row_is(slab.astype(F32), OWNERS)
            sorted_one = one_hot((slab + classes(start, SUB) * OWNERS).astype(F32), CLASSES * OWNERS)
            ranks = dot_nn(sorted_one, upper)
            place = ranks + jnp.concatenate([offset, offset], axis=1)
            position = jnp.sum(place * sorted_one.astype(F32), axis=0, keepdims=True) - 1.0
            offset = offset + jnp.broadcast_to(ranks[:, SUB - 1 : SUB], offset.shape)
            position_ref[0:1, spot] = position
            hots.append(one_hot(position, CAP))
            cell = cell_ref[0:1, spot]
            cell_high = lax.shift_right_logical(cell, 8)
            rows = [cell_high.astype(F32), (cell - cell_high * 256).astype(F32)]
            for value in [volume_ref[0:1, spot]] + [drag_ref[k, 0:1, spot] for k in range(3)]:
                high = value.astype(BF16).astype(F32)
                rows += [high, value - high]
            zero = jnp.zeros((), BF16)
            lefts.append(
                jnp.concatenate([jnp.where(member, spread(row, OWNERS), zero) for row in rows], axis=0)
            )
        acc[...] += dot_nt(jnp.concatenate(lefts, axis=1), jnp.concatenate(hots, axis=1))
        return offset

    lax.fori_loop(0, PARTS // PACK_BLOCK, step, jnp.concatenate(starts, axis=0))
    for comp in range(5):
        high = acc[2 * comp * OWNERS : (2 * comp + 1) * OWNERS, :]
        low = acc[(2 * comp + 1) * OWNERS : (2 * comp + 2) * OWNERS, :]
        whole = high * 256.0 + low if comp == 0 else high + low
        for half in range(2):
            out_ref[pl.ds(2 * comp + half, OWNERS, stride=ROWS), :] = whole[:, half * 128 : (half + 1) * 128]


def pack(count, slab, cell, volume, drag):
    vmem = pl.BlockSpec(memory_space=pltpu.VMEM)
    hbm = pl.BlockSpec(memory_space=pltpu.HBM)
    return pl.pallas_call(
        pack_kernel,
        out_shape=(
            jax.ShapeDtypeStruct((OWNERS * ROWS, 128), F32),
            jax.ShapeDtypeStruct((1, PARTS), F32),
        ),
        in_specs=[pl.BlockSpec(memory_space=pltpu.SMEM), hbm, hbm, hbm, hbm],
        out_specs=(vmem, vmem),
        scratch_shapes=[
            pltpu.VMEM((1, PARTS), I32),
            pltpu.VMEM((1, PARTS), I32),
            pltpu.VMEM((1, PARTS), F32),
            pltpu.VMEM((3, 1, PARTS), F32),
            pltpu.VMEM((10 * OWNERS, CAP), F32),
            pltpu.SemaphoreType.DMA((4,)),
        ],
        compiler_params=pltpu.CompilerParams(vmem_limit_bytes=8 * MIB),
        name="pack",
    )(count, slab, cell, volume, drag)


CHUNKS, CHUNK = 16, 1024
CLASS_HIGH = HI // CLASSES
ABREAST = 4
ITEMS = CHUNKS * CLASSES + 8
NOWHERE = 1024


def swap_halves(first, second):
    lane = lax.broadcasted_iota(I32, (8, 128), 1)
    return (
        jnp.where(lane < 64, first, pltpu.roll(second, 64, 1)),
        jnp.where(lane < 64, pltpu.roll(first, 64, 1), second),
    )


def low_hots(low_ref, chunk):
    return jnp.concatenate([one_hot(low_ref[chunk, r : r + 1, :], LO) for r in range(8)], axis=1)


def deposit_kernel(
    recv_ref, solid_any, drag_any,
    out_ref, first_ref, last_ref, prior_ref, high_ref, low_ref, items_ref,
    solid_ref, drag_ref, values, bounds_ref, sems,
):
    copies = [
        pltpu.make_async_copy(solid_any, solid_ref, sems.at[0]),
        pltpu.make_async_copy(drag_any, drag_ref, sems.at[1]),
    ]
    for copy in copies:
        copy.start()
    out_ref[...] = jnp.zeros_like(out_ref)
    zero = jnp.zeros((), BF16)

    def chunked(comp):
        tile = jnp.concatenate([recv_ref[pl.ds(2 * comp + half, OWNERS, stride=ROWS), :] for half in range(2)], axis=0)
        slots = jnp.transpose(tile)
        pairs = [swap_halves(slots[16 * m : 16 * m + 8], slots[16 * m + 8 : 16 * m + 16]) for m in range(8)]
        return [pair[0] for pair in pairs] + [pair[1] for pair in pairs]

    volumes = chunked(1)
    for chunk, cell in enumerate(chunked(0)):
        cell = cell.astype(I32)
        layer = lax.shift_right_logical(cell, 13)
        high = ((lax.shift_right_logical(cell, 8) & 1) * 16 + (lax.shift_right_logical(cell, 9) & 15)) * 8 + layer
        high_ref[chunk] = high.astype(F32)
        low_ref[chunk] = (cell & 255).astype(F32)
        values[0, chunk] = volumes[chunk]
        live = volumes[chunk] > 0.0
        kind = lax.shift_right_logical(high, 6).astype(F32)
        bounds_ref[chunk, 0] = jnp.min(jnp.where(live, kind, float(CLASSES))).astype(I32)
        bounds_ref[chunk, 1] = jnp.max(jnp.where(live, kind, -1.0)).astype(I32) + 1
    for comp in range(1, 4):
        for chunk, value in enumerate(chunked(comp + 1)):
            values[comp, chunk] = value

    def list_chunk(chunk, count):
        def list_class(kind, count):
            items_ref[0, count] = chunk
            items_ref[1, count] = kind * CLASS_HIGH
            items_ref[2, count] = kind * CLASS_HIGH
            return count + 1

        return lax.fori_loop(bounds_ref[chunk, 0], bounds_ref[chunk, 1], list_class, count)

    count = lax.fori_loop(0, CHUNKS, list_chunk, 0)
    for spare in range(ABREAST):
        items_ref[0, count + spare] = 0
        items_ref[1, count + spare] = NOWHERE
        items_ref[2, count + spare] = 0
    steps = (count + ABREAST - 1) // ABREAST
    items_ref[0, ITEMS - 1] = steps

    def step(index, carry):
        totals = []
        for item in range(ABREAST):
            chunk = items_ref[0, index * ABREAST + item]
            key = high_ref[chunk] - items_ref[1, index * ABREAST + item].astype(F32)
            members = [row_is(key[r : r + 1], CLASS_HIGH) for r in range(8)]
            lows = low_hots(low_ref, chunk)
            left = []
            for comp in range(4):
                value = values[comp, chunk]
                top = value.astype(BF16).astype(F32)
                left.append(
                    jnp.concatenate(
                        [
                            jnp.where(members[r], spread(piece[r : r + 1], CLASS_HIGH), zero)
                            for piece in (top, value - top)
                            for r in range(8)
                        ],
                        axis=1,
                    )
                )
            totals.append(dot_nt(jnp.concatenate(left, axis=0), jnp.concatenate([lows, lows], axis=1)))
        for item in range(ABREAST):
            spot = pl.ds(pl.multiple_of(items_ref[2, index * ABREAST + item], CLASS_HIGH), CLASS_HIGH)
            for comp in range(4):
                out_ref[comp, spot, :] += totals[item][comp * CLASS_HIGH : (comp + 1) * CLASS_HIGH, :]
        return carry

    lax.fori_loop(0, steps, step, 0)
    out_ref[0] = jnp.minimum(out_ref[0], PHI_LIMIT)
    for copy in copies:
        copy.wait()
    for row in range(4 * CX):
        prior_ref[row * LAYERS : (row + 1) * LAYERS, :] = prior_row(solid_ref, drag_ref, row, slice(None))

    def pieces(row):
        if row >= 4 * CX:
            row -= 4 * CX
            spot = slice(row * LAYERS, (row + 1) * LAYERS)
            return prior_ref[spot, 0:128], prior_ref[spot, CY - 128 : CY]
        comp, x = row // CX, row % CX
        first = out_ref[comp, x * LAYERS : (x + 1) * LAYERS, 0:128]
        last = out_ref[comp, (CX + x) * LAYERS : (CX + x + 1) * LAYERS, LO - 128 : LO]
        return first, last

    fold_sides(pieces, first_ref, last_ref)


def deposit(received, solid, drag):
    vmem = pl.BlockSpec(memory_space=pltpu.VMEM)
    hbm = pl.BlockSpec(memory_space=pltpu.HBM)
    side = jax.ShapeDtypeStruct((SIDE_ROWS, 128), F32)
    index = jax.ShapeDtypeStruct((CHUNKS, 8, 128), F32)
    return pl.pallas_call(
        deposit_kernel,
        out_shape=(
            jax.ShapeDtypeStruct((4, HI, LO), F32),
            side,
            side,
            jax.ShapeDtypeStruct((4 * CX * LAYERS, CY), F32),
            index,
            index,
            jax.ShapeDtypeStruct((3, ITEMS), I32),
        ),
        in_specs=[vmem, hbm, hbm],
        out_specs=(vmem,) * 6 + (pl.BlockSpec(memory_space=pltpu.SMEM),),
        scratch_shapes=[
            pltpu.VMEM((LAYERS, CX, CY), F32),
            pltpu.VMEM((3, LAYERS, CX, CY), F32),
            pltpu.VMEM((4, CHUNKS, 8, 128), F32),
            pltpu.SMEM((CHUNKS, 2), I32),
            pltpu.SemaphoreType.DMA((2,)),
        ],
        compiler_params=pltpu.CompilerParams(vmem_limit_bytes=16 * MIB),
        name="deposit",
    )(received, solid, drag)


def gather_kernel(
    items_ref, own_ref, above_ref, below_ref, high_ref, low_ref, fields_any, out_ref,
    fields, tops, bottoms, found, sem,
):
    top, bottom = at_edge("span")

    def smooth(comp, x):
        row = own_ref[pl.ds((comp * CX + x) * LAYERS, LAYERS), :]
        if x < RIM:
            spot = pl.ds((comp * RIM + x) * LAYERS, LAYERS)
            row = row + jnp.where(top, 0.0, above_ref[spot, :])
        if x >= CX - RIM:
            spot = pl.ds((comp * RIM + x - CX + RIM) * LAYERS, LAYERS)
            row = row + jnp.where(bottom, 0.0, below_ref[spot, :])
        return row

    for pair in range(0, CX, 2):
        void = [1.0 - smooth(0, x) for x in (pair, pair + 1)]
        for comp in range(4):
            rows = void if comp == 0 else [-smooth(comp, x) / v for x, v in zip((pair, pair + 1), void)]
            for x, row in zip((pair, pair + 1), rows):
                fields[comp, :, x, :] = row
            high, low = halves(jnp.concatenate(rows, axis=0))
            for half in range(2):
                spot = pl.ds((half * CX + pair) * LAYERS, 2 * LAYERS)
                tops[comp, spot, :] = high[:, half * LO : (half + 1) * LO]
                bottoms[comp, spot, :] = low[:, half * LO : (half + 1) * LO]
    copy = pltpu.make_async_copy(fields, fields_any, sem)
    copy.start()
    ids = lax.broadcasted_iota(I32, (CLASS_HIGH, 128), 0).astype(F32)

    found[...] = jnp.zeros_like(found)

    def step(index, carry):
        news = []
        for item in range(ABREAST):
            chunk = items_ref[0, index * ABREAST + item]
            key = high_ref[chunk] - items_ref[1, index * ABREAST + item].astype(F32)
            lows = low_hots(low_ref, chunk)
            spot = pl.ds(pl.multiple_of(items_ref[2, index * ABREAST + item], CLASS_HIGH), CLASS_HIGH)
            members = [ids == key[r : r + 1] for r in range(8)]
            table = [jnp.concatenate([part[comp, spot, :] for comp in range(4)], axis=0) for part in (tops, bottoms)]
            value = dot_nn(table[0], lows) + dot_nn(table[1], lows)
            new = []
            for comp in range(4):
                rows = value[comp * CLASS_HIGH : (comp + 1) * CLASS_HIGH]
                pieces = [
                    jnp.sum(jnp.where(members[r], rows[:, r * 128 : (r + 1) * 128], 0.0), axis=0, keepdims=True)
                    for r in range(8)
                ]
                new.append(jnp.concatenate(pieces, axis=0))
            news.append(new)
        for item in range(ABREAST):
            chunk = items_ref[0, index * ABREAST + item]
            for comp in range(4):
                found[comp, chunk] += news[item][comp]
        return carry

    lax.fori_loop(0, items_ref[0, ITEMS - 1], step, 0)
    for comp in range(4):
        slots = []
        for m in range(8):
            slots += swap_halves(found[comp, m], found[comp, m + 8])
        tile = jnp.transpose(jnp.concatenate(slots, axis=0))
        for half in range(2):
            out_ref[pl.ds(2 * comp + half, OWNERS, stride=BACK_ROWS), :] = tile[half * OWNERS : (half + 1) * OWNERS]
    copy.wait()


def gather(items, *arrays):
    vmem = pl.BlockSpec(memory_space=pltpu.VMEM)
    return pl.pallas_call(
        gather_kernel,
        out_shape=(
            jax.ShapeDtypeStruct((4, LAYERS, CX, CY), F32),
            jax.ShapeDtypeStruct((OWNERS * BACK_ROWS, 128), F32),
        ),
        in_specs=[pl.BlockSpec(memory_space=pltpu.SMEM)] + [vmem] * 5,
        out_specs=(pl.BlockSpec(memory_space=pltpu.HBM), vmem),
        scratch_shapes=[
            pltpu.VMEM((4, LAYERS, CX, CY), F32),
            pltpu.VMEM((4, HI, LO), BF16),
            pltpu.VMEM((4, HI, LO), BF16),
            pltpu.VMEM((4, CHUNKS, 8, 128), F32),
            pltpu.SemaphoreType.DMA,
        ],
        compiler_params=pltpu.CompilerParams(vmem_limit_bytes=16 * MIB),
        name="gather",
    )(items, *arrays)


PICK_BLOCK = 4096


def pick_kernel(count_ref, slab_ref, position_ref, back_ref, out_ref, tops, bottoms):
    count = count_ref[0, 0]
    for comp in range(4):
        tile = jnp.concatenate(
            [back_ref[pl.ds(2 * comp + half, OWNERS, stride=BACK_ROWS), :] for half in range(2)], axis=1
        )
        high, low = halves(tile)
        tops[comp * OWNERS : (comp + 1) * OWNERS, :] = high
        bottoms[comp * OWNERS : (comp + 1) * OWNERS, :] = low

    def step(block, carry):
        start = pl.multiple_of(block * PICK_BLOCK, PICK_BLOCK)
        spot = pl.ds(start, PICK_BLOCK)
        lane = lax.broadcasted_iota(I32, (1, PICK_BLOCK), 1) + start
        slab = jnp.where(lane < count, slab_ref[0:1, spot], OWNERS)
        position_hot = one_hot(position_ref[0:1, spot], CAP)
        value = dot_nn(tops[...], position_hot) + dot_nn(bottoms[...], position_hot)
        member = lax.broadcasted_iota(I32, (OWNERS, PICK_BLOCK), 0) == slab
        for comp in range(4):
            piece = value[comp * OWNERS : (comp + 1) * OWNERS, :]
            out_ref[comp, 0:1, spot] = jnp.sum(jnp.where(member, piece, 0.0), axis=0, keepdims=True)
        return carry

    lax.fori_loop(0, PARTS // PICK_BLOCK, step, 0)


def pick(count, slab, position, back):
    vmem = pl.BlockSpec(memory_space=pltpu.VMEM)
    return pl.pallas_call(
        pick_kernel,
        out_shape=jax.ShapeDtypeStruct((4, 1, PARTS), F32),
        in_specs=[pl.BlockSpec(memory_space=pltpu.SMEM), vmem, vmem, vmem],
        out_specs=vmem,
        scratch_shapes=[pltpu.VMEM((4 * OWNERS, CAP), BF16)] * 2,
        name="pick",
        compiler_params=pltpu.CompilerParams(vmem_limit_bytes=8 * MIB),
    )(count, slab, position, back)


WIDE = CY + 128
RELAX_FLOPS = 40_000_000


def relax_kernel(for_rim, target_ref, prior_ref, before, after, *refs):
    outs, (state, source) = refs[:-2], refs[-2:]
    top, bottom = at_edge("span")
    first, last = at_edge("depth")
    near = lax.broadcasted_iota(I32, (LAYERS, 128), 1)
    is_before = (near >= 120) & jnp.logical_not(first)
    is_after = (near < 8) & jnp.logical_not(last)
    blank = jnp.zeros((LAYERS, WIDE), F32)
    for comp in range(4):
        for x in range(CX):
            if for_rim and RIM <= x < CX - RIM:
                continue
            row = comp * CX + x
            for half in range(2):
                spot = pl.ds((half * CX + x) * LAYERS, LAYERS)
                source[comp, x, :, half * LO : (half + 1) * LO] = target_ref[comp, spot, :]
            source[comp, x, :, CY:WIDE] = unfold_side(row, before, after, is_before, is_after)
            state[comp, RIM + x, :, 0:CY] = prior_ref[row * LAYERS : (row + 1) * LAYERS, :]
            state[comp, RIM + x, :, CY:WIDE] = unfold_side(4 * CX + row, before, after, is_before, is_after)

    lane = lax.broadcasted_iota(I32, (LAYERS, WIDE), 1)
    outside = ((lane >= CY + 64) & first) | ((lane >= CY) & (lane < CY + 64) & last)
    factor = jnp.where(outside, 0.0, 0.2)
    above_factor = jnp.where(top, 0.0, factor)
    below_factor = jnp.where(bottom, 0.0, factor)

    def sweep_rows(comp, sweep, low, high):
        def old(x):
            return state[comp, x + RIM] if -sweep < x < CX - 1 + sweep else blank

        above, here = old(low - 1), old(low)
        for x in range(low, high + 1):
            below = old(x + 1)
            total = above + below
            if -sweep < x < CX - 1 + sweep:
                total = total + pltpu.roll(here, 1, 1) + pltpu.roll(here, WIDE - 1, 1)
            if 0 <= x < CX:
                total = total + source[comp, x]
            scale = above_factor if x < 0 else below_factor if x >= CX else factor
            state[comp, x + RIM] = total * scale
            above, here = here, below

    def comp_step(comp, carry):
        for sweep in range(1, SWEEPS + 1):
            if for_rim:
                sweep_rows(comp, sweep, -sweep, RIM - 1 - sweep)
                sweep_rows(comp, sweep, CX - RIM + sweep, CX - 1 + sweep)
            else:
                reach = min(sweep, SWEEPS - sweep)
                sweep_rows(comp, sweep, -reach, CX - 1 + reach)
        return carry

    lax.fori_loop(0, 4, comp_step, 0)
    for comp in range(4):
        if for_rim:
            for x in range(RIM):
                spot = pl.ds((comp * RIM + x) * LAYERS, LAYERS)
                outs[0][spot, :] = state[comp, x, :, 0:CY]
                outs[1][spot, :] = state[comp, RIM + CX + x, :, 0:CY]
        else:
            for x in range(CX):
                outs[0][pl.ds((comp * CX + x) * LAYERS, LAYERS), :] = state[comp, RIM + x, :, 0:CY]


def relax(for_rim, *arrays):
    vmem = pl.BlockSpec(memory_space=pltpu.VMEM)
    rim = jax.ShapeDtypeStruct((4 * RIM * LAYERS, CY), F32)
    own = jax.ShapeDtypeStruct((4 * CX * LAYERS, CY), F32)
    return pl.pallas_call(
        functools.partial(relax_kernel, for_rim),
        out_shape=(rim, rim) if for_rim else own,
        in_specs=[vmem] * 4,
        out_specs=(vmem, vmem) if for_rim else vmem,
        scratch_shapes=[
            pltpu.VMEM((4, CX + 2 * RIM, LAYERS, WIDE), F32),
            pltpu.VMEM((4, CX, LAYERS, WIDE), F32),
        ],
        compiler_params=pltpu.CompilerParams(vmem_limit_bytes=12 * MIB),
        cost_estimate=pl.CostEstimate(flops=RELAX_FLOPS, bytes_accessed=4 * MIB, transcendentals=0),
        name="relax_rim" if for_rim else "relax_own",
    )(*arrays)


def shifted(array, axis, step):
    count = lax.axis_size(axis)
    return lax.ppermute(array, axis, [(i, (i + step) % count) for i in range(count)])


def on_device(part_slab, part_cell, part_volume, part_drag, part_count, prior_solid, prior_drag):
    slab = part_slab.reshape(1, PARTS)
    in_hbm = [pltpu.with_memory_space_constraint(a, pltpu.HBM) for a in (slab, part_cell, part_volume, part_drag)]
    sent, position = pack(part_count, *in_hbm)
    received = lax.all_to_all(sent.reshape(OWNERS, 5, 2, 128), "span", 0, 0, tiled=True)
    received = received.reshape(OWNERS * ROWS, 128)
    target, first, last, prior, high, low, items = deposit(
        received, *[pltpu.with_memory_space_constraint(a, pltpu.HBM) for a in (prior_solid, prior_drag)]
    )
    before = shifted(last, "depth", 1)
    after = shifted(first, "depth", -1)
    arrays = (target, prior, before, after)
    up, down = relax(True, *arrays)
    from_above = shifted(down, "span", 1)
    from_below = shifted(up, "span", -1)
    own = relax(False, *arrays)
    fields, returned = gather(items, own, from_above, from_below, high, low)
    back = lax.all_to_all(returned.reshape(OWNERS, BACK_ROWS, 128), "span", 0, 0, tiled=True)
    feedback = pick(part_count, slab, position, back.reshape(OWNERS * BACK_ROWS, 128))
    return fields, feedback


def solution(mesh):
    in_specs = (
        P("depth", "span", None),
        P("depth", "span"),
        P("depth", "span"),
        P(None, "depth", "span"),
        P("depth", "span"),
        P(None, "span", "depth"),
        P(None, None, "span", "depth"),
    )
    out_specs = (P(None, None, "span", "depth"), P(None, "depth", "span"))
    return jax.shard_map(on_device, mesh=mesh, in_specs=in_specs, out_specs=out_specs, check_vma=False)
```

```python
import functools

import jax
import jax.numpy as jnp
from jax import lax
from jax.experimental import pallas as pl
from jax.experimental.pallas import tpu as pltpu
from jax.sharding import PartitionSpec as P

F32, BF16, I32 = jnp.float32, jnp.bfloat16, jnp.int32
MIB = 1 << 20
OWNERS = 64
CAP = 256
LAYERS, CX, CY = 8, 16, 512
PARTS = 8192
HI, LO = 256, 256
ROWS = 2 * 5
BACK_ROWS = 8
SWEEPS = 6
RIM = SWEEPS
SIDE_ROWS = 2 * 4 * CX // 16 * LAYERS
PHI_LIMIT = 0.6


def halves(value):
    high = value.astype(BF16)
    return high, (value - high.astype(F32)).astype(BF16)


def spread(row, size):
    n = row.shape[1]
    packed = jnp.broadcast_to(row, (16, n)).astype(BF16)
    return jnp.broadcast_to(packed[None], (size // 16, 16, n)).reshape(size, n)


def index_rows(size, n):
    return lax.broadcasted_iota(I32, (size, n), 0).astype(F32).astype(BF16)


def row_is(row, size):
    return index_rows(size, row.shape[1]) == spread(row, size)


def one_hot(row, size):
    return jnp.where(row_is(row, size), jnp.ones((), BF16), jnp.zeros((), BF16))


def dot_nt(left, right):
    return lax.dot_general(left, right, (((1,), (1,)), ((), ())), preferred_element_type=F32)


def dot_nn(left, right):
    return lax.dot_general(left, right, (((1,), (0,)), ((), ())), preferred_element_type=F32)


def at_edge(axis):
    place = lax.axis_index(axis)
    return place == 0, place == lax.axis_size(axis) - 1


def fold_sides(pieces, left_ref, right_ref):
    lane = lax.broadcasted_iota(I32, (LAYERS, 128), 1)
    for group in range(SIDE_ROWS // LAYERS):
        left = jnp.zeros((LAYERS, 128), F32)
        right = jnp.zeros((LAYERS, 128), F32)
        for place in range(16):
            first, last = pieces(group * 16 + place)
            here = (lane >= 8 * place) & (lane < 8 * place + 8)
            left = jnp.where(here, pltpu.roll(first, 8 * place, 1) if place else first, left)
            shift = (8 * place + 8) % 128
            right = jnp.where(here, pltpu.roll(last, shift, 1) if shift else last, right)
        left_ref[group * LAYERS : (group + 1) * LAYERS, :] = left
        right_ref[group * LAYERS : (group + 1) * LAYERS, :] = right


def unfold_side(row, before_ref, after_ref, is_before, is_after):
    group, place = row // 16, row % 16
    after = after_ref[group * LAYERS : (group + 1) * LAYERS, :]
    before = before_ref[group * LAYERS : (group + 1) * LAYERS, :]
    after = pltpu.roll(after, 128 - 8 * place, 1) if place else after
    shift = (120 - 8 * place) % 128
    before = pltpu.roll(before, shift, 1) if shift else before
    return jnp.where(is_after, after, jnp.where(is_before, before, 0.0))


def prior_row(solid_ref, drag_ref, row, lanes):
    comp, x = row // CX, row % CX
    return solid_ref[:, x, lanes] if comp == 0 else drag_ref[comp - 1, :, x, lanes]


PACK_BLOCK = 4096
SUB = 256
CLASSES = 8


def pack_kernel(
    count_ref, slab_any, cell_any, volume_any, drag_any, out_ref, position_ref,
    slab_ref, cell_ref, volume_ref, drag_ref, acc, sems,
):
    sources, targets = (slab_any, cell_any, volume_any, drag_any), (slab_ref, cell_ref, volume_ref, drag_ref)
    copies = [pltpu.make_async_copy(f, t, sems.at[i]) for i, (f, t) in enumerate(zip(sources, targets))]
    for copy in copies:
        copy.start()
    count = count_ref[0, 0]
    acc[...] = jnp.zeros_like(acc)
    earlier = lax.broadcasted_iota(I32, (SUB, SUB), 0)
    later = lax.broadcasted_iota(I32, (SUB, SUB), 1)
    upper = jnp.where(earlier <= later, 1.0, 0.0).astype(BF16)
    for copy in copies[:2]:
        copy.wait()

    def live_slab(start, size):
        lane = lax.broadcasted_iota(I32, (1, size), 1) + start
        return jnp.where(lane < count, slab_ref[0:1, pl.ds(start, size)], CLASSES * OWNERS)

    def classes(start, size):
        cell = cell_ref[0:1, pl.ds(start, size)]
        return (lax.shift_right_logical(cell, 8) & 1) * 4 + (lax.shift_right_logical(cell, 11) & 3)

    def count_step(block, counts):
        start = pl.multiple_of(block * PACK_BLOCK, PACK_BLOCK)
        member = one_hot(live_slab(start, PACK_BLOCK).astype(F32), OWNERS)
        kind = one_hot(classes(start, PACK_BLOCK).astype(F32), 128)
        return counts + dot_nt(member, kind)

    counts = lax.fori_loop(0, PARTS // PACK_BLOCK, count_step, jnp.zeros((OWNERS, 128), F32))
    numbers = [jnp.broadcast_to(counts[:, kind : kind + 1], (OWNERS, 128)) for kind in range(CLASSES)]
    for copy in copies[2:]:
        copy.wait()
    starts, end = [], jnp.zeros((OWNERS, 128), F32)
    for kind in range(CLASSES):
        rest = sum(numbers[kind:])
        starts.append(jnp.maximum(end, jnp.minimum(float(kind * CAP // CLASSES), CAP - rest)))
        end = starts[-1] + numbers[kind]

    def step(block, offset):
        hots, lefts = [], []
        for sub in range(PACK_BLOCK // SUB):
            start = pl.multiple_of(block * PACK_BLOCK + sub * SUB, SUB)
            spot = pl.ds(start, SUB)
            slab = live_slab(start, SUB)
            member = row_is(slab.astype(F32), OWNERS)
            order = slab + classes(start, SUB) * OWNERS
            sorted_one = jnp.concatenate(
                [one_hot((order - base).astype(F32), 256) for base in range(0, CLASSES * OWNERS, 256)], axis=0
            )
            ranks = dot_nn(sorted_one, upper)
            place = ranks + jnp.concatenate([offset, offset], axis=1)
            position = jnp.sum(place * sorted_one.astype(F32), axis=0, keepdims=True) - 1.0
            offset = offset + jnp.broadcast_to(ranks[:, SUB - 1 : SUB], offset.shape)
            position_ref[0:1, spot] = position
            hots.append(one_hot(position, CAP))
            cell = cell_ref[0:1, spot]
            cell_high = lax.shift_right_logical(cell, 8)
            rows = [cell_high.astype(F32), (cell - cell_high * 256).astype(F32)]
            for value in [volume_ref[0:1, spot]] + [drag_ref[k, 0:1, spot] for k in range(3)]:
                high = value.astype(BF16).astype(F32)
                rows += [high, value - high]
            zero = jnp.zeros((), BF16)
            lefts.append(
                jnp.concatenate([jnp.where(member, spread(row, OWNERS), zero) for row in rows], axis=0)
            )
        acc[...] += dot_nt(jnp.concatenate(lefts, axis=1), jnp.concatenate(hots, axis=1))
        return offset

    lax.fori_loop(0, PARTS // PACK_BLOCK, step, jnp.concatenate(starts, axis=0))
    for comp in range(5):
        high = acc[2 * comp * OWNERS : (2 * comp + 1) * OWNERS, :]
        low = acc[(2 * comp + 1) * OWNERS : (2 * comp + 2) * OWNERS, :]
        whole = high * 256.0 + low if comp == 0 else high + low
        for half in range(2):
            out_ref[pl.ds(2 * comp + half, OWNERS, stride=ROWS), :] = whole[:, half * 128 : (half + 1) * 128]


def pack(count, slab, cell, volume, drag):
    vmem = pl.BlockSpec(memory_space=pltpu.VMEM)
    hbm = pl.BlockSpec(memory_space=pltpu.HBM)
    return pl.pallas_call(
        pack_kernel,
        out_shape=(
            jax.ShapeDtypeStruct((OWNERS * ROWS, 128), F32),
            jax.ShapeDtypeStruct((1, PARTS), F32),
        ),
        in_specs=[pl.BlockSpec(memory_space=pltpu.SMEM), hbm, hbm, hbm, hbm],
        out_specs=(vmem, vmem),
        scratch_shapes=[
            pltpu.VMEM((1, PARTS), I32),
            pltpu.VMEM((1, PARTS), I32),
            pltpu.VMEM((1, PARTS), F32),
            pltpu.VMEM((3, 1, PARTS), F32),
            pltpu.VMEM((10 * OWNERS, CAP), F32),
            pltpu.SemaphoreType.DMA((4,)),
        ],
        compiler_params=pltpu.CompilerParams(vmem_limit_bytes=8 * MIB),
        name="pack",
    )(count, slab, cell, volume, drag)


CHUNKS, CHUNK = 16, 1024
CLASS_HIGH = HI // CLASSES
ABREAST = 8
ITEMS = CHUNKS * CLASSES + 16
NOWHERE = 1024


def swap_halves(first, second):
    lane = lax.broadcasted_iota(I32, (8, 128), 1)
    return (
        jnp.where(lane < 64, first, pltpu.roll(second, 64, 1)),
        jnp.where(lane < 64, pltpu.roll(first, 64, 1), second),
    )


def low_hots(low_ref, chunk):
    return jnp.concatenate([one_hot(low_ref[chunk, r : r + 1, :], LO) for r in range(8)], axis=1)


def deposit_kernel(
    recv_ref, solid_any, drag_any,
    out_ref, first_ref, last_ref, prior_ref, high_ref, low_ref, items_ref,
    solid_ref, drag_ref, values, bounds_ref, sems,
):
    copies = [
        pltpu.make_async_copy(solid_any, solid_ref, sems.at[0]),
        pltpu.make_async_copy(drag_any, drag_ref, sems.at[1]),
    ]
    for copy in copies:
        copy.start()
    out_ref[...] = jnp.zeros_like(out_ref)
    zero = jnp.zeros((), BF16)

    def chunked(comp):
        tile = jnp.concatenate([recv_ref[pl.ds(2 * comp + half, OWNERS, stride=ROWS), :] for half in range(2)], axis=0)
        slots = jnp.transpose(tile)
        pairs = [swap_halves(slots[16 * m : 16 * m + 8], slots[16 * m + 8 : 16 * m + 16]) for m in range(8)]
        return [pair[0] for pair in pairs] + [pair[1] for pair in pairs]

    volumes = chunked(1)
    for chunk, cell in enumerate(chunked(0)):
        cell = cell.astype(I32)
        layer = lax.shift_right_logical(cell, 13)
        high = ((lax.shift_right_logical(cell, 8) & 1) * 16 + (lax.shift_right_logical(cell, 9) & 15)) * 8 + layer
        high_ref[chunk] = high.astype(F32)
        low_ref[chunk] = (cell & 255).astype(F32)
        values[0, chunk] = volumes[chunk]
        live = volumes[chunk] > 0.0
        kind = lax.shift_right_logical(high, 5).astype(F32)
        bounds_ref[chunk, 0] = jnp.min(jnp.where(live, kind, float(CLASSES))).astype(I32)
        bounds_ref[chunk, 1] = jnp.max(jnp.where(live, kind, -1.0)).astype(I32) + 1
    for comp in range(1, 4):
        for chunk, value in enumerate(chunked(comp + 1)):
            values[comp, chunk] = value

    def list_chunk(chunk, count):
        def list_class(kind, count):
            items_ref[0, count] = chunk
            items_ref[1, count] = kind * CLASS_HIGH
            items_ref[2, count] = kind * CLASS_HIGH
            return count + 1

        return lax.fori_loop(bounds_ref[chunk, 0], bounds_ref[chunk, 1], list_class, count)

    count = lax.fori_loop(0, CHUNKS, list_chunk, 0)
    for spare in range(ABREAST):
        items_ref[0, count + spare] = 0
        items_ref[1, count + spare] = NOWHERE
        items_ref[2, count + spare] = 0
    steps = (count + ABREAST - 1) // ABREAST
    items_ref[0, ITEMS - 1] = steps

    def step(index, carry):
        totals = []
        for item in range(ABREAST):
            chunk = items_ref[0, index * ABREAST + item]
            key = high_ref[chunk] - items_ref[1, index * ABREAST + item].astype(F32)
            members = [row_is(key[r : r + 1], CLASS_HIGH) for r in range(8)]
            lows = low_hots(low_ref, chunk)
            left = []
            for comp in range(4):
                value = values[comp, chunk]
                top = value.astype(BF16).astype(F32)
                for piece in (top, value - top):
                    left.append(
                        jnp.concatenate(
                            [jnp.where(members[r], spread(piece[r : r + 1], CLASS_HIGH), zero) for r in range(8)],
                            axis=1,
                        )
                    )
            total = dot_nt(jnp.concatenate(left, axis=0), lows)
            totals.append(
                jnp.concatenate(
                    [
                        total[2 * comp * CLASS_HIGH : (2 * comp + 1) * CLASS_HIGH]
                        + total[(2 * comp + 1) * CLASS_HIGH : (2 * comp + 2) * CLASS_HIGH]
                        for comp in range(4)
                    ],
                    axis=0,
                )
            )
        for item in range(ABREAST):
            spot = pl.ds(pl.multiple_of(items_ref[2, index * ABREAST + item], CLASS_HIGH), CLASS_HIGH)
            for comp in range(4):
                out_ref[comp, spot, :] += totals[item][comp * CLASS_HIGH : (comp + 1) * CLASS_HIGH, :]
        return carry

    lax.fori_loop(0, steps, step, 0)
    out_ref[0] = jnp.minimum(out_ref[0], PHI_LIMIT)
    for copy in copies:
        copy.wait()
    for row in range(4 * CX):
        prior_ref[row * LAYERS : (row + 1) * LAYERS, :] = prior_row(solid_ref, drag_ref, row, slice(None))

    def pieces(row):
        if row >= 4 * CX:
            row -= 4 * CX
            spot = slice(row * LAYERS, (row + 1) * LAYERS)
            return prior_ref[spot, 0:128], prior_ref[spot, CY - 128 : CY]
        comp, x = row // CX, row % CX
        first = out_ref[comp, x * LAYERS : (x + 1) * LAYERS, 0:128]
        last = out_ref[comp, (CX + x) * LAYERS : (CX + x + 1) * LAYERS, LO - 128 : LO]
        return first, last

    fold_sides(pieces, first_ref, last_ref)


def deposit(received, solid, drag):
    vmem = pl.BlockSpec(memory_space=pltpu.VMEM)
    hbm = pl.BlockSpec(memory_space=pltpu.HBM)
    side = jax.ShapeDtypeStruct((SIDE_ROWS, 128), F32)
    index = jax.ShapeDtypeStruct((CHUNKS, 8, 128), F32)
    return pl.pallas_call(
        deposit_kernel,
        out_shape=(
            jax.ShapeDtypeStruct((4, HI, LO), F32),
            side,
            side,
            jax.ShapeDtypeStruct((4 * CX * LAYERS, CY), F32),
            index,
            index,
            jax.ShapeDtypeStruct((3, ITEMS), I32),
        ),
        in_specs=[vmem, hbm, hbm],
        out_specs=(vmem,) * 6 + (pl.BlockSpec(memory_space=pltpu.SMEM),),
        scratch_shapes=[
            pltpu.VMEM((LAYERS, CX, CY), F32),
            pltpu.VMEM((3, LAYERS, CX, CY), F32),
            pltpu.VMEM((4, CHUNKS, 8, 128), F32),
            pltpu.SMEM((CHUNKS, 2), I32),
            pltpu.SemaphoreType.DMA((2,)),
        ],
        compiler_params=pltpu.CompilerParams(vmem_limit_bytes=16 * MIB),
        name="deposit",
    )(received, solid, drag)


def gather_kernel(
    items_ref, own_ref, above_ref, below_ref, high_ref, low_ref, fields_any, out_ref,
    fields, tops, bottoms, found, sem,
):
    top, bottom = at_edge("span")

    def smooth(comp, x):
        row = own_ref[pl.ds((comp * CX + x) * LAYERS, LAYERS), :]
        if x < RIM:
            spot = pl.ds((comp * RIM + x) * LAYERS, LAYERS)
            row = row + jnp.where(top, 0.0, above_ref[spot, :])
        if x >= CX - RIM:
            spot = pl.ds((comp * RIM + x - CX + RIM) * LAYERS, LAYERS)
            row = row + jnp.where(bottom, 0.0, below_ref[spot, :])
        return row

    for pair in range(0, CX, 2):
        void = [1.0 - smooth(0, x) for x in (pair, pair + 1)]
        for comp in range(4):
            rows = void if comp == 0 else [-smooth(comp, x) / v for x, v in zip((pair, pair + 1), void)]
            for x, row in zip((pair, pair + 1), rows):
                fields[comp, :, x, :] = row
            high, low = halves(jnp.concatenate(rows, axis=0))
            for half in range(2):
                spot = pl.ds((half * CX + pair) * LAYERS, 2 * LAYERS)
                tops[comp, spot, :] = high[:, half * LO : (half + 1) * LO]
                bottoms[comp, spot, :] = low[:, half * LO : (half + 1) * LO]
    copy = pltpu.make_async_copy(fields, fields_any, sem)
    copy.start()
    ids = lax.broadcasted_iota(I32, (CLASS_HIGH, 128), 0).astype(F32)

    found[...] = jnp.zeros_like(found)

    def step(index, carry):
        news = []
        for item in range(ABREAST):
            chunk = items_ref[0, index * ABREAST + item]
            key = high_ref[chunk] - items_ref[1, index * ABREAST + item].astype(F32)
            lows = low_hots(low_ref, chunk)
            spot = pl.ds(pl.multiple_of(items_ref[2, index * ABREAST + item], CLASS_HIGH), CLASS_HIGH)
            members = [ids == key[r : r + 1] for r in range(8)]
            table = jnp.concatenate([part[comp, spot, :] for part in (tops, bottoms) for comp in range(4)], axis=0)
            value = dot_nn(table, lows)
            value = value[: 4 * CLASS_HIGH] + value[4 * CLASS_HIGH :]
            new = []
            for comp in range(4):
                rows = value[comp * CLASS_HIGH : (comp + 1) * CLASS_HIGH]
                pieces = [
                    jnp.sum(jnp.where(members[r], rows[:, r * 128 : (r + 1) * 128], 0.0), axis=0, keepdims=True)
                    for r in range(8)
                ]
                new.append(jnp.concatenate(pieces, axis=0))
            news.append(new)
        for item in range(ABREAST):
            chunk = items_ref[0, index * ABREAST + item]
            for comp in range(4):
                found[comp, chunk] += news[item][comp]
        return carry

    lax.fori_loop(0, items_ref[0, ITEMS - 1], step, 0)
    for comp in range(4):
        slots = []
        for m in range(8):
            slots += swap_halves(found[comp, m], found[comp, m + 8])
        tile = jnp.transpose(jnp.concatenate(slots, axis=0))
        for half in range(2):
            out_ref[pl.ds(2 * comp + half, OWNERS, stride=BACK_ROWS), :] = tile[half * OWNERS : (half + 1) * OWNERS]
    copy.wait()


def gather(items, *arrays):
    vmem = pl.BlockSpec(memory_space=pltpu.VMEM)
    return pl.pallas_call(
        gather_kernel,
        out_shape=(
            jax.ShapeDtypeStruct((4, LAYERS, CX, CY), F32),
            jax.ShapeDtypeStruct((OWNERS * BACK_ROWS, 128), F32),
        ),
        in_specs=[pl.BlockSpec(memory_space=pltpu.SMEM)] + [vmem] * 5,
        out_specs=(pl.BlockSpec(memory_space=pltpu.HBM), vmem),
        scratch_shapes=[
            pltpu.VMEM((4, LAYERS, CX, CY), F32),
            pltpu.VMEM((4, HI, LO), BF16),
            pltpu.VMEM((4, HI, LO), BF16),
            pltpu.VMEM((4, CHUNKS, 8, 128), F32),
            pltpu.SemaphoreType.DMA,
        ],
        compiler_params=pltpu.CompilerParams(vmem_limit_bytes=16 * MIB),
        name="gather",
    )(items, *arrays)


PICK_BLOCK = 4096


def pick_kernel(count_ref, slab_ref, position_ref, back_ref, out_ref, tops, bottoms):
    count = count_ref[0, 0]
    for comp in range(4):
        tile = jnp.concatenate(
            [back_ref[pl.ds(2 * comp + half, OWNERS, stride=BACK_ROWS), :] for half in range(2)], axis=1
        )
        high, low = halves(tile)
        tops[comp * OWNERS : (comp + 1) * OWNERS, :] = high
        bottoms[comp * OWNERS : (comp + 1) * OWNERS, :] = low

    def step(block, carry):
        start = pl.multiple_of(block * PICK_BLOCK, PICK_BLOCK)
        spot = pl.ds(start, PICK_BLOCK)
        lane = lax.broadcasted_iota(I32, (1, PICK_BLOCK), 1) + start
        slab = jnp.where(lane < count, slab_ref[0:1, spot], OWNERS)
        position_hot = one_hot(position_ref[0:1, spot], CAP)
        value = dot_nn(tops[...], position_hot) + dot_nn(bottoms[...], position_hot)
        member = lax.broadcasted_iota(I32, (OWNERS, PICK_BLOCK), 0) == slab
        for comp in range(4):
            piece = value[comp * OWNERS : (comp + 1) * OWNERS, :]
            out_ref[comp, 0:1, spot] = jnp.sum(jnp.where(member, piece, 0.0), axis=0, keepdims=True)
        return carry

    lax.fori_loop(0, PARTS // PICK_BLOCK, step, 0)


def pick(count, slab, position, back):
    vmem = pl.BlockSpec(memory_space=pltpu.VMEM)
    return pl.pallas_call(
        pick_kernel,
        out_shape=jax.ShapeDtypeStruct((4, 1, PARTS), F32),
        in_specs=[pl.BlockSpec(memory_space=pltpu.SMEM), vmem, vmem, vmem],
        out_specs=vmem,
        scratch_shapes=[pltpu.VMEM((4 * OWNERS, CAP), BF16)] * 2,
        name="pick",
        compiler_params=pltpu.CompilerParams(vmem_limit_bytes=8 * MIB),
    )(count, slab, position, back)


WIDE = CY + 128
RELAX_FLOPS = 40_000_000


def relax_kernel(for_rim, target_ref, prior_ref, before, after, *refs):
    outs, (state, source) = refs[:-2], refs[-2:]
    top, bottom = at_edge("span")
    first, last = at_edge("depth")
    near = lax.broadcasted_iota(I32, (LAYERS, 128), 1)
    is_before = (near >= 120) & jnp.logical_not(first)
    is_after = (near < 8) & jnp.logical_not(last)
    blank = jnp.zeros((LAYERS, WIDE), F32)
    for comp in range(4):
        for x in range(CX):
            if for_rim and RIM <= x < CX - RIM:
                continue
            row = comp * CX + x
            for half in range(2):
                spot = pl.ds((half * CX + x) * LAYERS, LAYERS)
                source[comp, x, :, half * LO : (half + 1) * LO] = target_ref[comp, spot, :]
            source[comp, x, :, CY:WIDE] = unfold_side(row, before, after, is_before, is_after)
            state[comp, RIM + x, :, 0:CY] = prior_ref[row * LAYERS : (row + 1) * LAYERS, :]
            state[comp, RIM + x, :, CY:WIDE] = unfold_side(4 * CX + row, before, after, is_before, is_after)

    lane = lax.broadcasted_iota(I32, (LAYERS, WIDE), 1)
    outside = ((lane >= CY + 64) & first) | ((lane >= CY) & (lane < CY + 64) & last)
    factor = jnp.where(outside, 0.0, 0.2)
    above_factor = jnp.where(top, 0.0, factor)
    below_factor = jnp.where(bottom, 0.0, factor)

    def sweep_rows(comp, sweep, low, high):
        def old(x):
            return state[comp, x + RIM] if -sweep < x < CX - 1 + sweep else blank

        above, here = old(low - 1), old(low)
        for x in range(low, high + 1):
            below = old(x + 1)
            total = above + below
            if -sweep < x < CX - 1 + sweep:
                total = total + pltpu.roll(here, 1, 1) + pltpu.roll(here, WIDE - 1, 1)
            if 0 <= x < CX:
                total = total + source[comp, x]
            scale = above_factor if x < 0 else below_factor if x >= CX else factor
            state[comp, x + RIM] = total * scale
            above, here = here, below

    def comp_step(comp, carry):
        for sweep in range(1, SWEEPS + 1):
            if for_rim:
                sweep_rows(comp, sweep, -sweep, RIM - 1 - sweep)
                sweep_rows(comp, sweep, CX - RIM + sweep, CX - 1 + sweep)
            else:
                reach = min(sweep, SWEEPS - sweep)
                sweep_rows(comp, sweep, -reach, CX - 1 + reach)
        return carry

    lax.fori_loop(0, 4, comp_step, 0)
    for comp in range(4):
        if for_rim:
            for x in range(RIM):
                spot = pl.ds((comp * RIM + x) * LAYERS, LAYERS)
                outs[0][spot, :] = state[comp, x, :, 0:CY]
                outs[1][spot, :] = state[comp, RIM + CX + x, :, 0:CY]
        else:
            for x in range(CX):
                outs[0][pl.ds((comp * CX + x) * LAYERS, LAYERS), :] = state[comp, RIM + x, :, 0:CY]


def relax(for_rim, *arrays):
    vmem = pl.BlockSpec(memory_space=pltpu.VMEM)
    rim = jax.ShapeDtypeStruct((4 * RIM * LAYERS, CY), F32)
    own = jax.ShapeDtypeStruct((4 * CX * LAYERS, CY), F32)
    return pl.pallas_call(
        functools.partial(relax_kernel, for_rim),
        out_shape=(rim, rim) if for_rim else own,
        in_specs=[vmem] * 4,
        out_specs=(vmem, vmem) if for_rim else vmem,
        scratch_shapes=[
            pltpu.VMEM((4, CX + 2 * RIM, LAYERS, WIDE), F32),
            pltpu.VMEM((4, CX, LAYERS, WIDE), F32),
        ],
        compiler_params=pltpu.CompilerParams(vmem_limit_bytes=12 * MIB),
        cost_estimate=pl.CostEstimate(flops=RELAX_FLOPS, bytes_accessed=4 * MIB, transcendentals=0),
        name="relax_rim" if for_rim else "relax_own",
    )(*arrays)


def shifted(array, axis, step):
    count = lax.axis_size(axis)
    return lax.ppermute(array, axis, [(i, (i + step) % count) for i in range(count)])


def on_device(part_slab, part_cell, part_volume, part_drag, part_count, prior_solid, prior_drag):
    slab = part_slab.reshape(1, PARTS)
    in_hbm = [pltpu.with_memory_space_constraint(a, pltpu.HBM) for a in (slab, part_cell, part_volume, part_drag)]
    sent, position = pack(part_count, *in_hbm)
    received = lax.all_to_all(sent.reshape(OWNERS, 5, 2, 128), "span", 0, 0, tiled=True)
    received = received.reshape(OWNERS * ROWS, 128)
    target, first, last, prior, high, low, items = deposit(
        received, *[pltpu.with_memory_space_constraint(a, pltpu.HBM) for a in (prior_solid, prior_drag)]
    )
    before = shifted(last, "depth", 1)
    after = shifted(first, "depth", -1)
    arrays = (target, prior, before, after)
    up, down = relax(True, *arrays)
    from_above = shifted(down, "span", 1)
    from_below = shifted(up, "span", -1)
    own = relax(False, *arrays)
    fields, returned = gather(items, own, from_above, from_below, high, low)
    back = lax.all_to_all(returned.reshape(OWNERS, BACK_ROWS, 128), "span", 0, 0, tiled=True)
    feedback = pick(part_count, slab, position, back.reshape(OWNERS * BACK_ROWS, 128))
    return fields, feedback


def solution(mesh):
    in_specs = (
        P("depth", "span", None),
        P("depth", "span"),
        P("depth", "span"),
        P(None, "depth", "span"),
        P("depth", "span"),
        P(None, "span", "depth"),
        P(None, None, "span", "depth"),
    )
    out_specs = (P(None, None, "span", "depth"), P(None, "depth", "span"))
    return jax.shard_map(on_device, mesh=mesh, in_specs=in_specs, out_specs=out_specs, check_vma=False)
```
